32 devices in a mesh: shard: 2 (over x), replica: 16 (over z, y, core).
Axes of the slice: x: 2, y: 2, z: 4, core: 2. Of those that a mesh axis runs over, the one named last changes fastest.
Arguments:
- tokens: bfloat16 [8192, 1152], P(('shard', 'replica')), may hold values from -6 to 6
- out_grad: bfloat16 [8192, 1152], P(('shard', 'replica')), may hold values from -6 to 6
- picture_ids: int32 [8192], P(('shard', 'replica')), may hold values from 0 to 3, as said below
- live_slots: int32 [8192], P(('shard', 'replica')), may hold values from 0 to 1, as said below
- ln1_gain: bfloat16 [1152], P('shard'), may hold values from 0.099609375 to 1.8984375
- ln1_bias: bfloat16 [1152], P('shard'), may hold values from -3 to 3
- query_weight: bfloat16 [1152, 1152], P(None, 'shard'), may hold values from -0.1875 to 0.1875
- query_bias: bfloat16 [1152], P('shard'), may hold values from -3 to 3
- key_weight: bfloat16 [1152, 1152], P(None, 'shard'), may hold values from -0.1875 to 0.1875
- value_weight: bfloat16 [1152, 1152], P(None, 'shard'), may hold values from -0.1875 to 0.1875
- value_bias: bfloat16 [1152], P('shard'), may hold values from -3 to 3
- proj_weight: bfloat16 [1152, 1152], P('shard'), may hold values from -1.5 to 1.5
- proj_bias: bfloat16 [1152], P('shard'), may hold values from -3 to 3
- ln2_gain: bfloat16 [1152], P('shard'), may hold values from 0.099609375 to 1.8984375
- ln2_bias: bfloat16 [1152], P('shard'), may hold values from -3 to 3
- up_weight: bfloat16 [1152, 4304], P(None, 'shard'), may hold values from -0.1875 to 0.1875
- up_bias: bfloat16 [4304], P('shard'), may hold values from -3 to 3
- down_weight: bfloat16 [4304, 1152], P('shard'), may hold values from -0.09375 to 0.09375
- down_bias: bfloat16 [1152], P('shard'), may hold values from -3 to 3
Outputs:
- block_out: bfloat16 [8192, 1152], P(('shard', 'replica'))
- tokens_grad: bfloat16 [8192, 1152], P(('shard', 'replica'))
- ln1_gain_grad: float32 [1152], P('shard')
- ln1_bias_grad: float32 [1152], P('shard')
- query_weight_grad: float32 [1152, 1152], P('replica', 'shard')
- query_bias_grad: float32 [1152], P('shard')
- key_weight_grad: float32 [1152, 1152], P('replica', 'shard')
- value_weight_grad: float32 [1152, 1152], P('replica', 'shard')
- value_bias_grad: float32 [1152], P('shard')
- proj_weight_grad: float32 [1152, 1152], P('shard', 'replica')
- proj_bias_grad: float32 [1152], P('shard')
- ln2_gain_grad: float32 [1152], P('shard')
- ln2_bias_grad: float32 [1152], P('shard')
- up_weight_grad: float32 [1152, 4304], P('replica', 'shard')
- up_bias_grad: float32 [4304], P('shard')
- down_weight_grad: float32 [4304, 1152], P('shard', 'replica')
- down_bias_grad: float32 [1152], P('shard')
The draws below stay inside these ranges and needn't reach their ends.
Inputs may be any that keep to these rules, and one draw needn't show every extreme that they name: `picture_ids`: within each aligned block of 256 slots (one device's) the ids start at 0, never fall, and every id occurs; pad slots carry the id of the block's last picture. `live_slots`: within each aligned block of 256 slots the zeros, if any, are the last slots, and every picture has live slots.
All inputs are finite; a program needn't handle non-finite values.
Results may differ from the reference program's by a relative error of at most 0.014.
Values may be sent and summed in bfloat16 or wider, within the bound.
A program may use at most 192 MiB of HBM per device.

```python
import jax
import jax.numpy as jnp
from jax import lax

D = 1152
HEADS = 16
HDIM = 72
FF = 4304
TOK_DEV = 256
PICS = 4
TOKENS = 8192


def slot_layout(key):
    row_count = TOKENS // TOK_DEV
    picture_sizes = jax.random.randint(jax.random.fold_in(key, 7), (row_count, PICS - 1), TOK_DEV // 16, TOK_DEV // 4 + 1)
    padding = jax.random.randint(jax.random.fold_in(key, 9), (row_count, 1), 0, TOK_DEV // 16 + 1)
    bounds = jnp.cumsum(picture_sizes, axis=1)
    slot_index = jnp.arange(TOK_DEV, dtype=jnp.int32)[None, :]
    picture = jnp.sum((slot_index[:, :, None] >= bounds[:, None, :]).astype(jnp.int32), axis=2)
    alive_rows = (slot_index < TOK_DEV - padding).astype(jnp.int32)
    return (picture.reshape(TOKENS), alive_rows.reshape(TOKENS))


def draw_picture_ids(key, part):
    return slot_layout(key)[0]


def draw_live_slots(key, part):
    return slot_layout(key)[1]


def block_levels(key, shape, shards, smallest, largest):
    loudness, own = 1.0, jax.random.fold_in(key, 6)
    for dim, blocks in shards:
        steps = jnp.exp(jax.random.uniform(jax.random.fold_in(own, dim), (blocks,), jnp.float32, smallest / len(shards), largest / len(shards)))
        loudness = loudness * jnp.repeat(steps, shape[dim] // blocks).reshape([-1 if axis == dim else 1 for axis in range(len(shape))])
    return loudness


def bell_draw(rng, dims, deviation, reach, cuts=(), kind=jnp.bfloat16):
    drawn = deviation * jax.random.normal(rng, dims, jnp.float32)
    if cuts:
        drawn = drawn * block_levels(rng, dims, cuts, -0.22, 0.18)
    return jnp.clip(drawn, -reach, reach).astype(kind)


def setup_inputs(seed: int = 0) -> dict:
    arg_keys = jax.random.split(jax.random.key(seed), 20)
    return {
        "tokens": bell_draw(arg_keys[0], (TOKENS, D), 1.0, 6.0, ((0, 32),)),
        "out_grad": bell_draw(arg_keys[1], (TOKENS, D), 1.0, 6.0, ((0, 32),)),
        "picture_ids": draw_picture_ids(jax.random.fold_in(arg_keys[19], 71), 0),
        "live_slots": draw_live_slots(jax.random.fold_in(arg_keys[19], 71), 0),
        "ln1_gain": jnp.clip(1.0 + 0.18 * jax.random.normal(arg_keys[4], (D,), jnp.float32), 0.099609375, 1.8984375).astype(jnp.bfloat16),
        "ln1_bias": bell_draw(arg_keys[5], (D,), 0.5, 3.0, ((0, 2),)),
        "query_weight": bell_draw(arg_keys[6], (D, D), D ** -0.5, 0.1875, ((1, 2),)),
        "query_bias": bell_draw(arg_keys[7], (D,), 0.5, 3.0, ((0, 2),)),
        "key_weight": bell_draw(arg_keys[8], (D, D), D ** -0.5, 0.1875, ((1, 2),)),
        "value_weight": bell_draw(arg_keys[9], (D, D), D ** -0.5, 0.1875, ((1, 2),)),
        "value_bias": bell_draw(arg_keys[10], (D,), 0.5, 3.0, ((0, 2),)),
        "proj_weight": bell_draw(arg_keys[11], (D, D), 16 ** -0.5, 1.5, ((0, 2),)),
        "proj_bias": bell_draw(arg_keys[12], (D,), 0.5, 3.0, ((0, 2),)),
        "ln2_gain": jnp.clip(1.0 + 0.18 * jax.random.normal(arg_keys[13], (D,), jnp.float32), 0.099609375, 1.8984375).astype(jnp.bfloat16),
        "ln2_bias": bell_draw(arg_keys[14], (D,), 0.5, 3.0, ((0, 2),)),
        "up_weight": bell_draw(arg_keys[15], (D, FF), D ** -0.5, 0.1875, ((1, 2),)),
        "up_bias": bell_draw(arg_keys[16], (FF,), 0.5, 3.0, ((0, 2),)),
        "down_weight": bell_draw(arg_keys[17], (FF, D), FF ** -0.5, 0.09375, ((0, 2),)),
        "down_bias": bell_draw(arg_keys[18], (D,), 0.5, 3.0, ((0, 2),)),
    }


@jax.custom_vjp
def low(v):
    return lax.optimization_barrier(v.astype(jnp.bfloat16)).astype(jnp.float32)

@jax.custom_vjp
def low_back(v):
    return v

def low_keep(v):
    return (low(v), None)

def low_pass(kept, grad):
    return (grad,)

def back_keep(v):
    return (v, None)

def back_low(kept, grad):
    return (low(grad),)
low.defvjp(low_keep, low_pass)
low_back.defvjp(back_keep, back_low)
highest = lax.Precision.HIGHEST
norm_eps = 1e-06

def layer_norm(values, scale_gain, shift_bias):
    centered = values - lax.optimization_barrier(jnp.mean(values, axis=-1, keepdims=True))
    variance = lax.optimization_barrier(jnp.mean(centered * centered, axis=-1, keepdims=True))
    return centered * lax.rsqrt(variance + norm_eps) * scale_gain + shift_bias

def matmul(left_side, right_side):
    return jnp.dot(left_side, right_side, precision=highest)

def attend_block(block_args):
    queries, keys_in, values_in, picture, alive_rows = block_args
    split_q = queries.reshape(TOK_DEV, HEADS, HDIM)
    split_k = keys_in.reshape(TOK_DEV, HEADS, HDIM)
    split_v = values_in.reshape(TOK_DEV, HEADS, HDIM)
    scores = jnp.einsum('qhd,khd->hqk', split_q, split_k, precision=highest) * HDIM ** (-0.5)
    scores = low_back(scores)
    allowed = (picture[:, None] == picture[None, :]) & (alive_rows[None, :] == 1)
    scores = jnp.where(allowed[None, :, :], scores, -1e+30)
    attn_probs = low(jax.nn.softmax(scores, axis=-1))
    mixed_out = jnp.einsum('hqk,khd->qhd', attn_probs, split_v, precision=highest)
    return mixed_out.reshape(TOK_DEV, HEADS * HDIM)

def forward(tokens_f, weights_f, picture_ids, live_slots):
    ln1_gain, ln1_bias, query_weight, query_bias, key_weight, value_weight, value_bias, proj_weight, proj_bias, ln2_gain, ln2_bias, up_weight, up_bias, down_weight, down_bias = weights_f
    alive_cols = live_slots.astype(tokens_f.dtype)[:, None]
    normed = low(layer_norm(tokens_f, ln1_gain, ln1_bias))
    queries = low_back(low(matmul(normed, query_weight) + query_bias))
    keys_all = low_back(low(matmul(normed, key_weight)))
    values_all = low_back(low(matmul(normed, value_weight) + value_bias))
    block_args = (queries.reshape(-1, TOK_DEV, D), keys_all.reshape(-1, TOK_DEV, D), values_all.reshape(-1, TOK_DEV, D), picture_ids.reshape(-1, TOK_DEV), live_slots.reshape(-1, TOK_DEV))
    mixed_out = lax.map(jax.checkpoint(attend_block), block_args).reshape(-1, D)
    mixed_out = low_back(low(mixed_out))
    hidden = tokens_f + low_back(matmul(mixed_out, proj_weight) + proj_bias)
    normed_two = low(layer_norm(hidden, ln2_gain, ln2_bias))
    up_proj = low_back(matmul(normed_two, up_weight) + up_bias)
    activated = low(jax.nn.gelu(up_proj, approximate=True))
    return (hidden + low_back(matmul(activated, down_weight) + down_bias)) * alive_cols

def reference(tokens, out_grad, picture_ids, live_slots, ln1_gain, ln1_bias, query_weight, query_bias, key_weight, value_weight, value_bias, proj_weight, proj_bias, ln2_gain, ln2_bias, up_weight, up_bias, down_weight, down_bias):
    params_f = tuple((tensor.astype(jnp.float32) for tensor in (ln1_gain, ln1_bias, query_weight, query_bias, key_weight, value_weight, value_bias, proj_weight, proj_bias, ln2_gain, ln2_bias, up_weight, up_bias, down_weight, down_bias)))

    def layer_fn(tokens_f, weights_f):
        return forward(tokens_f, weights_f, picture_ids, live_slots)
    block_out, pull_back = jax.vjp(layer_fn, tokens.astype(jnp.float32), params_f)
    tokens_grad, weight_grads = pull_back(out_grad.astype(jnp.float32))
    return (block_out.astype(jnp.bfloat16), tokens_grad.astype(jnp.bfloat16), weight_grads[0], weight_grads[1], weight_grads[2], weight_grads[3], weight_grads[4], weight_grads[5], weight_grads[6], weight_grads[7], weight_grads[8], weight_grads[9], weight_grads[10], weight_grads[11], weight_grads[12], weight_grads[13], weight_grads[14])
```

```python
import functools

import jax
import jax.numpy as jnp
from jax import lax
from jax.experimental import pallas as pl
from jax.experimental.pallas import tpu as pltpu
from jax.sharding import PartitionSpec as P

HDIM = 72
norm_eps = 1e-06
MESH = pl.DeviceIdType.MESH
CW = 256


def norm_stats(values):
    centered = values - jnp.mean(values, axis=-1, keepdims=True)
    variance = jnp.mean(centered * centered, axis=-1, keepdims=True)
    inverse = lax.rsqrt(variance + norm_eps)
    return centered * inverse, inverse


def norm_grad(xhat, inverse, gain, grad):
    scaled = grad * gain
    return (
        scaled
        - jnp.mean(scaled, axis=-1, keepdims=True)
        - xhat * jnp.mean(scaled * xhat, axis=-1, keepdims=True)
    ) * inverse


def gelu_tanh(values):
    return jax.nn.gelu(values, approximate=True)


def product(left_side, right_side):
    return jnp.dot(left_side, right_side, preferred_element_type=jnp.float32)


def product_nt(left_side, right_side):
    return lax.dot_general(
        left_side, right_side, (((1,), (1,)), ((), ())), preferred_element_type=jnp.float32
    )


def product_tn(left_side, right_side):
    return lax.dot_general(
        left_side, right_side, (((0,), (0,)), ((), ())), preferred_element_type=jnp.float32
    )


def column_sums(matrix):
    return jnp.sum(matrix, axis=0, dtype=jnp.float32)


def swap(value):
    return lax.ppermute(value, "shard", [(0, 1), (1, 0)])


def split_heads(matrix, block_rows):
    return matrix.reshape(-1, block_rows, matrix.shape[1] // HDIM, HDIM)


def attend(queries, keys_in, values_in, allowed, block_rows):
    scores = jnp.einsum(
        "bqhd,bkhd->bhqk",
        split_heads(queries, block_rows),
        split_heads(keys_in, block_rows),
        preferred_element_type=jnp.float32,
    ) * HDIM ** (-0.5)
    scores = jnp.where(allowed[:, None, :, :], scores, -1e30)
    highest = jnp.max(scores, axis=-1, keepdims=True)
    scaled_exp = jnp.exp(scores - highest)
    totals = jnp.sum(scaled_exp, axis=-1, keepdims=True)
    probs = scaled_exp / totals
    mixed_out = jnp.einsum(
        "bhqk,bkhd->bqhd",
        probs.astype(jnp.bfloat16),
        split_heads(values_in, block_rows),
        preferred_element_type=jnp.float32,
    )
    return mixed_out.reshape(queries.shape), probs


def attend_back(queries, keys_in, values_in, grad_mixed, probs, block_rows):
    score_scale = HDIM ** (-0.5)
    split_grad = split_heads(grad_mixed, block_rows)
    grad_probs = jnp.einsum(
        "bqhd,bkhd->bhqk",
        split_grad,
        split_heads(values_in, block_rows),
        preferred_element_type=jnp.float32,
    )
    grad_scores = (
        probs * (grad_probs - jnp.sum(probs * grad_probs, axis=-1, keepdims=True))
    ).astype(jnp.bfloat16)
    grad_queries = (
        jnp.einsum(
            "bhqk,bkhd->bqhd",
            grad_scores,
            split_heads(keys_in, block_rows),
            preferred_element_type=jnp.float32,
        )
        * score_scale
    )
    grad_keys = (
        jnp.einsum(
            "bhqk,bqhd->bkhd",
            grad_scores,
            split_heads(queries, block_rows),
            preferred_element_type=jnp.float32,
        )
        * score_scale
    )
    grad_values = jnp.einsum(
        "bhqk,bqhd->bkhd",
        probs.astype(jnp.bfloat16),
        split_grad,
        preferred_element_type=jnp.float32,
    )
    return (
        grad_queries.astype(jnp.bfloat16).reshape(queries.shape),
        grad_keys.astype(jnp.bfloat16).reshape(queries.shape),
        grad_values.astype(jnp.bfloat16).reshape(queries.shape),
    )


def add_low(first, second):
    return (first.astype(jnp.float32) + second.astype(jnp.float32)).astype(jnp.bfloat16)


def reduce_kernel(
    wide_left,
    wide_right,
    thin_left,
    thin_first,
    thin_second,
    vectors,
    sums_out,
    vectors_out,
    wide_left_in,
    wide_right_in,
    thin_left_in,
    thin_other_in,
    thin_first_in,
    thin_second_in,
    grads,
    from_y,
    from_low,
    from_high,
    summed,
    vector_sum,
    vector_in,
    pair_send,
    pair_recv,
    y_send,
    y_recv,
    low_send,
    low_recv,
    high_send,
    high_recv,
    core_send,
    core_recv,
    vec_send,
    vec_recv,
):
    chunks = grads.shape[0]
    rows = grads.shape[4]
    wide_chunks = chunks - 5
    shard = lax.axis_index("shard")
    replica = lax.axis_index("replica")
    core = lax.rem(replica, 2)
    y_bit = lax.rem(replica // 2, 2)
    low_bit = lax.rem(replica // 4, 2)
    high_bit = lax.rem(replica // 8, 2)
    partner = (shard, replica + 1 - 2 * core)
    y_peer = (shard, replica + 2 - 4 * y_bit)
    low_peer = (shard, replica + 4 - 8 * low_bit)
    high_peer = (shard, replica + 8 - 16 * high_bit)
    peers = (partner, y_peer, low_peer, high_peer)
    barrier = pltpu.get_barrier_semaphore()
    for peer in peers:
        pl.semaphore_signal(barrier, inc=1, device_id=peer, device_id_type=MESH)
    pl.semaphore_wait(barrier, len(peers))

    def remote(source, target, send, recv, peer):
        return pltpu.make_async_remote_copy(
            src_ref=source,
            dst_ref=target,
            send_sem=send,
            recv_sem=recv,
            device_id=peer,
            device_id_type=MESH,
        )

    other = 1 - core
    pairs = (
        (wide_left.at[other], wide_left_in),
        (wide_right.at[other], wide_right_in),
        (thin_left.at[0], thin_left_in),
        (thin_left.at[other], thin_other_in),
        (thin_first.at[other], thin_first_in),
        (thin_second.at[other], thin_second_in),
    )
    pair_copies = [
        remote(source, target, pair_send.at[i], pair_recv.at[i], partner)
        for i, (source, target) in enumerate(pairs)
    ]
    for copy in pair_copies:
        copy.start()

    def y_copy(j):
        return remote(
            grads.at[j, :, :, 1 - y_bit], from_y.at[j], y_send.at[j], y_recv.at[j], y_peer
        )

    def low_copy(j):
        return remote(
            grads.at[j, :, 1 - low_bit, y_bit],
            from_low.at[j],
            low_send.at[j],
            low_recv.at[j],
            low_peer,
        )

    def high_copy(j):
        return remote(
            grads.at[j, 1 - high_bit, low_bit, y_bit],
            from_high.at[j],
            high_send.at[j],
            high_recv.at[j],
            high_peer,
        )

    def core_copy(j):
        return remote(
            summed.at[j, other], sums_out.at[core, j], core_send.at[j], core_recv.at[j], partner
        )

    def core_arrival(j):
        return remote(
            summed.at[j, other], sums_out.at[other, j], core_send.at[j], core_recv.at[j], partner
        )

    def vector_copy(i):
        return remote(
            vector_sum.at[i], vector_in.at[i], vec_send.at[i], vec_recv.at[i], peers[i]
        )

    vector_sum[0] = vectors[...]
    vector_copy(0).start()

    def keep(j, value):
        grads[j] = value.astype(jnp.bfloat16).reshape(grads.shape[1:])
        y_copy(j).start()

    pair_copies[0].wait_recv()
    pair_copies[1].wait_recv()

    def wide_step(j, carry):
        columns = pl.ds(pl.multiple_of(j * CW, CW), CW)
        keep(
            j,
            product_tn(wide_left[core], wide_right[core, :, columns])
            + product_tn(wide_left_in[...], wide_right_in[:, columns]),
        )
        return carry

    lax.fori_loop(0, wide_chunks, wide_step, 0)
    for copy in pair_copies[2:]:
        copy.wait_recv()

    def first_part(columns):
        return product_tn(thin_left[0], thin_first[core, :, columns]) + product_tn(
            thin_left_in[...], thin_first_in[:, columns]
        )

    def second_part(columns):
        return product_tn(thin_left[core], thin_second[core, :, columns]) + product_tn(
            thin_other_in[...], thin_second_in[:, columns]
        )

    def thin_step(j, carry):
        columns = pl.ds(pl.multiple_of(j * CW, CW), CW)
        keep(wide_chunks + j, first_part(columns))
        keep(wide_chunks + 2 + j, second_part(columns))
        return carry

    lax.fori_loop(0, 2, thin_step, 0)
    thin_rest = pl.ds(2 * CW, thin_first.shape[2] - 2 * CW)
    wide_rest = pl.ds(wide_chunks * CW, CW // 2)
    keep(
        chunks - 1,
        jnp.concatenate(
            [
                product_tn(wide_left[core], wide_right[core, :, wide_rest])
                + product_tn(wide_left_in[...], wide_right_in[:, wide_rest]),
                first_part(thin_rest),
                second_part(thin_rest),
            ],
            axis=1,
        ),
    )

    for i in range(4):
        vector_copy(i).wait_recv()
        vector_sum[i + 1] = vector_sum[i] + vector_in[i]
        if i < 3:
            vector_copy(i + 1).start()
    vectors_out[...] = vector_sum[4]

    def pump(i, carry):
        @pl.when(i < chunks)
        def _():
            y_copy(i).wait_recv()
            grads[i, :, :, y_bit] = add_low(grads[i, :, :, y_bit], from_y[i])
            low_copy(i).start()

        @pl.when(jnp.logical_and(i >= 1, i < chunks + 1))
        def _():
            j = i - 1
            low_copy(j).wait_recv()
            grads[j, :, low_bit, y_bit] = add_low(grads[j, :, low_bit, y_bit], from_low[j])
            high_copy(j).start()

        @pl.when(jnp.logical_and(i >= 2, i < chunks + 2))
        def _():
            j = i - 2
            high_copy(j).wait_recv()
            total = grads[j, high_bit, low_bit, y_bit].astype(jnp.float32) + from_high[j].astype(
                jnp.float32
            )
            summed[j] = total.reshape(2, rows // 2, CW)
            core_copy(j).start()
            sums_out[core, j] = summed[j, core]

        @pl.when(i >= 3)
        def _():
            core_arrival(i - 3).wait_recv()

        return carry

    lax.fori_loop(0, chunks + 3, pump, 0)

    def drain(j, carry):
        y_copy(j).wait_send()
        low_copy(j).wait_send()
        high_copy(j).wait_send()
        core_copy(j).wait_send()
        return carry

    lax.fori_loop(0, chunks, drain, 0)
    for copy in pair_copies:
        copy.wait_send()
    for i in range(4):
        vector_copy(i).wait_send()


def reduce_call(wide_left, wide_right, thin_left, thin_first, thin_second, vectors):
    tokens, width = wide_left.shape[1:]
    thin_width = thin_first.shape[2]
    replicas = lax.axis_size("replica")
    rows = width // replicas * 2
    chunks = wide_right.shape[2] // CW + 5
    half = rows // 2
    low = jnp.bfloat16
    vmem = pl.BlockSpec(memory_space=pltpu.VMEM)
    dma = pltpu.SemaphoreType.DMA
    return pl.pallas_call(
        reduce_kernel,
        out_shape=(
            jax.ShapeDtypeStruct((2, chunks, half, CW), jnp.float32),
            jax.ShapeDtypeStruct(vectors.shape, jnp.float32),
        ),
        in_specs=[vmem] * 6,
        out_specs=(vmem, vmem),
        scratch_shapes=[
            pltpu.VMEM(wide_left.shape[1:], low),
            pltpu.VMEM(wide_right.shape[1:], low),
            pltpu.VMEM(thin_left.shape[1:], low),
            pltpu.VMEM(thin_left.shape[1:], low),
            pltpu.VMEM(thin_first.shape[1:], low),
            pltpu.VMEM(thin_second.shape[1:], low),
            pltpu.VMEM((chunks, 2, 2, 2, rows, CW), low),
            pltpu.VMEM((chunks, 2, 2, rows, CW), low),
            pltpu.VMEM((chunks, 2, rows, CW), low),
            pltpu.VMEM((chunks, rows, CW), low),
            pltpu.VMEM((chunks, 2, half, CW), jnp.float32),
            pltpu.VMEM((5,) + vectors.shape, jnp.float32),
            pltpu.VMEM((4,) + vectors.shape, jnp.float32),
            dma((6,)),
            dma((6,)),
            dma((chunks,)),
            dma((chunks,)),
            dma((chunks,)),
            dma((chunks,)),
            dma((chunks,)),
            dma((chunks,)),
            dma((chunks,)),
            dma((chunks,)),
            dma((4,)),
            dma((4,)),
        ],
        compiler_params=pltpu.CompilerParams(
            collective_id=0, has_side_effects=True, vmem_limit_bytes=60 << 20
        ),
        name="reduce_grads",
    )(wide_left, wide_right, thin_left, thin_first, thin_second, vectors)


def by_kernel(replicas, width):
    return replicas == 2**4 and width % (replicas // 2 * 16) == 0


def plain_sums(block_out, tokens_grad, vectors, half, wide, query, key, value, proj, up, down):
    def owned(pair):
        return lax.psum_scatter(product_tn(*pair), "replica", scatter_dimension=0, tiled=True)

    vectors = lax.psum(vectors, "replica")

    def vector_at(i):
        return vectors[i * half : (i + 1) * half]

    return (
        block_out, tokens_grad, vector_at(0), vector_at(1), owned(query), vector_at(6),
        owned(key), owned(value), vector_at(7), owned(proj).T, vector_at(2), vector_at(3),
        vector_at(4), owned(up), vectors[8 * half : 8 * half + wide], owned(down).T, vector_at(5),
    )


def paired(
    tokens, out_grad, picture_ids, live_slots, ln1_gain, ln1_bias, query_weight, query_bias,
    key_weight, value_weight, value_bias, proj_weight, proj_bias, ln2_gain, ln2_bias, up_weight,
    up_bias, down_weight, down_bias,
):
    low = jnp.bfloat16
    full = jnp.float32
    rows, width = tokens.shape
    half = width // 2
    wide = up_weight.shape[1]
    shard = lax.axis_index("shard")
    replicas = lax.axis_size("replica")
    own_vectors = jnp.stack([ln1_gain, ln1_bias, proj_bias, ln2_gain, ln2_bias, down_bias])
    slots = jnp.stack([picture_ids, live_slots])
    peer_tokens, peer_out, peer_vectors, peer_slots = (
        swap(tokens), swap(out_grad), swap(own_vectors), swap(slots),
    )
    gain_one, shift_one, bias_proj, gain_two, shift_two, bias_down = jnp.where(
        shard == 0,
        jnp.concatenate([own_vectors, peer_vectors], axis=1),
        jnp.concatenate([peer_vectors, own_vectors], axis=1),
    ).astype(full)
    slots = jnp.concatenate([slots, peer_slots], axis=1)
    alive = slots[1].astype(full)[:, None]
    ids = slots[0].reshape(2, rows)
    living = slots[1].reshape(2, rows)
    allowed = (ids[:, :, None] == ids[:, None, :]) & (living[:, None, :] == 1)
    all_tokens = jnp.concatenate([tokens, peer_tokens]).astype(full)
    all_out = jnp.concatenate([out_grad, peer_out]) * alive.astype(low)
    xhat_one, inverse_one = norm_stats(all_tokens)
    normed = (xhat_one * gain_one + shift_one).astype(low)
    queries = (product(normed, query_weight) + query_bias.astype(full)).astype(low)
    keys_all = product(normed, key_weight).astype(low)
    values_all = (product(normed, value_weight) + value_bias.astype(full)).astype(low)
    mixed_out, probs = attend(queries, keys_all, values_all, allowed, rows)
    mixed = mixed_out.astype(low)
    partial = product(mixed, proj_weight)
    hidden = all_tokens[:rows] + partial[:rows] + swap(partial[rows:].astype(low)).astype(full) + bias_proj
    xhat_two, inverse_two = norm_stats(hidden)
    normed_own = (xhat_two * gain_two + shift_two).astype(low)
    normed_two = jnp.concatenate([normed_own, swap(normed_own)])
    up_proj = product(normed_two, up_weight) + up_bias.astype(full)
    activated = gelu_tanh(up_proj).astype(low)
    grad_act = product_nt(all_out, down_weight)
    grad_up = jax.vjp(gelu_tanh, up_proj)[1](grad_act)[0].astype(low)
    partial = product_nt(grad_up, up_weight)
    grad_two = partial[:rows] + swap(partial[rows:].astype(low)).astype(full)
    partial = product(activated, down_weight)
    block_out = (
        (hidden + partial[:rows] + swap(partial[rows:].astype(low)).astype(full) + bias_down)
        * alive[:rows]
    ).astype(low)
    grad_hidden = all_out[:rows].astype(full) + norm_grad(xhat_two, inverse_two, gain_two, grad_two)
    hidden_own = grad_hidden.astype(low)
    hidden_low = jnp.concatenate([hidden_own, swap(hidden_own)])
    grad_mixed = product_nt(hidden_low, proj_weight).astype(low)
    grad_queries, grad_keys, grad_values = attend_back(
        queries, keys_all, values_all, grad_mixed, probs, rows
    )
    partial = (
        product_nt(grad_queries, query_weight)
        + product_nt(grad_keys, key_weight)
        + product_nt(grad_values, value_weight)
    )
    grad_one = partial[:rows] + swap(partial[rows:].astype(low)).astype(full)
    tokens_grad = (
        grad_hidden + norm_grad(xhat_one[:rows], inverse_one[:rows], gain_one, grad_one)
    ).astype(low)
    wholes = jnp.stack(
        [
            column_sums(grad_one * xhat_one[:rows]),
            column_sums(grad_one),
            column_sums(hidden_own),
            column_sums(grad_two * xhat_two),
            column_sums(grad_two),
            column_sums(all_out[:rows]),
        ]
    )
    mine = lax.dynamic_slice_in_dim(wholes, shard * half, half, 1)
    theirs = lax.dynamic_slice_in_dim(wholes, (1 - shard) * half, half, 1)
    halves = mine + swap(theirs)
    vectors = jnp.concatenate(
        [
            halves.reshape(-1),
            column_sums(grad_queries),
            column_sums(grad_values),
            column_sums(grad_up),
        ]
    )
    if not by_kernel(replicas, width):
        return plain_sums(
            block_out, tokens_grad, vectors, half, wide,
            (normed, grad_queries), (normed, grad_keys), (normed, grad_values),
            (hidden_low, mixed), (normed_two, grad_up), (all_out, activated),
        )
    lanes = 1024
    size = vectors.shape[0]
    vectors = jnp.pad(vectors, (0, -size % lanes)).reshape(-1, 128)
    wide_pad = -wide % 128
    wide_right = jnp.pad(jnp.stack([grad_up, activated]), ((0, 0), (0, 0), (0, wide_pad)))
    sums, vectors = reduce_call(
        jnp.stack([normed_two, all_out]),
        wide_right,
        jnp.stack([normed, hidden_low]),
        jnp.stack([grad_queries, grad_values]),
        jnp.stack([grad_keys, mixed]),
        vectors,
    )
    vectors = vectors.reshape(-1)
    chunks = sums.shape[1]
    block = sums.shape[2]
    wide_chunks = chunks - 5

    def columns(slot, first, count):
        return [sums[slot, first + i] for i in range(count)]

    rest = [sums[0, chunks - 1], sums[1, chunks - 1]]
    thin_rest = half - 2 * CW
    wide_rest = wide - wide_chunks * CW

    def wide_of(slot):
        return jnp.concatenate(columns(slot, 0, wide_chunks) + [rest[slot][:, :wide_rest]], axis=1)

    def thin_of(slot, place):
        start = CW // 2 + place * thin_rest
        return jnp.concatenate(
            columns(slot, wide_chunks + 2 * place, 2) + [rest[slot][:, start : start + thin_rest]],
            axis=1,
        )

    def vector_at(i):
        return vectors[i * half : (i + 1) * half]

    return (
        block_out,
        tokens_grad,
        vector_at(0),
        vector_at(1),
        thin_of(0, 0),
        vector_at(6),
        thin_of(0, 1),
        thin_of(1, 0),
        vector_at(7),
        thin_of(1, 1).T,
        vector_at(2),
        vector_at(3),
        vector_at(4),
        wide_of(0),
        vectors[8 * half : 8 * half + wide],
        wide_of(1).T,
        vector_at(5),
    )


def solution(mesh):
    in_specs = (
        P(("shard", "replica"), None),
        P(("shard", "replica"), None),
        P(("shard", "replica")),
        P(("shard", "replica")),
        P("shard"),
        P("shard"),
        P(None, "shard"),
        P("shard"),
        P(None, "shard"),
        P(None, "shard"),
        P("shard"),
        P("shard", None),
        P("shard"),
        P("shard"),
        P("shard"),
        P(None, "shard"),
        P("shard"),
        P("shard", None),
        P("shard"),
    )
    out_specs = (
        P(("shard", "replica"), None),
        P(("shard", "replica"), None),
        P("shard"),
        P("shard"),
        P("replica", "shard"),
        P("shard"),
        P("replica", "shard"),
        P("replica", "shard"),
        P("shard"),
        P("shard", "replica"),
        P("shard"),
        P("shard"),
        P("shard"),
        P("replica", "shard"),
        P("shard"),
        P("shard", "replica"),
        P("shard"),
    )
    return jax.shard_map(paired, mesh=mesh, in_specs=in_specs, out_specs=out_specs, check_vma=False)
```

```python
import functools

import jax
import jax.numpy as jnp
from jax import lax
from jax.experimental import pallas as pl
from jax.experimental.pallas import tpu as pltpu
from jax.sharding import PartitionSpec as P

HDIM = 72
norm_eps = 1e-06
MESH = pl.DeviceIdType.MESH
CW = 256
GELU_SCALE = 0.7978845608028654


def norm_stats(values):
    centered = values - jnp.mean(values, axis=-1, keepdims=True)
    variance = jnp.mean(centered * centered, axis=-1, keepdims=True)
    inverse = lax.rsqrt(variance + norm_eps)
    return centered * inverse, inverse


def norm_grad(xhat, inverse, gain, grad):
    scaled = grad * gain
    return (
        scaled
        - jnp.mean(scaled, axis=-1, keepdims=True)
        - xhat * jnp.mean(scaled * xhat, axis=-1, keepdims=True)
    ) * inverse


def gelu_tanh(values):
    return jax.nn.gelu(values, approximate=True)


def product(left_side, right_side):
    return jnp.dot(left_side, right_side, preferred_element_type=jnp.float32)


def product_nt(left_side, right_side):
    return lax.dot_general(
        left_side, right_side, (((1,), (1,)), ((), ())), preferred_element_type=jnp.float32
    )


def product_tn(left_side, right_side):
    return lax.dot_general(
        left_side, right_side, (((0,), (0,)), ((), ())), preferred_element_type=jnp.float32
    )


def column_sums(matrix):
    return jnp.sum(matrix, axis=0, dtype=jnp.float32)


def swap(value):
    return lax.ppermute(value, "shard", [(0, 1), (1, 0)])


def split_heads(matrix, block_rows):
    return matrix.reshape(-1, block_rows, matrix.shape[1] // HDIM, HDIM)


def attend(queries, keys_in, values_in, allowed, block_rows):
    scores = jnp.einsum(
        "bqhd,bkhd->bhqk",
        split_heads(queries, block_rows),
        split_heads(keys_in, block_rows),
        preferred_element_type=jnp.float32,
    ) * HDIM ** (-0.5)
    scores = jnp.where(allowed[:, None, :, :], scores, -1e30)
    highest = jnp.max(scores, axis=-1, keepdims=True)
    scaled_exp = jnp.exp(scores - highest)
    totals = jnp.sum(scaled_exp, axis=-1, keepdims=True)
    probs = scaled_exp / totals
    mixed_out = jnp.einsum(
        "bhqk,bkhd->bqhd",
        probs.astype(jnp.bfloat16),
        split_heads(values_in, block_rows),
        preferred_element_type=jnp.float32,
    )
    return mixed_out.reshape(queries.shape), probs


def attend_back(queries, keys_in, values_in, grad_mixed, probs, block_rows):
    score_scale = HDIM ** (-0.5)
    split_grad = split_heads(grad_mixed, block_rows)
    grad_probs = jnp.einsum(
        "bqhd,bkhd->bhqk",
        split_grad,
        split_heads(values_in, block_rows),
        preferred_element_type=jnp.float32,
    )
    grad_scores = (
        probs * (grad_probs - jnp.sum(probs * grad_probs, axis=-1, keepdims=True))
    ).astype(jnp.bfloat16)
    grad_queries = (
        jnp.einsum(
            "bhqk,bkhd->bqhd",
            grad_scores,
            split_heads(keys_in, block_rows),
            preferred_element_type=jnp.float32,
        )
        * score_scale
    )
    grad_keys = (
        jnp.einsum(
            "bhqk,bqhd->bkhd",
            grad_scores,
            split_heads(queries, block_rows),
            preferred_element_type=jnp.float32,
        )
        * score_scale
    )
    grad_values = jnp.einsum(
        "bhqk,bqhd->bkhd",
        probs.astype(jnp.bfloat16),
        split_grad,
        preferred_element_type=jnp.float32,
    )
    return (
        grad_queries.astype(jnp.bfloat16).reshape(queries.shape),
        grad_keys.astype(jnp.bfloat16).reshape(queries.shape),
        grad_values.astype(jnp.bfloat16).reshape(queries.shape),
    )


def add_low(first, second):
    return (first.astype(jnp.float32) + second.astype(jnp.float32)).astype(jnp.bfloat16)


def by_kernel(replicas, width):
    return replicas == 2**4 and width % (replicas // 2 * 16) == 0


def plain_sums(block_out, tokens_grad, vectors, half, wide, query, key, value, proj, up, down):
    def owned(pair):
        return lax.psum_scatter(product_tn(*pair), "replica", scatter_dimension=0, tiled=True)

    vectors = lax.psum(vectors, "replica")

    def vector_at(i):
        return vectors[i * half : (i + 1) * half]

    return (
        block_out, tokens_grad, vector_at(0), vector_at(1), owned(query), vector_at(6),
        owned(key), owned(value), vector_at(7), owned(proj).T, vector_at(2), vector_at(3),
        vector_at(4), owned(up), vectors[8 * half : 8 * half + wide], owned(down).T, vector_at(5),
    )


def paired(
    tokens, out_grad, picture_ids, live_slots, ln1_gain, ln1_bias, query_weight, query_bias,
    key_weight, value_weight, value_bias, proj_weight, proj_bias, ln2_gain, ln2_bias, up_weight,
    up_bias, down_weight, down_bias,
):
    low = jnp.bfloat16
    full = jnp.float32
    rows, width = tokens.shape
    half = width // 2
    wide = up_weight.shape[1]
    shard = lax.axis_index("shard")
    own_vectors = jnp.stack([ln1_gain, ln1_bias, proj_bias, ln2_gain, ln2_bias, down_bias])
    slots = jnp.stack([picture_ids, live_slots])
    peer_tokens, peer_out, peer_vectors, peer_slots = (
        swap(tokens), swap(out_grad), swap(own_vectors), swap(slots),
    )
    gain_one, shift_one, bias_proj, gain_two, shift_two, bias_down = jnp.where(
        shard == 0,
        jnp.concatenate([own_vectors, peer_vectors], axis=1),
        jnp.concatenate([peer_vectors, own_vectors], axis=1),
    ).astype(full)
    slots = jnp.concatenate([slots, peer_slots], axis=1)
    alive = slots[1].astype(full)[:, None]
    ids = slots[0].reshape(2, rows)
    living = slots[1].reshape(2, rows)
    allowed = (ids[:, :, None] == ids[:, None, :]) & (living[:, None, :] == 1)
    all_tokens = jnp.concatenate([tokens, peer_tokens]).astype(full)
    all_out = jnp.concatenate([out_grad, peer_out]) * alive.astype(low)
    xhat_one, inverse_one = norm_stats(all_tokens)
    normed = (xhat_one * gain_one + shift_one).astype(low)
    queries = (product(normed, query_weight) + query_bias.astype(full)).astype(low)
    keys_all = product(normed, key_weight).astype(low)
    values_all = (product(normed, value_weight) + value_bias.astype(full)).astype(low)
    mixed_out, probs = attend(queries, keys_all, values_all, allowed, rows)
    mixed = mixed_out.astype(low)
    partial = product(mixed, proj_weight)
    hidden = all_tokens[:rows] + partial[:rows] + swap(partial[rows:].astype(low)).astype(full) + bias_proj
    xhat_two, inverse_two = norm_stats(hidden)
    normed_own = (xhat_two * gain_two + shift_two).astype(low)
    normed_two = jnp.concatenate([normed_own, swap(normed_own)])
    up_proj = product(normed_two, up_weight) + up_bias.astype(full)
    activated = gelu_tanh(up_proj).astype(low)
    grad_act = product_nt(all_out, down_weight)
    grad_up = jax.vjp(gelu_tanh, up_proj)[1](grad_act)[0].astype(low)
    partial = product_nt(grad_up, up_weight)
    grad_two = partial[:rows] + swap(partial[rows:].astype(low)).astype(full)
    partial = product(activated, down_weight)
    block_out = (
        (hidden + partial[:rows] + swap(partial[rows:].astype(low)).astype(full) + bias_down)
        * alive[:rows]
    ).astype(low)
    grad_hidden = all_out[:rows].astype(full) + norm_grad(xhat_two, inverse_two, gain_two, grad_two)
    hidden_own = grad_hidden.astype(low)
    hidden_low = jnp.concatenate([hidden_own, swap(hidden_own)])
    grad_mixed = product_nt(hidden_low, proj_weight).astype(low)
    grad_queries, grad_keys, grad_values = attend_back(
        queries, keys_all, values_all, grad_mixed, probs, rows
    )
    partial = (
        product_nt(grad_queries, query_weight)
        + product_nt(grad_keys, key_weight)
        + product_nt(grad_values, value_weight)
    )
    grad_one = partial[:rows] + swap(partial[rows:].astype(low)).astype(full)
    tokens_grad = (
        grad_hidden + norm_grad(xhat_one[:rows], inverse_one[:rows], gain_one, grad_one)
    ).astype(low)
    wholes = jnp.stack(
        [
            column_sums(grad_one * xhat_one[:rows]),
            column_sums(grad_one),
            column_sums(hidden_own),
            column_sums(grad_two * xhat_two),
            column_sums(grad_two),
            column_sums(all_out[:rows]),
        ]
    )
    mine = lax.dynamic_slice_in_dim(wholes, shard * half, half, 1)
    theirs = lax.dynamic_slice_in_dim(wholes, (1 - shard) * half, half, 1)
    halves = mine + swap(theirs)
    vectors = jnp.concatenate(
        [
            halves.reshape(-1),
            column_sums(grad_queries),
            column_sums(grad_values),
            column_sums(grad_up),
        ]
    )
    return plain_sums(
        block_out, tokens_grad, vectors, half, wide,
        (normed, grad_queries), (normed, grad_keys), (normed, grad_values),
        (hidden_low, mixed), (normed_two, grad_up), (all_out, activated),
    )


def take(ref, start, count):
    return ref.at[pl.ds(start, count)]


def layer_kernel(
    tokens,
    out_grad,
    slots,
    vectors,
    up_bias,
    query_hbm,
    key_hbm,
    value_hbm,
    proj_hbm,
    up_hbm,
    down_hbm,
    block_out,
    tokens_grad,
    sums_out,
    vectors_out,
    up_bias_out,
    query_weight,
    key_weight,
    value_weight,
    proj_weight,
    all_tokens,
    out_in,
    all_slots,
    vectors_in,
    queries,
    keys_all,
    values_all,
    probs,
    hidden,
    grad_hidden,
    own_part,
    own_down,
    part_send,
    part_in,
    wide_left,
    wide_right,
    thin_left,
    thin_first,
    thin_second,
    wide_left_in,
    wide_right_in,
    thin_left_in,
    thin_other_in,
    thin_first_in,
    thin_second_in,
    from_y,
    from_low,
    from_high,
    totals,
    halves,
    halves_in,
    vector_sum,
    vector_in,
    up_sum,
    up_in,
    load_sem,
    swap_send,
    swap_recv,
    pair_send,
    pair_recv,
    y_send,
    y_recv,
    low_send,
    low_recv,
    high_send,
    high_recv,
    core_send,
    core_recv,
    keep_sem,
    vec_send,
    vec_recv,
):
    full = jnp.float32
    low = jnp.bfloat16
    chunks = from_y.shape[0]
    rows = from_y.shape[3]
    block, width = tokens.shape
    thin = queries.shape[1]
    wide = up_bias.shape[1]
    heads = thin // HDIM
    score_scale = HDIM ** (-0.5)
    wide_chunks = chunks - 5
    half_block = block // 2
    strip = 32
    shard = lax.axis_index("shard")
    replica = lax.axis_index("replica")
    core = lax.rem(replica, 2)
    other = 1 - core
    y_bit = lax.rem(replica // 2, 2)
    low_bit = lax.rem(replica // 4, 2)
    high_bit = lax.rem(replica // 8, 2)
    twin = (1 - shard, replica)
    partner = (shard, replica + 1 - 2 * core)
    y_peer = (shard, replica + 2 - 4 * y_bit)
    low_peer = (shard, replica + 4 - 8 * low_bit)
    high_peer = (shard, replica + 8 - 16 * high_bit)
    peers = (partner, y_peer, low_peer, high_peer)

    def remote(source, target, send, recv, peer):
        return pltpu.make_async_remote_copy(
            src_ref=source,
            dst_ref=target,
            send_sem=send,
            recv_sem=recv,
            device_id=peer,
            device_id_type=MESH,
        )

    def swapped(index, source, target):
        return remote(source, target, swap_send.at[index], swap_recv.at[index], twin)

    def paired_copy(index, source, target):
        return remote(source, target, pair_send.at[index], pair_recv.at[index], partner)

    loads = [
        pltpu.make_async_copy(source, target, load_sem.at[i])
        for i, (source, target) in enumerate(
            (
                (query_hbm, query_weight),
                (key_hbm, key_weight),
                (value_hbm, value_weight),
                (proj_hbm, proj_weight),
            )
        )
    ]
    for load in loads:
        load.start()

    barrier = pltpu.get_barrier_semaphore()
    for peer in (twin,) + peers:
        pl.semaphore_signal(barrier, inc=1, device_id=peer, device_id_type=MESH)
    pl.semaphore_wait(barrier, 5)

    vectors_swap = swapped(0, vectors, vectors_in)
    slots_swap = swapped(1, slots, all_slots.at[1])
    tokens_swap = swapped(2, tokens, take(all_tokens, block, block))
    out_swap = swapped(3, out_grad, out_in)
    part_swaps = [
        [
            swapped(
                4 + 2 * i + j,
                part_send.at[i, pl.ds(j * half_block, half_block)],
                part_in.at[i, pl.ds(j * half_block, half_block)],
            )
            for j in range(2)
        ]
        for i in range(4)
    ]
    normed_swaps = [
        swapped(
            12 + j,
            wide_left.at[0, pl.ds(j * half_block, half_block)],
            wide_left.at[0, pl.ds(block + j * half_block, half_block)],
        )
        for j in range(2)
    ]
    hidden_swaps = [
        swapped(
            14 + j,
            thin_left.at[1, pl.ds(j * half_block, half_block)],
            thin_left.at[1, pl.ds(block + j * half_block, half_block)],
        )
        for j in range(2)
    ]
    halves_swap = swapped(16, halves.at[1], halves_in)

    def pair_rows(index, source, target, b):
        here = pl.ds(b * block, block)
        return paired_copy(index + b, source.at[here], target.at[here])

    def left_pair(b):
        return pair_rows(0, wide_left.at[other], wide_left_in, b)

    def right_pair(b):
        return pair_rows(2, wide_right.at[other], wide_right_in, b)

    def normed_pair(b):
        return pair_rows(4, thin_left.at[0], thin_left_in, b)

    def other_pair(b):
        return pair_rows(6, thin_left.at[other], thin_other_in, b)

    def first_pair(b):
        return pair_rows(8, thin_first.at[other], thin_first_in, b)

    def second_pair(b):
        return pair_rows(10, thin_second.at[other], thin_second_in, b)

    vectors_swap.start()
    slots_swap.start()
    tokens_swap.start()
    out_swap.start()

    all_slots[0] = slots[...]
    take(all_tokens, 0, block)[...] = tokens[...]
    totals[...] = jnp.zeros_like(totals)
    up_sum[0] = jnp.zeros(up_sum.shape[1:], full)

    vectors_swap.wait_recv()
    slots_swap.wait_recv()
    here_half = vectors[...]
    there_half = vectors_in[...]
    joined = jnp.where(
        shard == 0,
        jnp.concatenate([here_half, there_half], axis=1),
        jnp.concatenate([there_half, here_half], axis=1),
    )
    gain_one, shift_one, bias_proj = joined[0:1], joined[1:2], joined[2:3]
    gain_two, shift_two, bias_down = joined[3:4], joined[4:5], joined[5:6]
    bias_query, bias_value = here_half[6:7], here_half[7:8]

    def strips(count, first, body):
        def step(i, carry):
            body(pl.ds(pl.multiple_of(first + i * strip, strip), strip))
            return carry

        lax.fori_loop(0, count // strip, step, 0, unroll=2)

    def mlp_scope(up_weight, down_weight, grad_act, wide_sem):
        wide_loads = [
            pltpu.make_async_copy(up_hbm, up_weight, wide_sem.at[0]),
            pltpu.make_async_copy(down_hbm, down_weight, wide_sem.at[1]),
        ]
        for load in wide_loads:
            load.start()

        def attend_step(b, carry):
            here = pl.ds(pl.multiple_of(b * block, block), block)

            @pl.when(b == 1)
            def _():
                tokens_swap.wait_recv()

            def norm_strip(at):
                xhat, _ = norm_stats(all_tokens[at, :].astype(full))
                thin_left[0, at, :] = (xhat * gain_one + shift_one).astype(low)

            strips(block, b * block, norm_strip)

            @pl.when(b == 0)
            def _():
                for load in loads:
                    load.wait()

            normed = thin_left[0, here, :]
            queries[here, :] = (product(normed, query_weight[...]) + bias_query).astype(low)
            keys_all[here, :] = product(normed, key_weight[...]).astype(low)
            values_all[here, :] = (product(normed, value_weight[...]) + bias_value).astype(low)
            marks = all_slots[b]
            across = jnp.where(marks[1:2] == 1.0, marks[0:1], -1.0)
            down_ids = jnp.transpose(marks)[:, 0:1]
            allowed = down_ids == across
            q_all = queries[here, :]
            k_all = keys_all[here, :]
            v_all = values_all[here, :]
            for h in range(heads):
                cut = slice(h * HDIM, (h + 1) * HDIM)
                scores = product_nt(q_all[:, cut], k_all[:, cut]) * score_scale
                scores = jnp.where(allowed, scores, -1e30)
                scaled = jnp.exp(scores - jnp.max(scores, axis=-1, keepdims=True))
                share = 1.0 / jnp.sum(scaled, axis=-1, keepdims=True)
                probs_low = (scaled * share).astype(low)
                probs[b * heads + h] = probs_low
                thin_second[1, here, cut] = product(probs_low, v_all[:, cut]).astype(low)
            mixed = thin_second[1, here, :]

            def proj_tile(n, inner):
                at = pl.ds(pl.multiple_of(n * 384, 384), 384)
                value = product(mixed, proj_weight[:, at])

                @pl.when(b == 0)
                def _():
                    own_part[:, at] = value

                @pl.when(b == 1)
                def _():
                    part_send[0, :, at] = value.astype(low)

                return inner

            lax.fori_loop(0, width // 384, proj_tile, 0)
            return carry

        lax.fori_loop(0, 2, attend_step, 0)
        for copy in part_swaps[0]:
            copy.start()
        for b in range(2):
            normed_pair(b).start()

        out_swap.wait_recv()
        for b, source in enumerate((out_grad, out_in)):
            alive = jnp.transpose(all_slots[b])[:, 1:2].astype(low)
            wide_left[1, pl.ds(b * block, block), :] = source[...] * alive
        wide_loads[1].wait()
        out_rows = wide_left[1]

        def act_tile(t, carry):
            at = pl.ds(pl.multiple_of(t * 512, 512), 512)
            grad_act[:, at] = product_nt(out_rows, down_weight[at, :]).astype(low)
            return carry

        lax.fori_loop(0, wide_chunks // 2, act_tile, 0)
        rest_from = wide_chunks * CW
        rest = wide - rest_from
        rest_at = pl.ds(rest_from, rest)
        grad_act[:, rest_at] = product_nt(out_rows, down_weight[rest_at, :]).astype(low)
        wide_loads[0].wait()
        pad_at = pl.ds(rest_from, CW // 2)
        wide_right[0, :, pad_at] = jnp.zeros((2 * block, CW // 2), low)
        wide_right[1, :, pad_at] = jnp.zeros((2 * block, CW // 2), low)

        for j in range(2):
            part_swaps[0][j].wait_recv()

            def hidden_strip(at):
                value = (
                    tokens[at, :].astype(full)
                    + own_part[at, :]
                    + part_in[0, at, :].astype(full)
                    + bias_proj
                )
                hidden[at, :] = value
                xhat, _ = norm_stats(value)
                wide_left[0, at, :] = (xhat * gain_two + shift_two).astype(low)

            strips(half_block, j * half_block, hidden_strip)
            normed_swaps[j].start()

        def mlp_step(b, carry):
            here = pl.ds(pl.multiple_of(b * block, block), block)

            @pl.when(b == 1)
            def _():
                for copy in normed_swaps:
                    copy.wait_recv()

            normed = wide_left[0, here, :]

            def gelu_tile(at):
                value = product(normed, up_weight[:, at]) + up_bias[:, at]
                square = value * value
                bent = jnp.tanh(GELU_SCALE * value * (1.0 + 0.044715 * square))
                bulge = 0.5 * (1.0 + bent)
                wide_right[1, here, at] = (value * bulge).astype(low)
                slope = bulge + 0.5 * value * (1.0 - bent * bent) * (
                    GELU_SCALE * (1.0 + 0.134145 * square)
                )
                grad = (slope * grad_act[here, at].astype(full)).astype(low)
                wide_right[0, here, at] = grad
                up_sum[0, :, at] += jnp.sum(grad.astype(full), axis=0, keepdims=True)

            def up_tile(t, inner):
                gelu_tile(pl.ds(pl.multiple_of(t * CW, CW), CW))
                return inner

            lax.fori_loop(0, wide_chunks, up_tile, 0)
            gelu_tile(rest_at)

            @pl.when(b == 0)
            def _():
                right_pair(0).start()

            @pl.when(b == 1)
            def _():
                left_pair(0).start()
                left_pair(1).start()
                right_pair(1).start()

            grad_rows = wide_right[0, here, pl.ds(0, wide)]

            def back_tile(n, inner):
                at = pl.ds(pl.multiple_of(n * 384, 384), 384)
                value = product_nt(grad_rows, up_weight[at, :])

                @pl.when(b == 0)
                def _():
                    own_part[:, at] = value

                @pl.when(b == 1)
                def _():
                    part_send[1, :, at] = value.astype(low)

                return inner

            lax.fori_loop(0, width // 384, back_tile, 0)

            @pl.when(b == 1)
            def _():
                for copy in part_swaps[1]:
                    copy.start()

            act_rows = wide_right[1, here, pl.ds(0, wide)]

            def down_tile(n, inner):
                at = pl.ds(pl.multiple_of(n * 384, 384), 384)
                value = product(act_rows, down_weight[:, at])

                @pl.when(b == 0)
                def _():
                    own_down[:, at] = value

                @pl.when(b == 1)
                def _():
                    part_send[2, :, at] = value.astype(low)

                return inner

            lax.fori_loop(0, width // 384, down_tile, 0)
            return carry

        lax.fori_loop(0, 2, mlp_step, 0)
        for copy in part_swaps[2]:
            copy.start()

    pl.run_scoped(
        mlp_scope,
        pltpu.VMEM(up_hbm.shape, low),
        pltpu.VMEM(down_hbm.shape, low),
        pltpu.VMEM((2 * block, wide_right.shape[2]), low),
        pltpu.SemaphoreType.DMA((2,)),
    )

    def grad_scope(grads, summed):
        def y_copy(j):
            return remote(
                grads.at[j, :, :, 1 - y_bit], from_y.at[j], y_send.at[j], y_recv.at[j], y_peer
            )

        def low_copy(j):
            return remote(
                grads.at[j, :, 1 - low_bit, y_bit],
                from_low.at[j],
                low_send.at[j],
                low_recv.at[j],
                low_peer,
            )

        def high_copy(j):
            return remote(
                grads.at[j, 1 - high_bit, low_bit, y_bit],
                from_high.at[j],
                high_send.at[j],
                high_recv.at[j],
                high_peer,
            )

        def core_copy(j):
            return remote(
                summed.at[j, other],
                sums_out.at[core, j],
                core_send.at[j],
                core_recv.at[j],
                partner,
            )

        def core_arrival(j):
            return remote(
                summed.at[j, other],
                sums_out.at[other, j],
                core_send.at[j],
                core_recv.at[j],
                partner,
            )

        def keep_copy(j):
            return pltpu.make_async_copy(summed.at[j, core], sums_out.at[core, j], keep_sem.at[j])

        def emit(j, value):
            grads[j] = value.astype(low).reshape(grads.shape[1:])
            y_copy(j).start()

        def pump(i):
            @pl.when(i < chunks)
            def _():
                y_copy(i).wait_recv()
                grads[i, :, :, y_bit] = add_low(grads[i, :, :, y_bit], from_y[i])
                low_copy(i).start()

            @pl.when(jnp.logical_and(i >= 1, i < chunks + 1))
            def _():
                j = i - 1
                low_copy(j).wait_recv()
                grads[j, :, low_bit, y_bit] = add_low(grads[j, :, low_bit, y_bit], from_low[j])
                high_copy(j).start()

            @pl.when(jnp.logical_and(i >= 2, i < chunks + 2))
            def _():
                j = i - 2
                high_copy(j).wait_recv()
                total = grads[j, high_bit, low_bit, y_bit].astype(full) + from_high[j].astype(full)
                summed[j] = total.reshape(2, rows // 2, CW)
                core_copy(j).start()
                keep_copy(j).start()

            @pl.when(i >= 3)
            def _():
                core_arrival(i - 3).wait_recv()
                keep_copy(i - 3).wait()

        def pump_step(i, carry):
            pump(i)
            return carry

        for b in range(2):
            left_pair(b).wait_recv()
            right_pair(b).wait_recv()

        def wide_step(j, carry):
            columns = pl.ds(pl.multiple_of(j * CW, CW), CW)
            emit(
                j,
                product_tn(wide_left[core], wide_right[core, :, columns])
                + product_tn(wide_left_in[...], wide_right_in[:, columns]),
            )
            return carry

        lax.fori_loop(0, wide_chunks, wide_step, 0)

        for j in range(2):
            part_swaps[1][j].wait_recv()

            def norm_back_strip(at):
                grad = own_part[at, :] + part_in[1, at, :].astype(full)
                xhat, inverse = norm_stats(hidden[at, :])
                out_rows = wide_left[1, at, :].astype(full)
                value = out_rows + norm_grad(xhat, inverse, gain_two, grad)
                grad_hidden[at, :] = value
                rounded = value.astype(low)
                thin_left[1, at, :] = rounded
                totals[2:3] += column_sums(rounded.astype(full))[None]
                totals[3:4] += column_sums(grad * xhat)[None]
                totals[4:5] += column_sums(grad)[None]
                totals[5:6] += column_sums(out_rows)[None]

            strips(half_block, j * half_block, norm_back_strip)
            hidden_swaps[j].start()

        def back_step(b, carry):
            here = pl.ds(pl.multiple_of(b * block, block), block)

            @pl.when(b == 1)
            def _():
                for copy in hidden_swaps:
                    copy.wait_recv()
                for i in range(2):
                    other_pair(i).start()

            grad_mixed = product_nt(thin_left[1, here, :], proj_weight[...]).astype(low)
            q_all = queries[here, :]
            k_all = keys_all[here, :]
            v_all = values_all[here, :]
            for h in range(heads):
                cut = slice(h * HDIM, (h + 1) * HDIM)
                probs_low = probs[b * heads + h]
                probs_full = probs_low.astype(full)
                mixed_grad = grad_mixed[:, cut]
                grad_probs = product_nt(mixed_grad, v_all[:, cut])
                weighted = probs_full * grad_probs
                grad_scores = (
                    weighted - probs_full * jnp.sum(weighted, axis=-1, keepdims=True)
                ).astype(low)
                thin_first[0, here, cut] = (product(grad_scores, k_all[:, cut]) * score_scale).astype(low)
                thin_second[0, here, cut] = (
                    product_tn(grad_scores, q_all[:, cut]) * score_scale
                ).astype(low)
                thin_first[1, here, cut] = product_tn(probs_low, mixed_grad).astype(low)

            @pl.when(b == 0)
            def _():
                first_pair(0).start()
                second_pair(0).start()

            @pl.when(b == 1)
            def _():
                first_pair(1).start()
                second_pair(1).start()

            grad_q = thin_first[0, here, :]
            grad_k = thin_second[0, here, :]
            grad_v = thin_first[1, here, :]

            def normed_tile(n, inner):
                at = pl.ds(pl.multiple_of(n * 384, 384), 384)
                value = (
                    product_nt(grad_q, query_weight[at, :])
                    + product_nt(grad_k, key_weight[at, :])
                    + product_nt(grad_v, value_weight[at, :])
                )

                @pl.when(b == 0)
                def _():
                    own_part[:, at] = value

                @pl.when(b == 1)
                def _():
                    part_send[3, :, at] = value.astype(low)

                return inner

            lax.fori_loop(0, width // 384, normed_tile, 0)
            lax.fori_loop(2 * b, 2 * b + 2, pump_step, 0)
            return carry

        lax.fori_loop(0, 2, back_step, 0)
        for copy in part_swaps[3]:
            copy.start()

        for b in range(2):
            for pair in (normed_pair, other_pair, first_pair, second_pair):
                pair(b).wait_recv()

        def first_part(columns):
            return product_tn(thin_left[0], thin_first[core, :, columns]) + product_tn(
                thin_left_in[...], thin_first_in[:, columns]
            )

        def second_part(columns):
            return product_tn(thin_left[core], thin_second[core, :, columns]) + product_tn(
                thin_other_in[...], thin_second_in[:, columns]
            )

        def thin_step(j, carry):
            columns = pl.ds(pl.multiple_of(j * CW, CW), CW)
            emit(wide_chunks + j, first_part(columns))
            emit(wide_chunks + 2 + j, second_part(columns))
            return carry

        lax.fori_loop(0, 2, thin_step, 0)
        thin_rest = pl.ds(2 * CW, thin - 2 * CW)
        wide_rest = pl.ds(wide_chunks * CW, CW // 2)
        emit(
            chunks - 1,
            jnp.concatenate(
                [
                    product_tn(wide_left[core], wide_right[core, :, wide_rest])
                    + product_tn(wide_left_in[...], wide_right_in[:, wide_rest]),
                    first_part(thin_rest),
                    second_part(thin_rest),
                ],
                axis=1,
            ),
        )

        for copy in part_swaps[2]:
            copy.wait_recv()

        def out_strip(at):
            alive = jnp.transpose(all_slots[0])
            value = hidden[at, :] + own_down[at, :] + part_in[2, at, :].astype(full) + bias_down
            block_out[at, :] = value.astype(low)

        strips(block, 0, out_strip)
        alive = jnp.transpose(all_slots[0])[:, 1:2].astype(low)
        block_out[...] = block_out[...] * alive

        for copy in part_swaps[3]:
            copy.wait_recv()

        def final_strip(at):
            grad = own_part[at, :] + part_in[3, at, :].astype(full)
            xhat, inverse = norm_stats(tokens[at, :].astype(full))
            tokens_grad[at, :] = (
                grad_hidden[at, :] + norm_grad(xhat, inverse, gain_one, grad)
            ).astype(low)
            totals[0:1] += column_sums(grad * xhat)[None]
            totals[1:2] += column_sums(grad)[None]

        strips(block, 0, final_strip)
        sums = totals[...]
        lower = sums[:, :thin]
        upper = sums[:, thin:]
        halves[0] = jnp.where(shard == 0, lower, upper)
        halves[1] = jnp.where(shard == 0, upper, lower)
        halves_swap.start()
        grad_query_bias = column_sums(thin_first[0].astype(full))[None]
        grad_value_bias = column_sums(thin_first[1].astype(full))[None]
        halves_swap.wait_recv()
        vector_sum[0] = halves[0] + halves_in[...]
        vector_sum[0, 6:7] = grad_query_bias
        vector_sum[0, 7:8] = grad_value_bias

        def vector_copies(i):
            return (
                remote(
                    vector_sum.at[i], vector_in.at[i], vec_send.at[2 * i], vec_recv.at[2 * i], peers[i]
                ),
                remote(
                    up_sum.at[i], up_in.at[i], vec_send.at[2 * i + 1], vec_recv.at[2 * i + 1], peers[i]
                ),
            )

        def vector_start(i):
            for copy in vector_copies(i):
                copy.start()

        def vector_finish(i):
            for copy in vector_copies(i):
                copy.wait_recv()
            vector_sum[i + 1] = vector_sum[i] + vector_in[i]
            up_sum[i + 1] = up_sum[i] + up_in[i]

        vector_start(0)
        vector_finish(0)
        vector_start(1)

        lax.fori_loop(4, chunks, pump_step, 0)
        vector_finish(1)
        vector_start(2)
        pump(chunks)
        vector_finish(2)
        vector_start(3)
        pump(chunks + 1)
        pump(chunks + 2)
        vector_finish(3)
        vectors_out[...] = vector_sum[4]
        up_bias_out[...] = up_sum[4]

        def drain(j, carry):
            y_copy(j).wait_send()
            low_copy(j).wait_send()
            high_copy(j).wait_send()
            core_copy(j).wait_send()
            return carry

        lax.fori_loop(0, chunks, drain, 0)
        for i in range(4):
            for copy in vector_copies(i):
                copy.wait_send()

    pl.run_scoped(
        grad_scope,
        pltpu.VMEM((chunks, 2, 2, 2, rows, CW), low),
        pltpu.VMEM((chunks, 2, rows // 2, CW), full),
    )
    for copy in [vectors_swap, slots_swap, tokens_swap, out_swap, halves_swap]:
        copy.wait_send()
    for copies in part_swaps + [normed_swaps, hidden_swaps]:
        for copy in copies:
            copy.wait_send()
    for b in range(2):
        for pair in (left_pair, right_pair, normed_pair, other_pair, first_pair, second_pair):
            pair(b).wait_send()


def layer_call(
    tokens, out_grad, slots, vectors, up_bias, query_weight, key_weight, value_weight, proj_weight,
    up_weight, down_weight,
):
    low = jnp.bfloat16
    full = jnp.float32
    block, width = tokens.shape
    thin = query_weight.shape[1]
    wide = up_weight.shape[1]
    wide_pad = wide + -wide % 128
    heads = thin // HDIM
    replicas = lax.axis_size("replica")
    rows = width // replicas * 2
    chunks = wide // CW + 5
    half = rows // 2
    both = 2 * block
    vmem = pl.BlockSpec(memory_space=pltpu.VMEM)
    anywhere = pl.BlockSpec(memory_space=pl.ANY)
    dma = pltpu.SemaphoreType.DMA
    return pl.pallas_call(
        layer_kernel,
        out_shape=(
            jax.ShapeDtypeStruct(tokens.shape, low),
            jax.ShapeDtypeStruct(tokens.shape, low),
            jax.ShapeDtypeStruct((2, chunks, half, CW), full),
            jax.ShapeDtypeStruct(vectors.shape, full),
            jax.ShapeDtypeStruct((1, wide_pad), full),
        ),
        in_specs=[vmem] * 5 + [anywhere] * 6,
        out_specs=(vmem, vmem, anywhere, vmem, vmem),
        scratch_shapes=[
            pltpu.VMEM((width, thin), low),
            pltpu.VMEM((width, thin), low),
            pltpu.VMEM((width, thin), low),
            pltpu.VMEM((thin, width), low),
            pltpu.VMEM((both, width), low),
            pltpu.VMEM((block, width), low),
            pltpu.VMEM((2,) + slots.shape, full),
            pltpu.VMEM(vectors.shape, full),
            pltpu.VMEM((both, thin), low),
            pltpu.VMEM((both, thin), low),
            pltpu.VMEM((both, thin), low),
            pltpu.VMEM((2 * heads, block, block), low),
            pltpu.VMEM((block, width), full),
            pltpu.VMEM((block, width), full),
            pltpu.VMEM((block, width), full),
            pltpu.VMEM((block, width), full),
            pltpu.VMEM((4, block, width), low),
            pltpu.VMEM((4, block, width), low),
            pltpu.VMEM((2, both, width), low),
            pltpu.VMEM((2, both, wide_pad), low),
            pltpu.VMEM((2, both, width), low),
            pltpu.VMEM((2, both, thin), low),
            pltpu.VMEM((2, both, thin), low),
            pltpu.VMEM((both, width), low),
            pltpu.VMEM((both, wide_pad), low),
            pltpu.VMEM((both, width), low),
            pltpu.VMEM((both, width), low),
            pltpu.VMEM((both, thin), low),
            pltpu.VMEM((both, thin), low),
            pltpu.VMEM((chunks, 2, 2, rows, CW), low),
            pltpu.VMEM((chunks, 2, rows, CW), low),
            pltpu.VMEM((chunks, rows, CW), low),
            pltpu.VMEM((8, width), full),
            pltpu.VMEM((2, 8, thin), full),
            pltpu.VMEM((8, thin), full),
            pltpu.VMEM((5, 8, thin), full),
            pltpu.VMEM((4, 8, thin), full),
            pltpu.VMEM((5, 1, wide_pad), full),
            pltpu.VMEM((4, 1, wide_pad), full),
            dma((4,)),
            dma((17,)),
            dma((17,)),
            dma((12,)),
            dma((12,)),
            dma((chunks,)),
            dma((chunks,)),
            dma((chunks,)),
            dma((chunks,)),
            dma((chunks,)),
            dma((chunks,)),
            dma((chunks,)),
            dma((chunks,)),
            dma((chunks,)),
            dma((8,)),
            dma((8,)),
        ],
        compiler_params=pltpu.CompilerParams(
            collective_id=0, has_side_effects=True, vmem_limit_bytes=67043328
        ),
        name="layer",
    )(
        tokens, out_grad, slots, vectors, up_bias, query_weight, key_weight, value_weight,
        proj_weight, up_weight, down_weight,
    )


def whole_layer(
    tokens, out_grad, picture_ids, live_slots, ln1_gain, ln1_bias, query_weight, query_bias,
    key_weight, value_weight, value_bias, proj_weight, proj_bias, ln2_gain, ln2_bias, up_weight,
    up_bias, down_weight, down_bias,
):
    full = jnp.float32
    width = tokens.shape[1]
    if not by_kernel(lax.axis_size("replica"), width):
        return paired(
            tokens, out_grad, picture_ids, live_slots, ln1_gain, ln1_bias, query_weight,
            query_bias, key_weight, value_weight, value_bias, proj_weight, proj_bias, ln2_gain,
            ln2_bias, up_weight, up_bias, down_weight, down_bias,
        )
    half = width // 2
    wide = up_weight.shape[1]
    vectors = jnp.stack(
        [ln1_gain, ln1_bias, proj_bias, ln2_gain, ln2_bias, down_bias, query_bias, value_bias]
    ).astype(full)
    slots = jnp.stack([picture_ids, live_slots] + [live_slots] * 6).astype(full)
    block_out, tokens_grad, sums, vectors, up_bias_grad = layer_call(
        tokens, out_grad, slots, vectors, up_bias.astype(full)[None], query_weight, key_weight,
        value_weight, proj_weight, up_weight, down_weight,
    )
    chunks = sums.shape[1]
    wide_chunks = chunks - 5

    def columns(slot, first, count):
        return [sums[slot, first + i] for i in range(count)]

    rest = [sums[0, chunks - 1], sums[1, chunks - 1]]
    thin_rest = half - 2 * CW
    wide_rest = wide - wide_chunks * CW

    def wide_of(slot):
        return jnp.concatenate(columns(slot, 0, wide_chunks) + [rest[slot][:, :wide_rest]], axis=1)

    def thin_of(slot, place):
        start = CW // 2 + place * thin_rest
        return jnp.concatenate(
            columns(slot, wide_chunks + 2 * place, 2) + [rest[slot][:, start : start + thin_rest]],
            axis=1,
        )

    return (
        block_out,
        tokens_grad,
        vectors[0],
        vectors[1],
        thin_of(0, 0),
        vectors[6],
        thin_of(0, 1),
        thin_of(1, 0),
        vectors[7],
        thin_of(1, 1).T,
        vectors[2],
        vectors[3],
        vectors[4],
        wide_of(0),
        up_bias_grad[0, :wide],
        wide_of(1).T,
        vectors[5],
    )


def solution(mesh):
    in_specs = (
        P(("shard", "replica"), None),
        P(("shard", "replica"), None),
        P(("shard", "replica")),
        P(("shard", "replica")),
        P("shard"),
        P("shard"),
        P(None, "shard"),
        P("shard"),
        P(None, "shard"),
        P(None, "shard"),
        P("shard"),
        P("shard", None),
        P("shard"),
        P("shard"),
        P("shard"),
        P(None, "shard"),
        P("shard"),
        P("shard", None),
        P("shard"),
    )
    out_specs = (
        P(("shard", "replica"), None),
        P(("shard", "replica"), None),
        P("shard"),
        P("shard"),
        P("replica", "shard"),
        P("shard"),
        P("replica", "shard"),
        P("replica", "shard"),
        P("shard"),
        P("shard", "replica"),
        P("shard"),
        P("shard"),
        P("shard"),
        P("replica", "shard"),
        P("shard"),
        P("shard", "replica"),
        P("shard"),
    )
    return jax.shard_map(whole_layer, mesh=mesh, in_specs=in_specs, out_specs=out_specs, check_vma=False)
```

```python
import functools

import jax
import jax.numpy as jnp
from jax import lax
from jax.experimental import pallas as pl
from jax.experimental.pallas import tpu as pltpu
from jax.sharding import PartitionSpec as P

HDIM = 72
norm_eps = 1e-06
MESH = pl.DeviceIdType.MESH
CW = 256
EARLY = 2
AHEAD = 3
GELU_SCALE = 0.7978845608028654


def norm_stats(values):
    centered = values - jnp.mean(values, axis=-1, keepdims=True)
    variance = jnp.mean(centered * centered, axis=-1, keepdims=True)
    inverse = lax.rsqrt(variance + norm_eps)
    return centered * inverse, inverse


def norm_grad(xhat, inverse, gain, grad):
    scaled = grad * gain
    return (
        scaled
        - jnp.mean(scaled, axis=-1, keepdims=True)
        - xhat * jnp.mean(scaled * xhat, axis=-1, keepdims=True)
    ) * inverse


def gelu_tanh(values):
    return jax.nn.gelu(values, approximate=True)


def product(left_side, right_side):
    return jnp.dot(left_side, right_side, preferred_element_type=jnp.float32)


def product_nt(left_side, right_side):
    return lax.dot_general(
        left_side, right_side, (((1,), (1,)), ((), ())), preferred_element_type=jnp.float32
    )


def product_tn(left_side, right_side):
    return lax.dot_general(
        left_side, right_side, (((0,), (0,)), ((), ())), preferred_element_type=jnp.float32
    )


def column_sums(matrix):
    return jnp.sum(matrix, axis=0, dtype=jnp.float32)


def swap(value):
    return lax.ppermute(value, "shard", [(0, 1), (1, 0)])


def split_heads(matrix, block_rows):
    return matrix.reshape(-1, block_rows, matrix.shape[1] // HDIM, HDIM)


def attend(queries, keys_in, values_in, allowed, block_rows):
    scores = jnp.einsum(
        "bqhd,bkhd->bhqk",
        split_heads(queries, block_rows),
        split_heads(keys_in, block_rows),
        preferred_element_type=jnp.float32,
    ) * HDIM ** (-0.5)
    scores = jnp.where(allowed[:, None, :, :], scores, -1e30)
    highest = jnp.max(scores, axis=-1, keepdims=True)
    scaled_exp = jnp.exp(scores - highest)
    totals = jnp.sum(scaled_exp, axis=-1, keepdims=True)
    probs = scaled_exp / totals
    mixed_out = jnp.einsum(
        "bhqk,bkhd->bqhd",
        probs.astype(jnp.bfloat16),
        split_heads(values_in, block_rows),
        preferred_element_type=jnp.float32,
    )
    return mixed_out.reshape(queries.shape), probs


def attend_back(queries, keys_in, values_in, grad_mixed, probs, block_rows):
    score_scale = HDIM ** (-0.5)
    split_grad = split_heads(grad_mixed, block_rows)
    grad_probs = jnp.einsum(
        "bqhd,bkhd->bhqk",
        split_grad,
        split_heads(values_in, block_rows),
        preferred_element_type=jnp.float32,
    )
    grad_scores = (
        probs * (grad_probs - jnp.sum(probs * grad_probs, axis=-1, keepdims=True))
    ).astype(jnp.bfloat16)
    grad_queries = (
        jnp.einsum(
            "bhqk,bkhd->bqhd",
            grad_scores,
            split_heads(keys_in, block_rows),
            preferred_element_type=jnp.float32,
        )
        * score_scale
    )
    grad_keys = (
        jnp.einsum(
            "bhqk,bqhd->bkhd",
            grad_scores,
            split_heads(queries, block_rows),
            preferred_element_type=jnp.float32,
        )
        * score_scale
    )
    grad_values = jnp.einsum(
        "bhqk,bqhd->bkhd",
        probs.astype(jnp.bfloat16),
        split_grad,
        preferred_element_type=jnp.float32,
    )
    return (
        grad_queries.astype(jnp.bfloat16).reshape(queries.shape),
        grad_keys.astype(jnp.bfloat16).reshape(queries.shape),
        grad_values.astype(jnp.bfloat16).reshape(queries.shape),
    )


def add_low(first, second):
    return (first.astype(jnp.float32) + second.astype(jnp.float32)).astype(jnp.bfloat16)


def by_kernel(replicas, width):
    return replicas == 2**4 and width % (replicas // 2 * 16) == 0


def plain_sums(block_out, tokens_grad, vectors, half, wide, query, key, value, proj, up, down):
    def owned(pair):
        return lax.psum_scatter(product_tn(*pair), "replica", scatter_dimension=0, tiled=True)

    vectors = lax.psum(vectors, "replica")

    def vector_at(i):
        return vectors[i * half : (i + 1) * half]

    return (
        block_out, tokens_grad, vector_at(0), vector_at(1), owned(query), vector_at(6),
        owned(key), owned(value), vector_at(7), owned(proj).T, vector_at(2), vector_at(3),
        vector_at(4), owned(up), vectors[8 * half : 8 * half + wide], owned(down).T, vector_at(5),
    )


def paired(
    tokens, out_grad, picture_ids, live_slots, ln1_gain, ln1_bias, query_weight, query_bias,
    key_weight, value_weight, value_bias, proj_weight, proj_bias, ln2_gain, ln2_bias, up_weight,
    up_bias, down_weight, down_bias,
):
    low = jnp.bfloat16
    full = jnp.float32
    rows, width = tokens.shape
    half = width // 2
    wide = up_weight.shape[1]
    shard = lax.axis_index("shard")
    own_vectors = jnp.stack([ln1_gain, ln1_bias, proj_bias, ln2_gain, ln2_bias, down_bias])
    slots = jnp.stack([picture_ids, live_slots])
    peer_tokens, peer_out, peer_vectors, peer_slots = (
        swap(tokens), swap(out_grad), swap(own_vectors), swap(slots),
    )
    gain_one, shift_one, bias_proj, gain_two, shift_two, bias_down = jnp.where(
        shard == 0,
        jnp.concatenate([own_vectors, peer_vectors], axis=1),
        jnp.concatenate([peer_vectors, own_vectors], axis=1),
    ).astype(full)
    slots = jnp.concatenate([slots, peer_slots], axis=1)
    alive = slots[1].astype(full)[:, None]
    ids = slots[0].reshape(2, rows)
    living = slots[1].reshape(2, rows)
    allowed = (ids[:, :, None] == ids[:, None, :]) & (living[:, None, :] == 1)
    all_tokens = jnp.concatenate([tokens, peer_tokens]).astype(full)
    all_out = jnp.concatenate([out_grad, peer_out]) * alive.astype(low)
    xhat_one, inverse_one = norm_stats(all_tokens)
    normed = (xhat_one * gain_one + shift_one).astype(low)
    queries = (product(normed, query_weight) + query_bias.astype(full)).astype(low)
    keys_all = product(normed, key_weight).astype(low)
    values_all = (product(normed, value_weight) + value_bias.astype(full)).astype(low)
    mixed_out, probs = attend(queries, keys_all, values_all, allowed, rows)
    mixed = mixed_out.astype(low)
    partial = product(mixed, proj_weight)
    hidden = all_tokens[:rows] + partial[:rows] + swap(partial[rows:].astype(low)).astype(full) + bias_proj
    xhat_two, inverse_two = norm_stats(hidden)
    normed_own = (xhat_two * gain_two + shift_two).astype(low)
    normed_two = jnp.concatenate([normed_own, swap(normed_own)])
    up_proj = product(normed_two, up_weight) + up_bias.astype(full)
    activated = gelu_tanh(up_proj).astype(low)
    grad_act = product_nt(all_out, down_weight)
    grad_up = jax.vjp(gelu_tanh, up_proj)[1](grad_act)[0].astype(low)
    partial = product_nt(grad_up, up_weight)
    grad_two = partial[:rows] + swap(partial[rows:].astype(low)).astype(full)
    partial = product(activated, down_weight)
    block_out = (
        (hidden + partial[:rows] + swap(partial[rows:].astype(low)).astype(full) + bias_down)
        * alive[:rows]
    ).astype(low)
    grad_hidden = all_out[:rows].astype(full) + norm_grad(xhat_two, inverse_two, gain_two, grad_two)
    hidden_own = grad_hidden.astype(low)
    hidden_low = jnp.concatenate([hidden_own, swap(hidden_own)])
    grad_mixed = product_nt(hidden_low, proj_weight).astype(low)
    grad_queries, grad_keys, grad_values = attend_back(
        queries, keys_all, values_all, grad_mixed, probs, rows
    )
    partial = (
        product_nt(grad_queries, query_weight)
        + product_nt(grad_keys, key_weight)
        + product_nt(grad_values, value_weight)
    )
    grad_one = partial[:rows] + swap(partial[rows:].astype(low)).astype(full)
    tokens_grad = (
        grad_hidden + norm_grad(xhat_one[:rows], inverse_one[:rows], gain_one, grad_one)
    ).astype(low)
    wholes = jnp.stack(
        [
            column_sums(grad_one * xhat_one[:rows]),
            column_sums(grad_one),
            column_sums(hidden_own),
            column_sums(grad_two * xhat_two),
            column_sums(grad_two),
            column_sums(all_out[:rows]),
        ]
    )
    mine = lax.dynamic_slice_in_dim(wholes, shard * half, half, 1)
    theirs = lax.dynamic_slice_in_dim(wholes, (1 - shard) * half, half, 1)
    halves = mine + swap(theirs)
    vectors = jnp.concatenate(
        [
            halves.reshape(-1),
            column_sums(grad_queries),
            column_sums(grad_values),
            column_sums(grad_up),
        ]
    )
    return plain_sums(
        block_out, tokens_grad, vectors, half, wide,
        (normed, grad_queries), (normed, grad_keys), (normed, grad_values),
        (hidden_low, mixed), (normed_two, grad_up), (all_out, activated),
    )


def take(ref, start, count):
    return ref.at[pl.ds(start, count)]


def layer_kernel(
    tokens_hbm,
    out_hbm,
    picture_ids,
    live_slots,
    ln1_gain,
    ln1_bias,
    proj_bias,
    ln2_gain,
    ln2_bias,
    down_bias,
    query_bias,
    value_bias,
    up_bias_in,
    query_hbm,
    key_hbm,
    value_hbm,
    proj_hbm,
    up_hbm,
    down_hbm,
    rows_out,
    wide_out,
    thin_out,
    vectors_out,
    up_bias_out,
    slots,
    vectors,
    up_bias,
    query_weight,
    key_weight,
    value_weight,
    proj_weight,
    all_tokens,
    all_slots,
    vectors_in,
    queries,
    keys_all,
    values_all,
    probs,
    hidden,
    grad_hidden,
    own_part,
    own_down,
    part_send,
    part_in,
    wide_left,
    wide_right,
    thin_left,
    thin_first,
    thin_second,
    wide_left_in,
    wide_right_in,
    thin_left_in,
    thin_other_in,
    thin_first_in,
    thin_second_in,
    early,
    from_first,
    from_second,
    from_high,
    rest_in,
    totals,
    halves,
    halves_in,
    vector_sum,
    vector_in,
    up_sum,
    up_in,
    flat_0,
    flat_1,
    flat_2,
    flat_3,
    flat_4,
    flat_5,
    flat_6,
    flat_7,
    flat_slots_0,
    flat_slots_1,
    flat_up,
    small_sem,
    load_sem,
    swap_send,
    swap_recv,
    pair_send,
    pair_recv,
    first_send,
    first_recv,
    second_send,
    second_recv,
    high_send,
    high_recv,
    core_send,
    core_recv,
    vec_send,
    vec_recv,
):
    full = jnp.float32
    low = jnp.bfloat16
    chunks = from_first.shape[0]
    rows = from_first.shape[3]
    early_chunks = early.shape[0]
    block, width = tokens_hbm.shape
    thin = queries.shape[1]
    wide = up_bias.shape[1]
    heads = thin // HDIM
    score_scale = HDIM ** (-0.5)
    wide_chunks = chunks - 5
    half_block = block // 2
    strip = 32
    shard = lax.axis_index("shard")
    replica = lax.axis_index("replica")
    core = lax.rem(replica, 2)
    other = 1 - core
    y_bit = lax.rem(replica // 2, 2)
    low_bit = lax.rem(replica // 4, 2)
    high_bit = lax.rem(replica // 8, 2)
    twin = (1 - shard, replica)
    partner = (shard, replica + 1 - 2 * core)
    y_peer = (shard, replica + 2 - 4 * y_bit)
    low_peer = (shard, replica + 4 - 8 * low_bit)
    high_peer = (shard, replica + 8 - 16 * high_bit)
    peers = (partner, y_peer, low_peer, high_peer)

    def remote(source, target, send, recv, peer):
        return pltpu.make_async_remote_copy(
            src_ref=source,
            dst_ref=target,
            send_sem=send,
            recv_sem=recv,
            device_id=peer,
            device_id_type=MESH,
        )

    def swapped(index, source, target):
        return remote(source, target, swap_send.at[index], swap_recv.at[index], twin)

    def paired_copy(index, source, target):
        return remote(source, target, pair_send.at[index], pair_recv.at[index], partner)

    loads = [
        pltpu.make_async_copy(source, target, load_sem.at[i])
        for i, (source, target) in enumerate(
            (
                (query_hbm, query_weight),
                (key_hbm, key_weight),
                (value_hbm, value_weight),
                (proj_hbm, proj_weight),
                (tokens_hbm, take(all_tokens, 0, block)),
                (out_hbm, wide_left.at[1, pl.ds(0, block)]),
            )
        )
    ]
    barrier = pltpu.get_barrier_semaphore()
    for peer in (twin,) + peers:
        pl.semaphore_signal(barrier, inc=1, device_id=peer, device_id_type=MESH)
    small = [
        pltpu.make_async_copy(source, target, small_sem.at[i])
        for i, (source, target) in enumerate(
            (
                (ln1_gain, flat_0),
                (ln1_bias, flat_1),
                (proj_bias, flat_2),
                (ln2_gain, flat_3),
                (ln2_bias, flat_4),
                (down_bias, flat_5),
                (query_bias, flat_6),
                (value_bias, flat_7),
                (picture_ids, flat_slots_0),
                (live_slots, flat_slots_1),
                (up_bias_in, flat_up),
            )
        )
    ]
    for load in small + loads[4:] + loads[:4]:
        load.start()
    slots[...] = jnp.zeros_like(slots)
    for load in small:
        load.wait()
    named = (flat_0, flat_1, flat_2, flat_3, flat_4, flat_5, flat_6, flat_7)
    for i, value in enumerate(named):
        vectors[i : i + 1, :] = value[...].astype(full).reshape(1, thin)
    slots[0:1, :] = flat_slots_0[...].astype(full).reshape(1, block)
    slots[1:2, :] = flat_slots_1[...].astype(full).reshape(1, block)
    up_bias[0:1, :] = flat_up[...].astype(full).reshape(1, wide)
    pl.semaphore_wait(barrier, 5)

    vectors_swap = swapped(0, vectors, vectors_in)
    slots_swap = swapped(1, slots, all_slots.at[1])
    tokens_swap = swapped(2, tokens_hbm, take(all_tokens, block, block))
    out_swap = swapped(3, out_hbm, wide_left.at[1, pl.ds(block, block)])
    part_swaps = [
        [
            swapped(
                4 + 2 * i + j,
                part_send.at[i, pl.ds(j * half_block, half_block)],
                part_in.at[i, pl.ds(j * half_block, half_block)],
            )
            for j in range(2)
        ]
        for i in range(4)
    ]
    normed_swaps = [
        swapped(
            12 + j,
            wide_left.at[0, pl.ds(j * half_block, half_block)],
            wide_left.at[0, pl.ds(block + j * half_block, half_block)],
        )
        for j in range(2)
    ]
    hidden_swaps = [
        swapped(
            14 + j,
            thin_left.at[1, pl.ds(j * half_block, half_block)],
            thin_left.at[1, pl.ds(block + j * half_block, half_block)],
        )
        for j in range(2)
    ]
    halves_swap = swapped(16, halves.at[1], halves_in)

    def pair_rows(index, source, target, b):
        here = pl.ds(b * block, block)
        return paired_copy(index + b, source.at[here], target.at[here])

    def left_pair(b):
        return pair_rows(0, wide_left.at[other], wide_left_in, b)

    def right_pair(b):
        return pair_rows(2, wide_right.at[other], wide_right_in, b)

    def normed_pair(b):
        return pair_rows(4, thin_left.at[0], thin_left_in, b)

    def other_pair(b):
        return pair_rows(6, thin_left.at[other], thin_other_in, b)

    def first_pair(b):
        return pair_rows(8, thin_first.at[other], thin_first_in, b)

    def second_pair(b):
        return pair_rows(10, thin_second.at[other], thin_second_in, b)

    vectors_swap.start()
    slots_swap.start()
    tokens_swap.start()
    out_swap.start()

    all_slots[0] = slots[...]
    for load in loads[4:]:
        load.wait()
    totals[...] = jnp.zeros_like(totals)
    up_sum[0] = jnp.zeros(up_sum.shape[1:], full)

    vectors_swap.wait_recv()
    slots_swap.wait_recv()
    here_half = vectors[...]
    there_half = vectors_in[...]
    joined = jnp.where(
        shard == 0,
        jnp.concatenate([here_half, there_half], axis=1),
        jnp.concatenate([there_half, here_half], axis=1),
    )
    gain_one, shift_one, bias_proj = joined[0:1], joined[1:2], joined[2:3]
    gain_two, shift_two, bias_down = joined[3:4], joined[4:5], joined[5:6]
    bias_query, bias_value = here_half[6:7], here_half[7:8]

    def strips(count, first, body):
        def step(i, carry):
            body(pl.ds(pl.multiple_of(first + i * strip, strip), strip))
            return carry

        lax.fori_loop(0, count // strip, step, 0, unroll=2)

    def is_low_first(j):
        return lax.rem(j, 4) == 1

    def first_pick(grads, k, low_first):
        if low_first:
            return grads.at[k, :, 1 - low_bit], low_peer
        return grads.at[k, :, :, 1 - y_bit], y_peer

    def second_pick(grads, k, low_first):
        if low_first:
            return grads.at[k, :, low_bit, 1 - y_bit], y_peer
        return grads.at[k, :, 1 - low_bit, y_bit], low_peer

    def first_copy(grads, k, j, low_first):
        source, peer = first_pick(grads, k, low_first)
        return remote(source, from_first.at[j], first_send.at[j], first_recv.at[j], peer)

    def second_copy(grads, k, j, low_first):
        source, peer = second_pick(grads, k, low_first)
        return remote(source, from_second.at[j], second_send.at[j], second_recv.at[j], peer)

    def high_copy(grads, k, j):
        return remote(
            grads.at[k, 1 - high_bit, low_bit, y_bit],
            from_high.at[j],
            high_send.at[j],
            high_recv.at[j],
            high_peer,
        )

    def by_order(j, action):
        low_first = is_low_first(j)

        @pl.when(low_first)
        def _():
            action(True)

        @pl.when(jnp.logical_not(low_first))
        def _():
            action(False)

    def issue(grads, k, j):
        by_order(j, lambda low_first: first_copy(grads, k, j, low_first).start())

    def emit(grads, k, j, value, ahead):
        grads[k] = value.astype(low).reshape(grads.shape[1:])

        @pl.when(j < ahead)
        def _():
            issue(grads, k, j)

    def take_first(grads, k, j):
        def action(low_first):
            first_copy(grads, k, j, low_first).wait_recv()
            if low_first:
                grads[k, :, low_bit] = add_low(grads[k, :, low_bit], from_first[j])
            else:
                grads[k, :, :, y_bit] = add_low(grads[k, :, :, y_bit], from_first[j])
            second_copy(grads, k, j, low_first).start()

        by_order(j, action)

    def take_second(grads, k, j):
        by_order(j, lambda low_first: second_copy(grads, k, j, low_first).wait_recv())
        grads[k, :, low_bit, y_bit] = add_low(grads[k, :, low_bit, y_bit], from_second[j])
        high_copy(grads, k, j).start()

    def rest_copy(summed, j):
        return remote(summed.at[j, other], rest_in, core_send.at[j], core_recv.at[j], partner)

    def wide_place(slot, j):
        return wide_out.at[slot, :, pl.ds(pl.multiple_of(j * CW, CW), CW)]

    def thin_place(slot, j):
        at = (j - wide_chunks) // 2
        return thin_out.at[
            slot, lax.rem(j - wide_chunks, 2), :, pl.ds(pl.multiple_of(at * CW, CW), CW)
        ]

    def core_copy(summed, j, place):
        return remote(
            summed.at[j, other], place(core, j), core_send.at[j], core_recv.at[j], partner
        )

    def take_high(grads, k, j, summed):
        high_copy(grads, k, j).wait_recv()
        total = grads[k, high_bit, low_bit, y_bit].astype(full) + from_high[j].astype(full)
        summed[j] = total.reshape(2, rows // 2, CW)

        @pl.when(j < wide_chunks)
        def _():
            core_copy(summed, j, wide_place).start()
            wide_place(core, j)[...] = summed[j, core]

        @pl.when(jnp.logical_and(j >= wide_chunks, j < chunks - 1))
        def _():
            core_copy(summed, j, thin_place).start()
            thin_place(core, j)[...] = summed[j, core]

        @pl.when(j == chunks - 1)
        def _():
            rest_copy(summed, j).start()

    def wide_value(j):
        columns = pl.ds(pl.multiple_of(j * CW, CW), CW)
        return product_tn(wide_left[core], wide_right[core, :, columns]) + product_tn(
            wide_left_in[...], wide_right_in[:, columns]
        )

    def mlp_scope(up_weight, down_weight, grad_act, wide_sem):
        wide_loads = [
            pltpu.make_async_copy(up_hbm, up_weight, wide_sem.at[0]),
            pltpu.make_async_copy(down_hbm, down_weight, wide_sem.at[1]),
        ]
        for load in wide_loads:
            load.start()

        def attend_step(b, carry):
            here = pl.ds(pl.multiple_of(b * block, block), block)

            @pl.when(b == 1)
            def _():
                tokens_swap.wait_recv()

            def norm_strip(at):
                xhat, _ = norm_stats(all_tokens[at, :].astype(full))
                thin_left[0, at, :] = (xhat * gain_one + shift_one).astype(low)

            strips(block, b * block, norm_strip)

            @pl.when(b == 0)
            def _():
                for load in loads[:4]:
                    load.wait()

            normed = thin_left[0, here, :]
            queries[here, :] = (product_nt(normed, query_weight[...]) + bias_query).astype(low)
            keys_all[here, :] = product_nt(normed, key_weight[...]).astype(low)
            values_all[here, :] = (product_nt(normed, value_weight[...]) + bias_value).astype(low)
            marks = all_slots[b]
            across = jnp.where(marks[1:2] == 1.0, marks[0:1], -1.0)
            down_ids = jnp.transpose(marks)[:, 0:1]
            allowed = down_ids == across
            q_all = queries[here, :]
            k_all = keys_all[here, :]
            v_all = values_all[here, :]
            for h in range(heads):
                cut = slice(h * HDIM, (h + 1) * HDIM)
                scores = product_nt(q_all[:, cut], k_all[:, cut]) * score_scale
                scores = jnp.where(allowed, scores, -1e30)
                scaled = jnp.exp(scores - jnp.max(scores, axis=-1, keepdims=True))
                share = 1.0 / jnp.sum(scaled, axis=-1, keepdims=True)
                probs_low = (scaled * share).astype(low)
                probs[b * heads + h] = probs_low
                thin_second[1, here, cut] = product(probs_low, v_all[:, cut]).astype(low)
            mixed = thin_second[1, here, :]

            def proj_tile(n, inner):
                at = pl.ds(pl.multiple_of(n * 384, 384), 384)
                value = product(mixed, proj_weight[:, at])

                @pl.when(b == 0)
                def _():
                    own_part[:, at] = value

                @pl.when(b == 1)
                def _():
                    part_send[0, :, at] = value.astype(low)

                return inner

            lax.fori_loop(0, width // 384, proj_tile, 0)
            return carry

        lax.fori_loop(0, 2, attend_step, 0)
        for copy in part_swaps[0]:
            copy.start()
        for b in range(2):
            normed_pair(b).start()

        out_swap.wait_recv()
        for b in range(2):
            alive = jnp.transpose(all_slots[b])[:, 1:2].astype(low)
            whole = pl.ds(b * block, block)
            wide_left[1, whole, :] = wide_left[1, whole, :] * alive
        wide_loads[1].wait()
        out_rows = wide_left[1]

        def act_tile(t, carry):
            at = pl.ds(pl.multiple_of(t * 512, 512), 512)
            grad_act[:, at] = product_nt(out_rows, down_weight[at, :]).astype(low)
            return carry

        lax.fori_loop(0, wide_chunks // 2, act_tile, 0)
        rest_from = wide_chunks * CW
        rest = wide - rest_from
        rest_at = pl.ds(rest_from, rest)
        grad_act[:, rest_at] = product_nt(out_rows, down_weight[rest_at, :]).astype(low)
        wide_loads[0].wait()
        pad_at = pl.ds(rest_from, CW // 2)
        wide_right[0, :, pad_at] = jnp.zeros((2 * block, CW // 2), low)
        wide_right[1, :, pad_at] = jnp.zeros((2 * block, CW // 2), low)

        for j in range(2):
            part_swaps[0][j].wait_recv()

            def hidden_strip(at):
                value = (
                    all_tokens[at, :].astype(full)
                    + own_part[at, :]
                    + part_in[0, at, :].astype(full)
                    + bias_proj
                )
                hidden[at, :] = value
                xhat, _ = norm_stats(value)
                wide_left[0, at, :] = (xhat * gain_two + shift_two).astype(low)

            strips(half_block, j * half_block, hidden_strip)
            normed_swaps[j].start()

        def mlp_step(b, carry):
            here = pl.ds(pl.multiple_of(b * block, block), block)

            @pl.when(b == 1)
            def _():
                for copy in normed_swaps:
                    copy.wait_recv()

            normed = wide_left[0, here, :]

            def gelu_tile(at):
                value = product_nt(normed, up_weight[at, :]) + up_bias[0:1, at]
                square = value * value
                bent = jnp.tanh(GELU_SCALE * value * (1.0 + 0.044715 * square))
                bulge = 0.5 * (1.0 + bent)
                wide_right[1, here, at] = (value * bulge).astype(low)
                slope = bulge + 0.5 * value * (1.0 - bent * bent) * (
                    GELU_SCALE * (1.0 + 0.134145 * square)
                )
                grad = (slope * grad_act[here, at].astype(full)).astype(low)
                wide_right[0, here, at] = grad
                up_sum[0, :, at] += jnp.sum(grad.astype(full), axis=0, keepdims=True)

            def up_tile(t, inner):
                gelu_tile(pl.ds(pl.multiple_of(t * CW, CW), CW))
                return inner

            lax.fori_loop(0, wide_chunks, up_tile, 0)
            gelu_tile(rest_at)

            @pl.when(b == 0)
            def _():
                right_pair(0).start()

            @pl.when(b == 1)
            def _():
                left_pair(0).start()
                left_pair(1).start()
                right_pair(1).start()

            @pl.when(b == 1)
            def _():
                for i in range(2):
                    left_pair(i).wait_recv()
                    right_pair(i).wait_recv()

                def early_step(j, inner):
                    emit(early, j, j, wide_value(j), AHEAD)
                    return inner

                lax.fori_loop(0, early_chunks, early_step, 0)

            grad_rows = wide_right[0, here, pl.ds(0, wide)]

            def back_tile(n, inner):
                at = pl.ds(pl.multiple_of(n * 384, 384), 384)
                value = product(grad_rows, up_weight[:, at])

                @pl.when(b == 0)
                def _():
                    own_part[:, at] = value

                @pl.when(b == 1)
                def _():
                    part_send[1, :, at] = value.astype(low)

                return inner

            lax.fori_loop(0, width // 384, back_tile, 0)

            @pl.when(b == 1)
            def _():
                for copy in part_swaps[1]:
                    copy.start()

            act_rows = wide_right[1, here, pl.ds(0, wide)]

            def down_tile(n, inner):
                at = pl.ds(pl.multiple_of(n * 384, 384), 384)
                value = product(act_rows, down_weight[:, at])

                @pl.when(b == 0)
                def _():
                    own_down[:, at] = value

                @pl.when(b == 1)
                def _():
                    part_send[2, :, at] = value.astype(low)

                return inner

            lax.fori_loop(0, width // 384, down_tile, 0)
            return carry

        lax.fori_loop(0, 2, mlp_step, 0)

    pl.run_scoped(
        mlp_scope,
        pltpu.VMEM(up_hbm.shape, low),
        pltpu.VMEM(down_hbm.shape, low),
        pltpu.VMEM((2 * block, wide_right.shape[2]), low),
        pltpu.SemaphoreType.DMA((2,)),
    )

    def grad_scope(grads, summed):
        def held(j, action):
            @pl.when(j < early_chunks)
            def _():
                action(early, j, j)

            @pl.when(j >= early_chunks)
            def _():
                action(grads, j - early_chunks, j)

        def pump_step(i, carry):
            @pl.when(i >= 6)
            def _():
                rest_copy(summed, i - 6).wait_recv()

            @pl.when(jnp.logical_and(i >= 4, i < chunks + 4))
            def _():
                held(i - 4, lambda ref, k, j: take_high(ref, k, j, summed))

            @pl.when(jnp.logical_and(i >= 2, i < chunks + 2))
            def _():
                held(i - 2, take_second)

            @pl.when(i < chunks)
            def _():
                held(i, take_first)

            return carry

        def pump(first, last, made=wide_chunks):
            def step(i, carry):
                pump_step(i, carry)

                @pl.when(i + AHEAD < made)
                def _():
                    issue(grads, i + AHEAD - early_chunks, i + AHEAD)

                return carry

            lax.fori_loop(first, last, step, 0)

        def emit_late(j, value, ahead):
            emit(grads, j - early_chunks, j, value, ahead)

        def wide_step(j, carry):
            emit_late(j, wide_value(j), AHEAD)
            return carry

        lax.fori_loop(early_chunks, wide_chunks, wide_step, 0)
        pump(0, 2)

        for j in range(2):
            part_swaps[1][j].wait_recv()

            def norm_back_strip(at):
                grad = own_part[at, :] + part_in[1, at, :].astype(full)
                xhat, inverse = norm_stats(hidden[at, :])
                out_rows = wide_left[1, at, :].astype(full)
                value = out_rows + norm_grad(xhat, inverse, gain_two, grad)
                grad_hidden[at, :] = value
                rounded = value.astype(low)
                thin_left[1, at, :] = rounded
                totals[2:3] += column_sums(rounded.astype(full))[None]
                totals[3:4] += column_sums(grad * xhat)[None]
                totals[4:5] += column_sums(grad)[None]
                totals[5:6] += column_sums(out_rows)[None]

            strips(half_block, j * half_block, norm_back_strip)
            hidden_swaps[j].start()
        for copy in part_swaps[2]:
            copy.start()

        pump(2, 3)

        def back_step(b, carry):
            here = pl.ds(pl.multiple_of(b * block, block), block)

            @pl.when(b == 1)
            def _():
                for copy in hidden_swaps:
                    copy.wait_recv()
                for i in range(2):
                    other_pair(i).start()

            grad_mixed = product_nt(thin_left[1, here, :], proj_weight[...]).astype(low)
            q_all = queries[here, :]
            k_all = keys_all[here, :]
            v_all = values_all[here, :]
            for h in range(heads):
                cut = slice(h * HDIM, (h + 1) * HDIM)
                probs_low = probs[b * heads + h]
                probs_full = probs_low.astype(full)
                mixed_grad = grad_mixed[:, cut]
                grad_probs = product_nt(mixed_grad, v_all[:, cut])
                weighted = probs_full * grad_probs
                grad_scores = (
                    weighted - probs_full * jnp.sum(weighted, axis=-1, keepdims=True)
                ).astype(low)
                thin_first[0, here, cut] = (product(grad_scores, k_all[:, cut]) * score_scale).astype(low)
                thin_second[0, here, cut] = (
                    product_tn(grad_scores, q_all[:, cut]) * score_scale
                ).astype(low)
                thin_first[1, here, cut] = product_tn(probs_low, mixed_grad).astype(low)

            @pl.when(b == 0)
            def _():
                first_pair(0).start()
                second_pair(0).start()

            @pl.when(b == 1)
            def _():
                first_pair(1).start()
                second_pair(1).start()

            grad_q = thin_first[0, here, :]
            grad_k = thin_second[0, here, :]
            grad_v = thin_first[1, here, :]

            def normed_tile(n, inner):
                at = pl.ds(pl.multiple_of(n * 384, 384), 384)
                value = (
                    product(grad_q, query_weight[:, at])
                    + product(grad_k, key_weight[:, at])
                    + product(grad_v, value_weight[:, at])
                )

                @pl.when(b == 0)
                def _():
                    own_part[:, at] = value

                @pl.when(b == 1)
                def _():
                    part_send[3, :, at] = value.astype(low)

                return inner

            lax.fori_loop(0, width // 384, normed_tile, 0)
            pump(3 + 2 * b, 5 + 2 * b)
            return carry

        lax.fori_loop(0, 2, back_step, 0)
        for copy in part_swaps[3]:
            copy.start()

        for b in range(2):
            for pair in (normed_pair, other_pair, first_pair, second_pair):
                pair(b).wait_recv()

        def first_part(columns):
            return product_tn(thin_left[0], thin_first[core, :, columns]) + product_tn(
                thin_left_in[...], thin_first_in[:, columns]
            )

        def second_part(columns):
            return product_tn(thin_left[core], thin_second[core, :, columns]) + product_tn(
                thin_other_in[...], thin_second_in[:, columns]
            )

        def thin_step(j, carry):
            columns = pl.ds(pl.multiple_of(j * CW, CW), CW)
            emit_late(wide_chunks + 2 * j, first_part(columns), 7 + AHEAD)
            emit_late(wide_chunks + 2 * j + 1, second_part(columns), 7 + AHEAD)
            return carry

        lax.fori_loop(0, 2, thin_step, 0)
        thin_rest = pl.ds(2 * CW, thin - 2 * CW)
        wide_rest = pl.ds(wide_chunks * CW, CW // 2)
        rest = wide - wide_chunks * CW
        rest_columns = pl.ds(wide_chunks * CW, rest)
        emit_late(
            chunks - 1,
            jnp.concatenate(
                [
                    product_tn(wide_left[core], wide_right[core, :, wide_rest])
                    + product_tn(wide_left_in[...], wide_right_in[:, wide_rest]),
                    first_part(thin_rest),
                    second_part(thin_rest),
                ],
                axis=1,
            ),
            7 + AHEAD,
        )
        pump(7, 10, chunks)

        for copy in part_swaps[3]:
            copy.wait_recv()

        def final_strip(at):
            grad = own_part[at, :] + part_in[3, at, :].astype(full)
            xhat, inverse = norm_stats(all_tokens[at, :].astype(full))
            rows_out[1, at, :] = (
                grad_hidden[at, :] + norm_grad(xhat, inverse, gain_one, grad)
            ).astype(low)
            totals[0:1] += column_sums(grad * xhat)[None]
            totals[1:2] += column_sums(grad)[None]

        strips(block, 0, final_strip)
        sums = totals[...]
        lower = sums[:, :thin]
        upper = sums[:, thin:]
        halves[0] = jnp.where(shard == 0, lower, upper)
        halves[1] = jnp.where(shard == 0, upper, lower)
        halves_swap.start()
        pump(10, 12, chunks)
        grad_query_bias = column_sums(thin_first[0].astype(full))[None]
        grad_value_bias = column_sums(thin_first[1].astype(full))[None]
        halves_swap.wait_recv()
        vector_sum[0] = halves[0] + halves_in[...]
        vector_sum[0, 6:7] = grad_query_bias
        vector_sum[0, 7:8] = grad_value_bias

        def vector_copies(i):
            return (
                remote(
                    vector_sum.at[i], vector_in.at[i], vec_send.at[2 * i], vec_recv.at[2 * i], peers[i]
                ),
                remote(
                    up_sum.at[i], up_in.at[i], vec_send.at[2 * i + 1], vec_recv.at[2 * i + 1], peers[i]
                ),
            )

        def vector_start(i):
            for copy in vector_copies(i):
                copy.start()

        def vector_finish(i):
            for copy in vector_copies(i):
                copy.wait_recv()
            vector_sum[i + 1] = vector_sum[i] + vector_in[i]
            up_sum[i + 1] = up_sum[i] + up_in[i]

        vector_start(0)
        for copy in part_swaps[2]:
            copy.wait_recv()

        def out_strip(at):
            value = hidden[at, :] + own_down[at, :] + part_in[2, at, :].astype(full) + bias_down
            rows_out[0, at, :] = value.astype(low)

        strips(block, 0, out_strip)
        alive = jnp.transpose(all_slots[0])[:, 1:2].astype(low)
        rows_out[0] = rows_out[0] * alive

        vector_finish(0)
        vector_start(1)
        pump(12, chunks + 1, chunks)
        vector_finish(1)
        vector_start(2)
        pump(chunks + 1, chunks + 4, chunks)
        vector_finish(2)
        vector_start(3)
        pump(chunks + 4, chunks + 6, chunks)
        for slot in range(2):
            source = jnp.where(core == slot, summed[chunks - 1, core], rest_in[...])
            wide_out[slot, :, rest_columns] = source[:, :rest]
            for place in range(2):
                start = CW // 2 + place * (thin - 2 * CW)
                thin_out[slot, place, :, thin_rest] = source[:, start : start + thin - 2 * CW]
        vector_finish(3)
        vectors_out[...] = vector_sum[4]
        up_bias_out[...] = up_sum[4]

        def drain(j, carry):
            held(j, lambda ref, k, i: first_copy(ref, k, i, False).wait_send())
            held(j, lambda ref, k, i: second_copy(ref, k, i, False).wait_send())
            held(j, lambda ref, k, i: high_copy(ref, k, i).wait_send())
            rest_copy(summed, j).wait_send()
            return carry

        lax.fori_loop(0, chunks, drain, 0)
        for i in range(4):
            for copy in vector_copies(i):
                copy.wait_send()

    pl.run_scoped(
        grad_scope,
        pltpu.VMEM((chunks - early_chunks, 2, 2, 2, rows, CW), low),
        pltpu.VMEM((chunks, 2, rows // 2, CW), full),
    )
    for copy in [vectors_swap, slots_swap, tokens_swap, out_swap, halves_swap]:
        copy.wait_send()
    for copies in part_swaps + [normed_swaps, hidden_swaps]:
        for copy in copies:
            copy.wait_send()
    for b in range(2):
        for pair in (left_pair, right_pair, normed_pair, other_pair, first_pair, second_pair):
            pair(b).wait_send()


def layer_call(tokens, out_grad, slots, vectors, up_bias, matrices):
    query_weight, up_weight, down_weight = matrices[0], matrices[4], matrices[5]
    low = jnp.bfloat16
    full = jnp.float32
    block, width = tokens.shape
    thin = query_weight.shape[0]
    wide = up_weight.shape[0]
    wide_pad = wide + -wide % 128
    heads = thin // HDIM
    replicas = lax.axis_size("replica")
    rows = width // replicas * 2
    chunks = wide // CW + 5
    half = rows // 2
    both = 2 * block
    vmem = pl.BlockSpec(memory_space=pltpu.VMEM)
    anywhere = pl.BlockSpec(memory_space=pl.ANY)
    dma = pltpu.SemaphoreType.DMA
    return pl.pallas_call(
        layer_kernel,
        out_shape=(
            jax.ShapeDtypeStruct((2,) + tokens.shape, low),
            jax.ShapeDtypeStruct((2, half, wide), full),
            jax.ShapeDtypeStruct((2, 2, half, thin), full),
            jax.ShapeDtypeStruct((8, thin), full),
            jax.ShapeDtypeStruct((1, wide_pad), full),
        ),
        in_specs=[anywhere] * 19,
        out_specs=(vmem,) * 5,
        scratch_shapes=[
            pltpu.VMEM((8, block), full),
            pltpu.VMEM((8, thin), full),
            pltpu.VMEM((8, wide), full),
            pltpu.VMEM((thin, width), low),
            pltpu.VMEM((thin, width), low),
            pltpu.VMEM((thin, width), low),
            pltpu.VMEM((thin, width), low),
            pltpu.VMEM((both, width), low),
            pltpu.VMEM((2, 8, block), full),
            pltpu.VMEM((8, thin), full),
            pltpu.VMEM((both, thin), low),
            pltpu.VMEM((both, thin), low),
            pltpu.VMEM((both, thin), low),
            pltpu.VMEM((2 * heads, block, block), low),
            pltpu.VMEM((block, width), full),
            pltpu.VMEM((block, width), full),
            pltpu.VMEM((block, width), full),
            pltpu.VMEM((block, width), full),
            pltpu.VMEM((4, block, width), low),
            pltpu.VMEM((4, block, width), low),
            pltpu.VMEM((2, both, width), low),
            pltpu.VMEM((2, both, wide_pad), low),
            pltpu.VMEM((2, both, width), low),
            pltpu.VMEM((2, both, thin), low),
            pltpu.VMEM((2, both, thin), low),
            pltpu.VMEM((both, width), low),
            pltpu.VMEM((both, wide_pad), low),
            pltpu.VMEM((both, width), low),
            pltpu.VMEM((both, width), low),
            pltpu.VMEM((both, thin), low),
            pltpu.VMEM((both, thin), low),
            pltpu.VMEM((EARLY, 2, 2, 2, rows, CW), low),
            pltpu.VMEM((chunks, 2, 2, rows, CW), low),
            pltpu.VMEM((chunks, 2, rows, CW), low),
            pltpu.VMEM((chunks, rows, CW), low),
            pltpu.VMEM((half, CW), full),
            pltpu.VMEM((8, width), full),
            pltpu.VMEM((2, 8, thin), full),
            pltpu.VMEM((8, thin), full),
            pltpu.VMEM((5, 8, thin), full),
            pltpu.VMEM((4, 8, thin), full),
            pltpu.VMEM((5, 1, wide_pad), full),
            pltpu.VMEM((4, 1, wide_pad), full),
            *[pltpu.VMEM((thin,), low)] * 8,
            *[pltpu.VMEM((block,), jnp.int32)] * 2,
            pltpu.VMEM((wide,), low),
            dma((11,)),
            dma((6,)),
            dma((17,)),
            dma((17,)),
            dma((12,)),
            dma((12,)),
            dma((chunks,)),
            dma((chunks,)),
            dma((chunks,)),
            dma((chunks,)),
            dma((chunks,)),
            dma((chunks,)),
            dma((chunks,)),
            dma((chunks,)),
            dma((8,)),
            dma((8,)),
        ],
        compiler_params=pltpu.CompilerParams(
            collective_id=0, has_side_effects=True, vmem_limit_bytes=67043328
        ),
        name="layer",
    )(tokens, out_grad, *slots, *vectors, up_bias, *matrices)


def whole_layer(
    tokens, out_grad, picture_ids, live_slots, ln1_gain, ln1_bias, query_weight, query_bias,
    key_weight, value_weight, value_bias, proj_weight, proj_bias, ln2_gain, ln2_bias, up_weight,
    up_bias, down_weight, down_bias,
):
    width = tokens.shape[1]
    if not by_kernel(lax.axis_size("replica"), width):
        return paired(
            tokens, out_grad, picture_ids, live_slots, ln1_gain, ln1_bias, query_weight,
            query_bias, key_weight, value_weight, value_bias, proj_weight, proj_bias, ln2_gain,
            ln2_bias, up_weight, up_bias, down_weight, down_bias,
        )
    wide = up_weight.shape[1]
    rows_out, wide_out, thin_out, vectors, up_bias_grad = layer_call(
        tokens,
        out_grad,
        (picture_ids, live_slots),
        (ln1_gain, ln1_bias, proj_bias, ln2_gain, ln2_bias, down_bias, query_bias, value_bias),
        up_bias,
        (query_weight.T, key_weight.T, value_weight.T, proj_weight, up_weight.T, down_weight),
    )
    return (
        rows_out[0],
        rows_out[1],
        vectors[0],
        vectors[1],
        thin_out[0, 0],
        vectors[6],
        thin_out[0, 1],
        thin_out[1, 0],
        vectors[7],
        thin_out[1, 1].T,
        vectors[2],
        vectors[3],
        vectors[4],
        wide_out[0],
        up_bias_grad[0, :wide],
        wide_out[1].T,
        vectors[5],
    )


def solution(mesh):
    in_specs = (
        P(("shard", "replica"), None),
        P(("shard", "replica"), None),
        P(("shard", "replica")),
        P(("shard", "replica")),
        P("shard"),
        P("shard"),
        P(None, "shard"),
        P("shard"),
        P(None, "shard"),
        P(None, "shard"),
        P("shard"),
        P("shard", None),
        P("shard"),
        P("shard"),
        P("shard"),
        P(None, "shard"),
        P("shard"),
        P("shard", None),
        P("shard"),
    )
    out_specs = (
        P(("shard", "replica"), None),
        P(("shard", "replica"), None),
        P("shard"),
        P("shard"),
        P("replica", "shard"),
        P("shard"),
        P("replica", "shard"),
        P("replica", "shard"),
        P("shard"),
        P("shard", "replica"),
        P("shard"),
        P("shard"),
        P("shard"),
        P("replica", "shard"),
        P("shard"),
        P("shard", "replica"),
        P("shard"),
    )
    return jax.shard_map(whole_layer, mesh=mesh, in_specs=in_specs, out_specs=out_specs, check_vma=False)
```

```python
import functools

import jax
import jax.numpy as jnp
from jax import lax
from jax.experimental import pallas as pl
from jax.experimental.pallas import tpu as pltpu
from jax.sharding import PartitionSpec as P

HDIM = 72
norm_eps = 1e-06
MESH = pl.DeviceIdType.MESH
CW = 256
EARLY = 2
AHEAD = 3
UNROLL = 2
GELU_SCALE = 0.7978845608028654


def norm_stats(values):
    centered = values - jnp.mean(values, axis=-1, keepdims=True)
    variance = jnp.mean(centered * centered, axis=-1, keepdims=True)
    inverse = lax.rsqrt(variance + norm_eps)
    return centered * inverse, inverse


def norm_grad(xhat, inverse, gain, grad):
    scaled = grad * gain
    return (
        scaled
        - jnp.mean(scaled, axis=-1, keepdims=True)
        - xhat * jnp.mean(scaled * xhat, axis=-1, keepdims=True)
    ) * inverse


def gelu_tanh(values):
    return jax.nn.gelu(values, approximate=True)


def product(left_side, right_side):
    return jnp.dot(left_side, right_side, preferred_element_type=jnp.float32)


def product_nt(left_side, right_side):
    return lax.dot_general(
        left_side, right_side, (((1,), (1,)), ((), ())), preferred_element_type=jnp.float32
    )


def product_tn(left_side, right_side):
    return lax.dot_general(
        left_side, right_side, (((0,), (0,)), ((), ())), preferred_element_type=jnp.float32
    )


def column_sums(matrix):
    return jnp.sum(matrix, axis=0, dtype=jnp.float32)


def swap(value):
    return lax.ppermute(value, "shard", [(0, 1), (1, 0)])


def split_heads(matrix, block_rows):
    return matrix.reshape(-1, block_rows, matrix.shape[1] // HDIM, HDIM)


def attend(queries, keys_in, values_in, allowed, block_rows):
    scores = jnp.einsum(
        "bqhd,bkhd->bhqk",
        split_heads(queries, block_rows),
        split_heads(keys_in, block_rows),
        preferred_element_type=jnp.float32,
    ) * HDIM ** (-0.5)
    scores = jnp.where(allowed[:, None, :, :], scores, -1e30)
    highest = jnp.max(scores, axis=-1, keepdims=True)
    scaled_exp = jnp.exp(scores - highest)
    totals = jnp.sum(scaled_exp, axis=-1, keepdims=True)
    probs = scaled_exp / totals
    mixed_out = jnp.einsum(
        "bhqk,bkhd->bqhd",
        probs.astype(jnp.bfloat16),
        split_heads(values_in, block_rows),
        preferred_element_type=jnp.float32,
    )
    return mixed_out.reshape(queries.shape), probs


def attend_back(queries, keys_in, values_in, grad_mixed, probs, block_rows):
    score_scale = HDIM ** (-0.5)
    split_grad = split_heads(grad_mixed, block_rows)
    grad_probs = jnp.einsum(
        "bqhd,bkhd->bhqk",
        split_grad,
        split_heads(values_in, block_rows),
        preferred_element_type=jnp.float32,
    )
    grad_scores = (
        probs * (grad_probs - jnp.sum(probs * grad_probs, axis=-1, keepdims=True))
    ).astype(jnp.bfloat16)
    grad_queries = (
        jnp.einsum(
            "bhqk,bkhd->bqhd",
            grad_scores,
            split_heads(keys_in, block_rows),
            preferred_element_type=jnp.float32,
        )
        * score_scale
    )
    grad_keys = (
        jnp.einsum(
            "bhqk,bqhd->bkhd",
            grad_scores,
            split_heads(queries, block_rows),
            preferred_element_type=jnp.float32,
        )
        * score_scale
    )
    grad_values = jnp.einsum(
        "bhqk,bqhd->bkhd",
        probs.astype(jnp.bfloat16),
        split_grad,
        preferred_element_type=jnp.float32,
    )
    return (
        grad_queries.astype(jnp.bfloat16).reshape(queries.shape),
        grad_keys.astype(jnp.bfloat16).reshape(queries.shape),
        grad_values.astype(jnp.bfloat16).reshape(queries.shape),
    )


def add_low(first, second):
    return (first.astype(jnp.float32) + second.astype(jnp.float32)).astype(jnp.bfloat16)


def by_kernel(replicas, width):
    return replicas == 2**4 and width % (replicas // 2 * 16) == 0


def plain_sums(block_out, tokens_grad, vectors, half, wide, query, key, value, proj, up, down):
    def owned(pair):
        return lax.psum_scatter(product_tn(*pair), "replica", scatter_dimension=0, tiled=True)

    vectors = lax.psum(vectors, "replica")

    def vector_at(i):
        return vectors[i * half : (i + 1) * half]

    return (
        block_out, tokens_grad, vector_at(0), vector_at(1), owned(query), vector_at(6),
        owned(key), owned(value), vector_at(7), owned(proj).T, vector_at(2), vector_at(3),
        vector_at(4), owned(up), vectors[8 * half : 8 * half + wide], owned(down).T, vector_at(5),
    )


def paired(
    tokens, out_grad, picture_ids, live_slots, ln1_gain, ln1_bias, query_weight, query_bias,
    key_weight, value_weight, value_bias, proj_weight, proj_bias, ln2_gain, ln2_bias, up_weight,
    up_bias, down_weight, down_bias,
):
    low = jnp.bfloat16
    full = jnp.float32
    rows, width = tokens.shape
    half = width // 2
    wide = up_weight.shape[1]
    shard = lax.axis_index("shard")
    own_vectors = jnp.stack([ln1_gain, ln1_bias, proj_bias, ln2_gain, ln2_bias, down_bias])
    slots = jnp.stack([picture_ids, live_slots])
    peer_tokens, peer_out, peer_vectors, peer_slots = (
        swap(tokens), swap(out_grad), swap(own_vectors), swap(slots),
    )
    gain_one, shift_one, bias_proj, gain_two, shift_two, bias_down = jnp.where(
        shard == 0,
        jnp.concatenate([own_vectors, peer_vectors], axis=1),
        jnp.concatenate([peer_vectors, own_vectors], axis=1),
    ).astype(full)
    slots = jnp.concatenate([slots, peer_slots], axis=1)
    alive = slots[1].astype(full)[:, None]
    ids = slots[0].reshape(2, rows)
    living = slots[1].reshape(2, rows)
    allowed = (ids[:, :, None] == ids[:, None, :]) & (living[:, None, :] == 1)
    all_tokens = jnp.concatenate([tokens, peer_tokens]).astype(full)
    all_out = jnp.concatenate([out_grad, peer_out]) * alive.astype(low)
    xhat_one, inverse_one = norm_stats(all_tokens)
    normed = (xhat_one * gain_one + shift_one).astype(low)
    queries = (product(normed, query_weight) + query_bias.astype(full)).astype(low)
    keys_all = product(normed, key_weight).astype(low)
    values_all = (product(normed, value_weight) + value_bias.astype(full)).astype(low)
    mixed_out, probs = attend(queries, keys_all, values_all, allowed, rows)
    mixed = mixed_out.astype(low)
    partial = product(mixed, proj_weight)
    hidden = all_tokens[:rows] + partial[:rows] + swap(partial[rows:].astype(low)).astype(full) + bias_proj
    xhat_two, inverse_two = norm_stats(hidden)
    normed_own = (xhat_two * gain_two + shift_two).astype(low)
    normed_two = jnp.concatenate([normed_own, swap(normed_own)])
    up_proj = product(normed_two, up_weight) + up_bias.astype(full)
    activated = gelu_tanh(up_proj).astype(low)
    grad_act = product_nt(all_out, down_weight)
    grad_up = jax.vjp(gelu_tanh, up_proj)[1](grad_act)[0].astype(low)
    partial = product_nt(grad_up, up_weight)
    grad_two = partial[:rows] + swap(partial[rows:].astype(low)).astype(full)
    partial = product(activated, down_weight)
    block_out = (
        (hidden + partial[:rows] + swap(partial[rows:].astype(low)).astype(full) + bias_down)
        * alive[:rows]
    ).astype(low)
    grad_hidden = all_out[:rows].astype(full) + norm_grad(xhat_two, inverse_two, gain_two, grad_two)
    hidden_own = grad_hidden.astype(low)
    hidden_low = jnp.concatenate([hidden_own, swap(hidden_own)])
    grad_mixed = product_nt(hidden_low, proj_weight).astype(low)
    grad_queries, grad_keys, grad_values = attend_back(
        queries, keys_all, values_all, grad_mixed, probs, rows
    )
    partial = (
        product_nt(grad_queries, query_weight)
        + product_nt(grad_keys, key_weight)
        + product_nt(grad_values, value_weight)
    )
    grad_one = partial[:rows] + swap(partial[rows:].astype(low)).astype(full)
    tokens_grad = (
        grad_hidden + norm_grad(xhat_one[:rows], inverse_one[:rows], gain_one, grad_one)
    ).astype(low)
    wholes = jnp.stack(
        [
            column_sums(grad_one * xhat_one[:rows]),
            column_sums(grad_one),
            column_sums(hidden_own),
            column_sums(grad_two * xhat_two),
            column_sums(grad_two),
            column_sums(all_out[:rows]),
        ]
    )
    mine = lax.dynamic_slice_in_dim(wholes, shard * half, half, 1)
    theirs = lax.dynamic_slice_in_dim(wholes, (1 - shard) * half, half, 1)
    halves = mine + swap(theirs)
    vectors = jnp.concatenate(
        [
            halves.reshape(-1),
            column_sums(grad_queries),
            column_sums(grad_values),
            column_sums(grad_up),
        ]
    )
    return plain_sums(
        block_out, tokens_grad, vectors, half, wide,
        (normed, grad_queries), (normed, grad_keys), (normed, grad_values),
        (hidden_low, mixed), (normed_two, grad_up), (all_out, activated),
    )


def take(ref, start, count):
    return ref.at[pl.ds(start, count)]


def layer_kernel(
    tokens_hbm,
    out_hbm,
    picture_ids,
    live_slots,
    ln1_gain,
    ln1_bias,
    proj_bias,
    ln2_gain,
    ln2_bias,
    down_bias,
    query_bias,
    value_bias,
    up_bias_in,
    query_hbm,
    key_hbm,
    value_hbm,
    proj_hbm,
    up_hbm,
    down_hbm,
    rows_out,
    wide_out,
    thin_out,
    vectors_out,
    up_bias_out,
    slots,
    vectors,
    up_bias,
    query_weight,
    key_weight,
    value_weight,
    proj_weight,
    all_tokens,
    all_slots,
    vectors_in,
    queries,
    keys_all,
    values_all,
    probs,
    hidden,
    grad_hidden,
    own_part,
    own_down,
    part_send,
    part_in,
    wide_left,
    wide_right,
    thin_left,
    thin_first,
    thin_second,
    wide_left_in,
    wide_right_in,
    thin_left_in,
    thin_other_in,
    thin_first_in,
    thin_second_in,
    early,
    from_first,
    from_second,
    from_high,
    rest_in,
    totals,
    halves,
    halves_in,
    vector_sum,
    vector_in,
    up_sum,
    up_in,
    flat_0,
    flat_1,
    flat_2,
    flat_3,
    flat_4,
    flat_5,
    flat_6,
    flat_7,
    flat_slots_0,
    flat_slots_1,
    flat_up,
    small_sem,
    load_sem,
    swap_send,
    swap_recv,
    pair_send,
    pair_recv,
    first_send,
    first_recv,
    second_send,
    second_recv,
    high_send,
    high_recv,
    core_send,
    core_recv,
    vec_send,
    vec_recv,
):
    full = jnp.float32
    low = jnp.bfloat16
    chunks = from_first.shape[0]
    rows = from_first.shape[3]
    early_chunks = early.shape[0]
    block, width = tokens_hbm.shape
    thin = queries.shape[1]
    wide = up_bias.shape[1]
    heads = thin // HDIM
    score_scale = HDIM ** (-0.5)
    wide_chunks = chunks - 5
    half_block = block // 2
    strip = 32
    shard = lax.axis_index("shard")
    replica = lax.axis_index("replica")
    core = lax.rem(replica, 2)
    other = 1 - core
    y_bit = lax.rem(replica // 2, 2)
    low_bit = lax.rem(replica // 4, 2)
    high_bit = lax.rem(replica // 8, 2)
    twin = (1 - shard, replica)
    partner = (shard, replica + 1 - 2 * core)
    y_peer = (shard, replica + 2 - 4 * y_bit)
    low_peer = (shard, replica + 4 - 8 * low_bit)
    high_peer = (shard, replica + 8 - 16 * high_bit)
    peers = (partner, y_peer, low_peer, high_peer)

    def remote(source, target, send, recv, peer):
        return pltpu.make_async_remote_copy(
            src_ref=source,
            dst_ref=target,
            send_sem=send,
            recv_sem=recv,
            device_id=peer,
            device_id_type=MESH,
        )

    def swapped(index, source, target):
        return remote(source, target, swap_send.at[index], swap_recv.at[index], twin)

    def paired_copy(index, source, target):
        return remote(source, target, pair_send.at[index], pair_recv.at[index], partner)

    loads = [
        pltpu.make_async_copy(source, target, load_sem.at[i])
        for i, (source, target) in enumerate(
            (
                (query_hbm, query_weight),
                (key_hbm, key_weight),
                (value_hbm, value_weight),
                (proj_hbm, proj_weight),
                (tokens_hbm, take(all_tokens, 0, block)),
                (out_hbm, wide_left.at[1, pl.ds(0, block)]),
            )
        )
    ]
    barrier = pltpu.get_barrier_semaphore()
    for peer in (twin,) + peers:
        pl.semaphore_signal(barrier, inc=1, device_id=peer, device_id_type=MESH)
    small = [
        pltpu.make_async_copy(source, target, small_sem.at[i])
        for i, (source, target) in enumerate(
            (
                (ln1_gain, flat_0),
                (ln1_bias, flat_1),
                (proj_bias, flat_2),
                (ln2_gain, flat_3),
                (ln2_bias, flat_4),
                (down_bias, flat_5),
                (query_bias, flat_6),
                (value_bias, flat_7),
                (picture_ids, flat_slots_0),
                (live_slots, flat_slots_1),
                (up_bias_in, flat_up),
            )
        )
    ]
    for load in small + loads[4:] + loads[:4]:
        load.start()
    slots[...] = jnp.zeros_like(slots)
    tokens_swaps = [
        swapped(
            index,
            tokens_hbm.at[pl.ds(j * half_block, half_block)],
            all_tokens.at[pl.ds(block + j * half_block, half_block)],
        )
        for j, index in ((0, 2), (1, 17))
    ]
    pl.semaphore_wait(barrier, 5)
    tokens_swaps[0].start()
    for load in small:
        load.wait()
    named = (flat_0, flat_1, flat_2, flat_3, flat_4, flat_5, flat_6, flat_7)
    for i, value in enumerate(named):
        vectors[i : i + 1, :] = value[...].astype(full).reshape(1, thin)
    slots[0:1, :] = flat_slots_0[...].astype(full).reshape(1, block)
    slots[1:2, :] = flat_slots_1[...].astype(full).reshape(1, block)
    up_bias[0:1, :] = flat_up[...].astype(full).reshape(1, wide)

    vectors_swap = swapped(0, vectors, vectors_in)
    slots_swap = swapped(1, slots, all_slots.at[1])
    out_swap = swapped(3, out_hbm, wide_left.at[1, pl.ds(block, block)])
    part_swaps = [
        [
            swapped(
                4 + 2 * i + j,
                part_send.at[i, pl.ds(j * half_block, half_block)],
                part_in.at[i, pl.ds(j * half_block, half_block)],
            )
            for j in range(2)
        ]
        for i in range(4)
    ]
    normed_swaps = [
        swapped(
            12 + j,
            wide_left.at[0, pl.ds(j * half_block, half_block)],
            wide_left.at[0, pl.ds(block + j * half_block, half_block)],
        )
        for j in range(2)
    ]
    hidden_swaps = [
        swapped(
            14 + j,
            thin_left.at[1, pl.ds(j * half_block, half_block)],
            thin_left.at[1, pl.ds(block + j * half_block, half_block)],
        )
        for j in range(2)
    ]
    halves_swap = swapped(16, halves.at[1], halves_in)

    def pair_rows(index, source, target, b):
        here = pl.ds(b * block, block)
        return paired_copy(index + b, source.at[here], target.at[here])

    def left_pair(b):
        return pair_rows(0, wide_left.at[other], wide_left_in, b)

    def right_pair(q):
        here = pl.ds(q * half_block, half_block)
        return paired_copy(2 + q, wide_right.at[other, here], wide_right_in.at[here])

    def normed_pair(b):
        return pair_rows(6, thin_left.at[0], thin_left_in, b)

    def other_pair(b):
        return pair_rows(8, thin_left.at[other], thin_other_in, b)

    def first_pair(b):
        return pair_rows(10, thin_first.at[other], thin_first_in, b)

    def second_pair(b):
        return pair_rows(12, thin_second.at[other], thin_second_in, b)

    vectors_swap.start()
    slots_swap.start()
    tokens_swaps[1].start()
    out_swap.start()

    all_slots[0] = slots[...]
    for load in loads[4:]:
        load.wait()
    totals[...] = jnp.zeros_like(totals)
    up_sum[0] = jnp.zeros(up_sum.shape[1:], full)

    vectors_swap.wait_recv()
    slots_swap.wait_recv()
    here_half = vectors[...]
    there_half = vectors_in[...]
    joined = jnp.where(
        shard == 0,
        jnp.concatenate([here_half, there_half], axis=1),
        jnp.concatenate([there_half, here_half], axis=1),
    )
    gain_one, shift_one, bias_proj = joined[0:1], joined[1:2], joined[2:3]
    gain_two, shift_two, bias_down = joined[3:4], joined[4:5], joined[5:6]
    bias_query, bias_value = here_half[6:7], here_half[7:8]

    def strips(count, first, body):
        def step(i, carry):
            body(pl.ds(pl.multiple_of(first + i * strip, strip), strip))
            return carry

        lax.fori_loop(0, count // strip, step, 0, unroll=2)

    def is_low_first(j):
        return lax.rem(j, 4) == 1

    def first_pick(grads, k, low_first):
        if low_first:
            return grads.at[k, :, 1 - low_bit], low_peer
        return grads.at[k, :, :, 1 - y_bit], y_peer

    def second_pick(grads, k, low_first):
        if low_first:
            return grads.at[k, :, low_bit, 1 - y_bit], y_peer
        return grads.at[k, :, 1 - low_bit, y_bit], low_peer

    def first_copy(grads, k, j, low_first):
        source, peer = first_pick(grads, k, low_first)
        return remote(source, from_first.at[j], first_send.at[j], first_recv.at[j], peer)

    def second_copy(grads, k, j, low_first):
        source, peer = second_pick(grads, k, low_first)
        return remote(source, from_second.at[j], second_send.at[j], second_recv.at[j], peer)

    def high_copy(grads, k, j):
        return remote(
            grads.at[k, 1 - high_bit, low_bit, y_bit],
            from_high.at[j],
            high_send.at[j],
            high_recv.at[j],
            high_peer,
        )

    def by_order(j, action):
        low_first = is_low_first(j)

        @pl.when(low_first)
        def _():
            action(True)

        @pl.when(jnp.logical_not(low_first))
        def _():
            action(False)

    def issue(grads, k, j):
        by_order(j, lambda low_first: first_copy(grads, k, j, low_first).start())

    def emit(grads, k, j, value, ahead):
        grads[k] = value.astype(low).reshape(grads.shape[1:])

        @pl.when(j < ahead)
        def _():
            issue(grads, k, j)

    def take_first(grads, k, j):
        def action(low_first):
            first_copy(grads, k, j, low_first).wait_recv()
            if low_first:
                grads[k, :, low_bit] = add_low(grads[k, :, low_bit], from_first[j])
            else:
                grads[k, :, :, y_bit] = add_low(grads[k, :, :, y_bit], from_first[j])
            second_copy(grads, k, j, low_first).start()

        by_order(j, action)

    def take_second(grads, k, j):
        by_order(j, lambda low_first: second_copy(grads, k, j, low_first).wait_recv())
        grads[k, :, low_bit, y_bit] = add_low(grads[k, :, low_bit, y_bit], from_second[j])
        high_copy(grads, k, j).start()

    def rest_copy(summed, j):
        return remote(summed.at[j, other], rest_in, core_send.at[j], core_recv.at[j], partner)

    def wide_place(slot, j):
        return wide_out.at[slot, :, pl.ds(pl.multiple_of(j * CW, CW), CW)]

    def thin_place(slot, j):
        at = (j - wide_chunks) // 2
        return thin_out.at[
            slot, lax.rem(j - wide_chunks, 2), :, pl.ds(pl.multiple_of(at * CW, CW), CW)
        ]

    def core_copy(summed, j, place):
        return remote(
            summed.at[j, other], place(core, j), core_send.at[j], core_recv.at[j], partner
        )

    def take_high(grads, k, j, summed):
        high_copy(grads, k, j).wait_recv()
        total = grads[k, high_bit, low_bit, y_bit].astype(full) + from_high[j].astype(full)
        summed[j] = total.reshape(2, rows // 2, CW)

        @pl.when(j < wide_chunks)
        def _():
            core_copy(summed, j, wide_place).start()
            wide_place(core, j)[...] = summed[j, core]

        @pl.when(jnp.logical_and(j >= wide_chunks, j < chunks - 1))
        def _():
            core_copy(summed, j, thin_place).start()
            thin_place(core, j)[...] = summed[j, core]

        @pl.when(j == chunks - 1)
        def _():
            rest_copy(summed, j).start()

    def wide_value(j):
        columns = pl.ds(pl.multiple_of(j * CW, CW), CW)
        return product_tn(wide_left[core], wide_right[core, :, columns]) + product_tn(
            wide_left_in[...], wide_right_in[:, columns]
        )

    def mlp_scope(up_weight, down_weight, grad_act, wide_sem):
        wide_loads = [
            pltpu.make_async_copy(up_hbm, up_weight, wide_sem.at[0]),
            pltpu.make_async_copy(down_hbm, down_weight, wide_sem.at[1]),
        ]
        for load in wide_loads:
            load.start()

        def attend_step(b, carry):
            here = pl.ds(pl.multiple_of(b * block, block), block)

            @pl.when(b == 1)
            def _():
                for copy in tokens_swaps:
                    copy.wait_recv()

            def norm_strip(at):
                xhat, _ = norm_stats(all_tokens[at, :].astype(full))
                thin_left[0, at, :] = (xhat * gain_one + shift_one).astype(low)

            strips(block, b * block, norm_strip)

            @pl.when(b == 0)
            def _():
                for load in loads[:4]:
                    load.wait()

            normed = thin_left[0, here, :]
            queries[here, :] = (product_nt(normed, query_weight[...]) + bias_query).astype(low)
            keys_all[here, :] = product_nt(normed, key_weight[...]).astype(low)
            values_all[here, :] = (product_nt(normed, value_weight[...]) + bias_value).astype(low)
            marks = all_slots[b]
            across = jnp.where(marks[1:2] == 1.0, marks[0:1], -1.0)
            down_ids = jnp.transpose(marks)[:, 0:1]
            allowed = down_ids == across
            q_all = queries[here, :]
            k_all = keys_all[here, :]
            v_all = values_all[here, :]
            for h in range(heads):
                cut = slice(h * HDIM, (h + 1) * HDIM)
                scores = product_nt(q_all[:, cut], k_all[:, cut]) * score_scale
                scores = jnp.where(allowed, scores, -1e30)
                scaled = jnp.exp(scores - jnp.max(scores, axis=-1, keepdims=True))
                share = 1.0 / jnp.sum(scaled, axis=-1, keepdims=True)
                probs_low = (scaled * share).astype(low)
                probs[b * heads + h] = probs_low
                thin_second[1, here, cut] = product(probs_low, v_all[:, cut]).astype(low)
            mixed = thin_second[1, here, :]

            def proj_tile(n, inner):
                at = pl.ds(pl.multiple_of(n * 384, 384), 384)
                value = product(mixed, proj_weight[:, at])

                @pl.when(b == 0)
                def _():
                    own_part[:, at] = value

                @pl.when(b == 1)
                def _():
                    part_send[0, :, at] = value.astype(low)

                return inner

            lax.fori_loop(0, width // 384, proj_tile, 0)
            return carry

        lax.fori_loop(0, 2, attend_step, 0)
        for copy in part_swaps[0]:
            copy.start()
        for b in range(2):
            normed_pair(b).start()

        out_swap.wait_recv()
        for b in range(2):
            alive = jnp.transpose(all_slots[b])[:, 1:2].astype(low)
            whole = pl.ds(b * block, block)
            wide_left[1, whole, :] = wide_left[1, whole, :] * alive
        wide_loads[1].wait()
        out_rows = wide_left[1]

        def act_tile(t, carry):
            at = pl.ds(pl.multiple_of(t * 512, 512), 512)
            grad_act[:, at] = product_nt(out_rows, down_weight[at, :]).astype(low)
            return carry

        lax.fori_loop(0, wide_chunks // 2, act_tile, 0)
        rest_from = wide_chunks * CW
        rest = wide - rest_from
        rest_at = pl.ds(rest_from, rest)
        grad_act[:, rest_at] = product_nt(out_rows, down_weight[rest_at, :]).astype(low)
        wide_loads[0].wait()
        pad_at = pl.ds(rest_from, CW // 2)
        wide_right[0, :, pad_at] = jnp.zeros((2 * block, CW // 2), low)
        wide_right[1, :, pad_at] = jnp.zeros((2 * block, CW // 2), low)

        for j in range(2):
            part_swaps[0][j].wait_recv()

            def hidden_strip(at):
                value = (
                    all_tokens[at, :].astype(full)
                    + own_part[at, :]
                    + part_in[0, at, :].astype(full)
                    + bias_proj
                )
                hidden[at, :] = value
                xhat, _ = norm_stats(value)
                wide_left[0, at, :] = (xhat * gain_two + shift_two).astype(low)

            strips(half_block, j * half_block, hidden_strip)
            normed_swaps[j].start()

        left_pair(0).start()

        def gelu_tile(here, at):
            value = product_nt(wide_left[0, here, :], up_weight[at, :]) + up_bias[0:1, at]
            square = value * value
            bent = jnp.tanh(GELU_SCALE * value * (1.0 + 0.044715 * square))
            bulge = 0.5 * (1.0 + bent)
            wide_right[1, here, at] = (value * bulge).astype(low)
            slope = bulge + 0.5 * value * (1.0 - bent * bent) * (
                GELU_SCALE * (1.0 + 0.134145 * square)
            )
            grad = (slope * grad_act[here, at].astype(full)).astype(low)
            wide_right[0, here, at] = grad
            up_sum[0, :, at] += jnp.sum(grad.astype(full), axis=0, keepdims=True)

        def back_tiles(b):
            grad_rows = wide_right[0, pl.ds(b * block, block), pl.ds(0, wide)]

            def back_tile(n, inner):
                at = pl.ds(pl.multiple_of(n * 384, 384), 384)
                value = product(grad_rows, up_weight[:, at])
                if b == 0:
                    own_part[:, at] = value
                else:
                    part_send[1, :, at] = value.astype(low)
                return inner

            lax.fori_loop(0, width // 384, back_tile, 0)

        def mlp_step(q, carry):
            here = pl.ds(pl.multiple_of(q * half_block, half_block), half_block)
            for j in range(2):

                @pl.when(q == 2 + j)
                def _():
                    normed_swaps[j].wait_recv()
                    if j == 1:
                        left_pair(1).start()

            def up_tile(t, inner):
                gelu_tile(here, pl.ds(pl.multiple_of(t * CW, CW), CW))
                return inner

            lax.fori_loop(0, wide_chunks, up_tile, 0, unroll=UNROLL)
            gelu_tile(here, rest_at)
            right_pair(q).start()

            @pl.when(q == 1)
            def _():
                back_tiles(0)

            return carry

        lax.fori_loop(0, 4, mlp_step, 0)
        for i in range(2):
            left_pair(i).wait_recv()
        for q in range(4):
            right_pair(q).wait_recv()

        def early_step(j, inner):
            emit(early, j, j, wide_value(j), AHEAD)
            return inner

        lax.fori_loop(0, early_chunks, early_step, 0)
        back_tiles(1)
        for copy in part_swaps[1]:
            copy.start()
        act_rows = wide_right[1, :, pl.ds(0, wide)]

        def down_tile(n, inner):
            at = pl.ds(pl.multiple_of(n * 384, 384), 384)
            value = product(act_rows, down_weight[:, at])
            own_down[:, at] = value[:block]
            part_send[2, :, at] = value[block:].astype(low)
            return inner

        lax.fori_loop(0, width // 384, down_tile, 0)

    pl.run_scoped(
        mlp_scope,
        pltpu.VMEM(up_hbm.shape, low),
        pltpu.VMEM(down_hbm.shape, low),
        pltpu.VMEM((2 * block, wide_right.shape[2]), low),
        pltpu.SemaphoreType.DMA((2,)),
    )

    def grad_scope(grads, summed):
        def held(j, action):
            @pl.when(j < early_chunks)
            def _():
                action(early, j, j)

            @pl.when(j >= early_chunks)
            def _():
                action(grads, j - early_chunks, j)

        def pump_step(i, carry):
            @pl.when(i >= 6)
            def _():
                rest_copy(summed, i - 6).wait_recv()

            @pl.when(jnp.logical_and(i >= 4, i < chunks + 4))
            def _():
                held(i - 4, lambda ref, k, j: take_high(ref, k, j, summed))

            @pl.when(jnp.logical_and(i >= 2, i < chunks + 2))
            def _():
                held(i - 2, take_second)

            @pl.when(i < chunks)
            def _():
                held(i, take_first)

            return carry

        def pump(first, last, made=wide_chunks):
            def step(i, carry):
                pump_step(i, carry)

                @pl.when(i + AHEAD < made)
                def _():
                    issue(grads, i + AHEAD - early_chunks, i + AHEAD)

                return carry

            lax.fori_loop(first, last, step, 0)

        def emit_late(j, value, ahead):
            emit(grads, j - early_chunks, j, value, ahead)

        def wide_step(j, carry):
            emit_late(j, wide_value(j), AHEAD)
            return carry

        lax.fori_loop(early_chunks, wide_chunks, wide_step, 0)
        pump(0, 2)

        for j in range(2):
            part_swaps[1][j].wait_recv()

            def norm_back_strip(at):
                grad = own_part[at, :] + part_in[1, at, :].astype(full)
                xhat, inverse = norm_stats(hidden[at, :])
                out_rows = wide_left[1, at, :].astype(full)
                value = out_rows + norm_grad(xhat, inverse, gain_two, grad)
                grad_hidden[at, :] = value
                rounded = value.astype(low)
                thin_left[1, at, :] = rounded
                totals[2:3] += column_sums(rounded.astype(full))[None]
                totals[3:4] += column_sums(grad * xhat)[None]
                totals[4:5] += column_sums(grad)[None]
                totals[5:6] += column_sums(out_rows)[None]

            strips(half_block, j * half_block, norm_back_strip)
            hidden_swaps[j].start()
        for copy in part_swaps[2]:
            copy.start()

        pump(2, 3)

        def back_step(b, carry):
            here = pl.ds(pl.multiple_of(b * block, block), block)

            @pl.when(b == 1)
            def _():
                for copy in hidden_swaps:
                    copy.wait_recv()
                for i in range(2):
                    other_pair(i).start()

            grad_mixed = product_nt(thin_left[1, here, :], proj_weight[...]).astype(low)
            q_all = queries[here, :]
            k_all = keys_all[here, :]
            v_all = values_all[here, :]
            for h in range(heads):
                cut = slice(h * HDIM, (h + 1) * HDIM)
                probs_low = probs[b * heads + h]
                probs_full = probs_low.astype(full)
                mixed_grad = grad_mixed[:, cut]
                grad_probs = product_nt(mixed_grad, v_all[:, cut])
                weighted = probs_full * grad_probs
                grad_scores = (
                    weighted - probs_full * jnp.sum(weighted, axis=-1, keepdims=True)
                ).astype(low)
                thin_first[0, here, cut] = (product(grad_scores, k_all[:, cut]) * score_scale).astype(low)
                thin_second[0, here, cut] = (
                    product_tn(grad_scores, q_all[:, cut]) * score_scale
                ).astype(low)
                thin_first[1, here, cut] = product_tn(probs_low, mixed_grad).astype(low)

            @pl.when(b == 0)
            def _():
                first_pair(0).start()
                second_pair(0).start()

            @pl.when(b == 1)
            def _():
                first_pair(1).start()
                second_pair(1).start()

            grad_q = thin_first[0, here, :]
            grad_k = thin_second[0, here, :]
            grad_v = thin_first[1, here, :]

            def normed_tile(n, inner):
                at = pl.ds(pl.multiple_of(n * 384, 384), 384)
                value = (
                    product(grad_q, query_weight[:, at])
                    + product(grad_k, key_weight[:, at])
                    + product(grad_v, value_weight[:, at])
                )

                @pl.when(b == 0)
                def _():
                    own_part[:, at] = value

                @pl.when(b == 1)
                def _():
                    part_send[3, :, at] = value.astype(low)

                return inner

            lax.fori_loop(0, width // 384, normed_tile, 0)
            pump(3 + 2 * b, 5 + 2 * b)
            return carry

        lax.fori_loop(0, 2, back_step, 0)
        for copy in part_swaps[3]:
            copy.start()

        for b in range(2):
            for pair in (normed_pair, other_pair, first_pair, second_pair):
                pair(b).wait_recv()

        def first_part(columns):
            return product_tn(thin_left[0], thin_first[core, :, columns]) + product_tn(
                thin_left_in[...], thin_first_in[:, columns]
            )

        def second_part(columns):
            return product_tn(thin_left[core], thin_second[core, :, columns]) + product_tn(
                thin_other_in[...], thin_second_in[:, columns]
            )

        def thin_step(j, carry):
            columns = pl.ds(pl.multiple_of(j * CW, CW), CW)
            emit_late(wide_chunks + 2 * j, first_part(columns), 7 + AHEAD)
            emit_late(wide_chunks + 2 * j + 1, second_part(columns), 7 + AHEAD)
            return carry

        lax.fori_loop(0, 2, thin_step, 0)
        thin_rest = pl.ds(2 * CW, thin - 2 * CW)
        wide_rest = pl.ds(wide_chunks * CW, CW // 2)
        rest = wide - wide_chunks * CW
        rest_columns = pl.ds(wide_chunks * CW, rest)
        emit_late(
            chunks - 1,
            jnp.concatenate(
                [
                    product_tn(wide_left[core], wide_right[core, :, wide_rest])
                    + product_tn(wide_left_in[...], wide_right_in[:, wide_rest]),
                    first_part(thin_rest),
                    second_part(thin_rest),
                ],
                axis=1,
            ),
            7 + AHEAD,
        )
        pump(7, 10, chunks)

        for copy in part_swaps[3]:
            copy.wait_recv()

        def final_strip(at):
            grad = own_part[at, :] + part_in[3, at, :].astype(full)
            xhat, inverse = norm_stats(all_tokens[at, :].astype(full))
            rows_out[1, at, :] = (
                grad_hidden[at, :] + norm_grad(xhat, inverse, gain_one, grad)
            ).astype(low)
            totals[0:1] += column_sums(grad * xhat)[None]
            totals[1:2] += column_sums(grad)[None]

        strips(block, 0, final_strip)
        sums = totals[...]
        lower = sums[:, :thin]
        upper = sums[:, thin:]
        halves[0] = jnp.where(shard == 0, lower, upper)
        halves[1] = jnp.where(shard == 0, upper, lower)
        halves_swap.start()
        pump(10, 12, chunks)
        grad_query_bias = column_sums(thin_first[0].astype(full))[None]
        grad_value_bias = column_sums(thin_first[1].astype(full))[None]
        halves_swap.wait_recv()
        vector_sum[0] = halves[0] + halves_in[...]
        vector_sum[0, 6:7] = grad_query_bias
        vector_sum[0, 7:8] = grad_value_bias

        def vector_copies(i):
            return (
                remote(
                    vector_sum.at[i], vector_in.at[i], vec_send.at[2 * i], vec_recv.at[2 * i], peers[i]
                ),
                remote(
                    up_sum.at[i], up_in.at[i], vec_send.at[2 * i + 1], vec_recv.at[2 * i + 1], peers[i]
                ),
            )

        def vector_start(i):
            for copy in vector_copies(i):
                copy.start()

        def vector_finish(i):
            for copy in vector_copies(i):
                copy.wait_recv()
            vector_sum[i + 1] = vector_sum[i] + vector_in[i]
            up_sum[i + 1] = up_sum[i] + up_in[i]

        vector_start(0)
        for copy in part_swaps[2]:
            copy.wait_recv()

        def out_strip(at):
            value = hidden[at, :] + own_down[at, :] + part_in[2, at, :].astype(full) + bias_down
            rows_out[0, at, :] = value.astype(low)

        strips(block, 0, out_strip)
        alive = jnp.transpose(all_slots[0])[:, 1:2].astype(low)
        rows_out[0] = rows_out[0] * alive

        vector_finish(0)
        vector_start(1)
        pump(12, chunks + 1, chunks)
        vector_finish(1)
        vector_start(2)
        pump(chunks + 1, chunks + 4, chunks)
        vector_finish(2)
        vector_start(3)
        pump(chunks + 4, chunks + 6, chunks)
        for slot in range(2):
            source = jnp.where(core == slot, summed[chunks - 1, core], rest_in[...])
            wide_out[slot, :, rest_columns] = source[:, :rest]
            for place in range(2):
                start = CW // 2 + place * (thin - 2 * CW)
                thin_out[slot, place, :, thin_rest] = source[:, start : start + thin - 2 * CW]
        vector_finish(3)
        vectors_out[...] = vector_sum[4]
        up_bias_out[...] = up_sum[4]

        def drain(j, carry):
            held(j, lambda ref, k, i: first_copy(ref, k, i, False).wait_send())
            held(j, lambda ref, k, i: second_copy(ref, k, i, False).wait_send())
            held(j, lambda ref, k, i: high_copy(ref, k, i).wait_send())
            rest_copy(summed, j).wait_send()
            return carry

        lax.fori_loop(0, chunks, drain, 0)
        for i in range(4):
            for copy in vector_copies(i):
                copy.wait_send()

    pl.run_scoped(
        grad_scope,
        pltpu.VMEM((chunks - early_chunks, 2, 2, 2, rows, CW), low),
        pltpu.VMEM((chunks, 2, rows // 2, CW), full),
    )
    for copy in [vectors_swap, slots_swap, *tokens_swaps, out_swap, halves_swap]:
        copy.wait_send()
    for copies in part_swaps + [normed_swaps, hidden_swaps]:
        for copy in copies:
            copy.wait_send()
    for q in range(4):
        right_pair(q).wait_send()
    for b in range(2):
        for pair in (left_pair, normed_pair, other_pair, first_pair, second_pair):
            pair(b).wait_send()


def publish_kernel(rows_in, wide_in, thin_in, vectors_in, up_in, *refs):
    outs, (rows_at, wide_at, thin_at, vectors_at, up_at) = refs[:17], refs[17:22]
    flats, in_sem, out_sem = refs[22:31], refs[31], refs[32]
    loads = [
        pltpu.make_async_copy(source, target, in_sem.at[i])
        for i, (source, target) in enumerate(
            (
                (vectors_in, vectors_at),
                (up_in, up_at),
                (thin_in, thin_at),
                (wide_in, wide_at),
                (rows_in, rows_at),
            )
        )
    ]
    for load in loads:
        load.start()
    stores = []

    def store(source, place):
        copy = pltpu.make_async_copy(source, outs[place], out_sem.at[place])
        copy.start()
        stores.append(copy)

    loads[0].wait()
    loads[1].wait()
    for i in range(8):
        flats[i][...] = vectors_at[i : i + 1, :].reshape(flats[i].shape)
    wide = flats[8].shape[0]
    flats[8][...] = up_at[:, :wide].reshape(flats[8].shape)
    loads[2].wait()
    for source, place in ((thin_at.at[0, 0], 4), (thin_at.at[0, 1], 6), (thin_at.at[1, 0], 7), (thin_at.at[1, 1], 9)):
        store(source, place)
    loads[3].wait()
    store(wide_at.at[0], 13)
    store(wide_at.at[1], 15)
    loads[4].wait()
    store(rows_at.at[0], 0)
    store(rows_at.at[1], 1)
    for flat, place in zip(flats, (2, 3, 10, 11, 12, 16, 5, 8, 14)):
        store(flat, place)
    for copy in stores:
        copy.wait()


def publish_call(rows_out, wide_out, thin_out, vectors, up_bias_grad):
    full = jnp.float32
    thin = vectors.shape[1]
    _, half, wide = wide_out.shape
    anywhere = pl.BlockSpec(memory_space=pl.ANY)
    vector = jax.ShapeDtypeStruct((thin,), full)
    matrix = jax.ShapeDtypeStruct((half, thin), full)
    tall = jax.ShapeDtypeStruct((half, wide), full)
    rows = jax.ShapeDtypeStruct(rows_out.shape[1:], rows_out.dtype)
    inputs = (rows_out, wide_out, thin_out, vectors, up_bias_grad)
    return pl.pallas_call(
        publish_kernel,
        out_shape=(
            rows, rows, vector, vector, matrix, vector, matrix, matrix, vector, matrix, vector,
            vector, vector, tall, jax.ShapeDtypeStruct((wide,), full), tall, vector,
        ),
        in_specs=[anywhere] * 5,
        out_specs=(anywhere,) * 17,
        scratch_shapes=[
            *[pltpu.VMEM(value.shape, value.dtype) for value in inputs],
            *[pltpu.VMEM((thin,), full)] * 8,
            pltpu.VMEM((wide,), full),
            pltpu.SemaphoreType.DMA((5,)),
            pltpu.SemaphoreType.DMA((17,)),
        ],
        name="publish",
    )(*inputs)


def layer_call(tokens, out_grad, slots, vectors, up_bias, matrices):
    query_weight, up_weight, down_weight = matrices[0], matrices[4], matrices[5]
    low = jnp.bfloat16
    full = jnp.float32
    block, width = tokens.shape
    thin = query_weight.shape[0]
    wide = up_weight.shape[0]
    wide_pad = wide + -wide % 128
    heads = thin // HDIM
    replicas = lax.axis_size("replica")
    rows = width // replicas * 2
    chunks = wide // CW + 5
    half = rows // 2
    both = 2 * block
    vmem = pl.BlockSpec(memory_space=pltpu.VMEM)
    anywhere = pl.BlockSpec(memory_space=pl.ANY)
    dma = pltpu.SemaphoreType.DMA
    return pl.pallas_call(
        layer_kernel,
        out_shape=(
            jax.ShapeDtypeStruct((2,) + tokens.shape, low),
            jax.ShapeDtypeStruct((2, half, wide), full),
            jax.ShapeDtypeStruct((2, 2, half, thin), full),
            jax.ShapeDtypeStruct((8, thin), full),
            jax.ShapeDtypeStruct((1, wide_pad), full),
        ),
        in_specs=[anywhere] * 19,
        out_specs=(vmem,) * 5,
        scratch_shapes=[
            pltpu.VMEM((8, block), full),
            pltpu.VMEM((8, thin), full),
            pltpu.VMEM((8, wide), full),
            pltpu.VMEM((thin, width), low),
            pltpu.VMEM((thin, width), low),
            pltpu.VMEM((thin, width), low),
            pltpu.VMEM((thin, width), low),
            pltpu.VMEM((both, width), low),
            pltpu.VMEM((2, 8, block), full),
            pltpu.VMEM((8, thin), full),
            pltpu.VMEM((both, thin), low),
            pltpu.VMEM((both, thin), low),
            pltpu.VMEM((both, thin), low),
            pltpu.VMEM((2 * heads, block, block), low),
            pltpu.VMEM((block, width), full),
            pltpu.VMEM((block, width), full),
            pltpu.VMEM((block, width), full),
            pltpu.VMEM((block, width), full),
            pltpu.VMEM((4, block, width), low),
            pltpu.VMEM((4, block, width), low),
            pltpu.VMEM((2, both, width), low),
            pltpu.VMEM((2, both, wide_pad), low),
            pltpu.VMEM((2, both, width), low),
            pltpu.VMEM((2, both, thin), low),
            pltpu.VMEM((2, both, thin), low),
            pltpu.VMEM((both, width), low),
            pltpu.VMEM((both, wide_pad), low),
            pltpu.VMEM((both, width), low),
            pltpu.VMEM((both, width), low),
            pltpu.VMEM((both, thin), low),
            pltpu.VMEM((both, thin), low),
            pltpu.VMEM((EARLY, 2, 2, 2, rows, CW), low),
            pltpu.VMEM((chunks, 2, 2, rows, CW), low),
            pltpu.VMEM((chunks, 2, rows, CW), low),
            pltpu.VMEM((chunks, rows, CW), low),
            pltpu.VMEM((half, CW), full),
            pltpu.VMEM((8, width), full),
            pltpu.VMEM((2, 8, thin), full),
            pltpu.VMEM((8, thin), full),
            pltpu.VMEM((5, 8, thin), full),
            pltpu.VMEM((4, 8, thin), full),
            pltpu.VMEM((5, 1, wide_pad), full),
            pltpu.VMEM((4, 1, wide_pad), full),
            *[pltpu.VMEM((thin,), low)] * 8,
            *[pltpu.VMEM((block,), jnp.int32)] * 2,
            pltpu.VMEM((wide,), low),
            dma((11,)),
            dma((6,)),
            dma((18,)),
            dma((18,)),
            dma((14,)),
            dma((14,)),
            dma((chunks,)),
            dma((chunks,)),
            dma((chunks,)),
            dma((chunks,)),
            dma((chunks,)),
            dma((chunks,)),
            dma((chunks,)),
            dma((chunks,)),
            dma((8,)),
            dma((8,)),
        ],
        compiler_params=pltpu.CompilerParams(
            collective_id=0, has_side_effects=True, vmem_limit_bytes=67043328
        ),
        name="layer",
    )(tokens, out_grad, *slots, *vectors, up_bias, *matrices)


def whole_layer(
    tokens, out_grad, picture_ids, live_slots, ln1_gain, ln1_bias, query_weight, query_bias,
    key_weight, value_weight, value_bias, proj_weight, proj_bias, ln2_gain, ln2_bias, up_weight,
    up_bias, down_weight, down_bias,
):
    width = tokens.shape[1]
    if not by_kernel(lax.axis_size("replica"), width):
        return paired(
            tokens, out_grad, picture_ids, live_slots, ln1_gain, ln1_bias, query_weight,
            query_bias, key_weight, value_weight, value_bias, proj_weight, proj_bias, ln2_gain,
            ln2_bias, up_weight, up_bias, down_weight, down_bias,
        )
    packed = layer_call(
        tokens,
        out_grad,
        (picture_ids, live_slots),
        (ln1_gain, ln1_bias, proj_bias, ln2_gain, ln2_bias, down_bias, query_bias, value_bias),
        up_bias,
        (query_weight.T, key_weight.T, value_weight.T, proj_weight, up_weight.T, down_weight),
    )
    outs = list(publish_call(*packed))
    outs[9] = outs[9].T
    outs[15] = outs[15].T
    return tuple(outs)


def solution(mesh):
    in_specs = (
        P(("shard", "replica"), None),
        P(("shard", "replica"), None),
        P(("shard", "replica")),
        P(("shard", "replica")),
        P("shard"),
        P("shard"),
        P(None, "shard"),
        P("shard"),
        P(None, "shard"),
        P(None, "shard"),
        P("shard"),
        P("shard", None),
        P("shard"),
        P("shard"),
        P("shard"),
        P(None, "shard"),
        P("shard"),
        P("shard", None),
        P("shard"),
    )
    out_specs = (
        P(("shard", "replica"), None),
        P(("shard", "replica"), None),
        P("shard"),
        P("shard"),
        P("replica", "shard"),
        P("shard"),
        P("replica", "shard"),
        P("replica", "shard"),
        P("shard"),
        P("shard", "replica"),
        P("shard"),
        P("shard"),
        P("shard"),
        P("replica", "shard"),
        P("shard"),
        P("shard", "replica"),
        P("shard"),
    )
    return jax.shard_map(whole_layer, mesh=mesh, in_specs=in_specs, out_specs=out_specs, check_vma=False)
```

```python
import functools

import jax
import jax.numpy as jnp
from jax import lax
from jax.experimental import pallas as pl
from jax.experimental.pallas import tpu as pltpu
from jax.sharding import PartitionSpec as P

HDIM = 72
norm_eps = 1e-06
MESH = pl.DeviceIdType.MESH
CW = 256
SUB = 128
EARLY = 4
AHEAD = 6
LAGS = (3, 6, 8)
UNROLL = 2
GELU_SCALE = 0.7978845608028654


def norm_stats(values):
    centered = values - jnp.mean(values, axis=-1, keepdims=True)
    variance = jnp.mean(centered * centered, axis=-1, keepdims=True)
    inverse = lax.rsqrt(variance + norm_eps)
    return centered * inverse, inverse


def norm_grad(xhat, inverse, gain, grad):
    scaled = grad * gain
    return (
        scaled
        - jnp.mean(scaled, axis=-1, keepdims=True)
        - xhat * jnp.mean(scaled * xhat, axis=-1, keepdims=True)
    ) * inverse


def gelu_tanh(values):
    return jax.nn.gelu(values, approximate=True)


def product(left_side, right_side):
    return jnp.dot(left_side, right_side, preferred_element_type=jnp.float32)


def product_nt(left_side, right_side):
    return lax.dot_general(
        left_side, right_side, (((1,), (1,)), ((), ())), preferred_element_type=jnp.float32
    )


def product_tn(left_side, right_side):
    return lax.dot_general(
        left_side, right_side, (((0,), (0,)), ((), ())), preferred_element_type=jnp.float32
    )


def column_sums(matrix):
    return jnp.sum(matrix, axis=0, dtype=jnp.float32)


def swap(value):
    return lax.ppermute(value, "shard", [(0, 1), (1, 0)])


def split_heads(matrix, block_rows):
    return matrix.reshape(-1, block_rows, matrix.shape[1] // HDIM, HDIM)


def attend(queries, keys_in, values_in, allowed, block_rows):
    scores = jnp.einsum(
        "bqhd,bkhd->bhqk",
        split_heads(queries, block_rows),
        split_heads(keys_in, block_rows),
        preferred_element_type=jnp.float32,
    ) * HDIM ** (-0.5)
    scores = jnp.where(allowed[:, None, :, :], scores, -1e30)
    highest = jnp.max(scores, axis=-1, keepdims=True)
    scaled_exp = jnp.exp(scores - highest)
    totals = jnp.sum(scaled_exp, axis=-1, keepdims=True)
    probs = scaled_exp / totals
    mixed_out = jnp.einsum(
        "bhqk,bkhd->bqhd",
        probs.astype(jnp.bfloat16),
        split_heads(values_in, block_rows),
        preferred_element_type=jnp.float32,
    )
    return mixed_out.reshape(queries.shape), probs


def attend_back(queries, keys_in, values_in, grad_mixed, probs, block_rows):
    score_scale = HDIM ** (-0.5)
    split_grad = split_heads(grad_mixed, block_rows)
    grad_probs = jnp.einsum(
        "bqhd,bkhd->bhqk",
        split_grad,
        split_heads(values_in, block_rows),
        preferred_element_type=jnp.float32,
    )
    grad_scores = (
        probs * (grad_probs - jnp.sum(probs * grad_probs, axis=-1, keepdims=True))
    ).astype(jnp.bfloat16)
    grad_queries = (
        jnp.einsum(
            "bhqk,bkhd->bqhd",
            grad_scores,
            split_heads(keys_in, block_rows),
            preferred_element_type=jnp.float32,
        )
        * score_scale
    )
    grad_keys = (
        jnp.einsum(
            "bhqk,bqhd->bkhd",
            grad_scores,
            split_heads(queries, block_rows),
            preferred_element_type=jnp.float32,
        )
        * score_scale
    )
    grad_values = jnp.einsum(
        "bhqk,bqhd->bkhd",
        probs.astype(jnp.bfloat16),
        split_grad,
        preferred_element_type=jnp.float32,
    )
    return (
        grad_queries.astype(jnp.bfloat16).reshape(queries.shape),
        grad_keys.astype(jnp.bfloat16).reshape(queries.shape),
        grad_values.astype(jnp.bfloat16).reshape(queries.shape),
    )


def add_low(first, second):
    return (first.astype(jnp.float32) + second.astype(jnp.float32)).astype(jnp.bfloat16)


def by_kernel(replicas, width):
    return replicas == 2**4 and width % (replicas // 2 * 16) == 0


def plain_sums(block_out, tokens_grad, vectors, half, wide, query, key, value, proj, up, down):
    def owned(pair):
        return lax.psum_scatter(product_tn(*pair), "replica", scatter_dimension=0, tiled=True)

    vectors = lax.psum(vectors, "replica")

    def vector_at(i):
        return vectors[i * half : (i + 1) * half]

    return (
        block_out, tokens_grad, vector_at(0), vector_at(1), owned(query), vector_at(6),
        owned(key), owned(value), vector_at(7), owned(proj).T, vector_at(2), vector_at(3),
        vector_at(4), owned(up), vectors[8 * half : 8 * half + wide], owned(down).T, vector_at(5),
    )


def paired(
    tokens, out_grad, picture_ids, live_slots, ln1_gain, ln1_bias, query_weight, query_bias,
    key_weight, value_weight, value_bias, proj_weight, proj_bias, ln2_gain, ln2_bias, up_weight,
    up_bias, down_weight, down_bias,
):
    low = jnp.bfloat16
    full = jnp.float32
    rows, width = tokens.shape
    half = width // 2
    wide = up_weight.shape[1]
    shard = lax.axis_index("shard")
    own_vectors = jnp.stack([ln1_gain, ln1_bias, proj_bias, ln2_gain, ln2_bias, down_bias])
    slots = jnp.stack([picture_ids, live_slots])
    peer_tokens, peer_out, peer_vectors, peer_slots = (
        swap(tokens), swap(out_grad), swap(own_vectors), swap(slots),
    )
    gain_one, shift_one, bias_proj, gain_two, shift_two, bias_down = jnp.where(
        shard == 0,
        jnp.concatenate([own_vectors, peer_vectors], axis=1),
        jnp.concatenate([peer_vectors, own_vectors], axis=1),
    ).astype(full)
    slots = jnp.concatenate([slots, peer_slots], axis=1)
    alive = slots[1].astype(full)[:, None]
    ids = slots[0].reshape(2, rows)
    living = slots[1].reshape(2, rows)
    allowed = (ids[:, :, None] == ids[:, None, :]) & (living[:, None, :] == 1)
    all_tokens = jnp.concatenate([tokens, peer_tokens]).astype(full)
    all_out = jnp.concatenate([out_grad, peer_out]) * alive.astype(low)
    xhat_one, inverse_one = norm_stats(all_tokens)
    normed = (xhat_one * gain_one + shift_one).astype(low)
    queries = (product(normed, query_weight) + query_bias.astype(full)).astype(low)
    keys_all = product(normed, key_weight).astype(low)
    values_all = (product(normed, value_weight) + value_bias.astype(full)).astype(low)
    mixed_out, probs = attend(queries, keys_all, values_all, allowed, rows)
    mixed = mixed_out.astype(low)
    partial = product(mixed, proj_weight)
    hidden = all_tokens[:rows] + partial[:rows] + swap(partial[rows:].astype(low)).astype(full) + bias_proj
    xhat_two, inverse_two = norm_stats(hidden)
    normed_own = (xhat_two * gain_two + shift_two).astype(low)
    normed_two = jnp.concatenate([normed_own, swap(normed_own)])
    up_proj = product(normed_two, up_weight) + up_bias.astype(full)
    activated = gelu_tanh(up_proj).astype(low)
    grad_act = product_nt(all_out, down_weight)
    grad_up = jax.vjp(gelu_tanh, up_proj)[1](grad_act)[0].astype(low)
    partial = product_nt(grad_up, up_weight)
    grad_two = partial[:rows] + swap(partial[rows:].astype(low)).astype(full)
    partial = product(activated, down_weight)
    block_out = (
        (hidden + partial[:rows] + swap(partial[rows:].astype(low)).astype(full) + bias_down)
        * alive[:rows]
    ).astype(low)
    grad_hidden = all_out[:rows].astype(full) + norm_grad(xhat_two, inverse_two, gain_two, grad_two)
    hidden_own = grad_hidden.astype(low)
    hidden_low = jnp.concatenate([hidden_own, swap(hidden_own)])
    grad_mixed = product_nt(hidden_low, proj_weight).astype(low)
    grad_queries, grad_keys, grad_values = attend_back(
        queries, keys_all, values_all, grad_mixed, probs, rows
    )
    partial = (
        product_nt(grad_queries, query_weight)
        + product_nt(grad_keys, key_weight)
        + product_nt(grad_values, value_weight)
    )
    grad_one = partial[:rows] + swap(partial[rows:].astype(low)).astype(full)
    tokens_grad = (
        grad_hidden + norm_grad(xhat_one[:rows], inverse_one[:rows], gain_one, grad_one)
    ).astype(low)
    wholes = jnp.stack(
        [
            column_sums(grad_one * xhat_one[:rows]),
            column_sums(grad_one),
            column_sums(hidden_own),
            column_sums(grad_two * xhat_two),
            column_sums(grad_two),
            column_sums(all_out[:rows]),
        ]
    )
    mine = lax.dynamic_slice_in_dim(wholes, shard * half, half, 1)
    theirs = lax.dynamic_slice_in_dim(wholes, (1 - shard) * half, half, 1)
    halves = mine + swap(theirs)
    vectors = jnp.concatenate(
        [
            halves.reshape(-1),
            column_sums(grad_queries),
            column_sums(grad_values),
            column_sums(grad_up),
        ]
    )
    return plain_sums(
        block_out, tokens_grad, vectors, half, wide,
        (normed, grad_queries), (normed, grad_keys), (normed, grad_values),
        (hidden_low, mixed), (normed_two, grad_up), (all_out, activated),
    )


def take(ref, start, count):
    return ref.at[pl.ds(start, count)]


def layer_kernel(
    tokens_hbm,
    out_hbm,
    picture_ids,
    live_slots,
    ln1_gain,
    ln1_bias,
    proj_bias,
    ln2_gain,
    ln2_bias,
    down_bias,
    query_bias,
    value_bias,
    up_bias_in,
    query_hbm,
    key_hbm,
    value_hbm,
    proj_hbm,
    up_hbm,
    down_hbm,
    rows_hbm,
    wide_hbm,
    thin_hbm,
    rest_hbm,
    vectors_hbm,
    up_sum_hbm,
    rows_out,
    wide_out,
    thin_out,
    rest_out,
    slots,
    vectors,
    up_bias,
    query_weight,
    key_weight,
    value_weight,
    proj_weight,
    proj_other,
    mixed_other,
    all_tokens,
    all_slots,
    vectors_in,
    queries,
    keys_all,
    values_all,
    probs,
    hidden,
    own_part,
    own_down,
    part_send,
    part_in,
    wide_left,
    wide_right,
    thin_left,
    thin_first,
    thin_second,
    wide_left_in,
    wide_right_in,
    thin_left_in,
    thin_other_in,
    thin_first_in,
    thin_second_in,
    early,
    from_first,
    from_second,
    from_high,
    totals,
    halves,
    halves_in,
    vector_sum,
    vector_in,
    up_sum,
    up_in,
    flat_0,
    flat_1,
    flat_2,
    flat_3,
    flat_4,
    flat_5,
    flat_6,
    flat_7,
    flat_slots_0,
    flat_slots_1,
    flat_up,
    small_sem,
    load_sem,
    swap_send,
    swap_recv,
    proj_send,
    proj_recv,
    pair_send,
    pair_recv,
    first_send,
    first_recv,
    second_send,
    second_recv,
    high_send,
    high_recv,
    core_send,
    core_recv,
    vec_send,
    vec_recv,
    out_sem,
):
    full = jnp.float32
    low = jnp.bfloat16
    chunks = from_first.shape[0]
    rows = from_first.shape[3]
    early_chunks = early.shape[0]
    second_lag, high_lag, core_lag = LAGS
    block, width = tokens_hbm.shape
    thin = queries.shape[1]
    wide = up_bias.shape[1]
    heads = thin // HDIM
    score_scale = HDIM ** (-0.5)
    wide_chunks = chunks // 2 - 5
    wide_subs = 2 * wide_chunks
    half_block = block // 2
    strip = 32
    shard = lax.axis_index("shard")
    replica = lax.axis_index("replica")
    core = lax.rem(replica, 2)
    other = 1 - core
    y_bit = lax.rem(replica // 2, 2)
    low_bit = lax.rem(replica // 4, 2)
    high_bit = lax.rem(replica // 8, 2)
    twin = (1 - shard, replica)
    partner = (shard, replica + 1 - 2 * core)
    y_peer = (shard, replica + 2 - 4 * y_bit)
    low_peer = (shard, replica + 4 - 8 * low_bit)
    high_peer = (shard, replica + 8 - 16 * high_bit)
    peers = (partner, y_peer, low_peer, high_peer)
    vector_peers = (partner, high_peer, low_peer, y_peer)

    def remote(source, target, send, recv, peer):
        return pltpu.make_async_remote_copy(
            src_ref=source,
            dst_ref=target,
            send_sem=send,
            recv_sem=recv,
            device_id=peer,
            device_id_type=MESH,
        )

    def swapped(index, source, target):
        return remote(source, target, swap_send.at[index], swap_recv.at[index], twin)

    def paired_copy(index, source, target):
        return remote(source, target, pair_send.at[index], pair_recv.at[index], partner)

    loads = [
        pltpu.make_async_copy(source, target, load_sem.at[i])
        for i, (source, target) in enumerate(
            (
                (query_hbm, query_weight),
                (key_hbm, key_weight),
                (value_hbm, value_weight),
                (proj_hbm, proj_weight),
                (tokens_hbm, take(all_tokens, 0, block)),
                (out_hbm, wide_left.at[1, pl.ds(0, block)]),
            )
        )
    ]
    barrier = pltpu.get_barrier_semaphore()
    for peer in (twin,) + peers:
        pl.semaphore_signal(barrier, inc=1, device_id=peer, device_id_type=MESH)
    small = [
        pltpu.make_async_copy(source, target, small_sem.at[i])
        for i, (source, target) in enumerate(
            (
                (ln1_gain, flat_0),
                (ln1_bias, flat_1),
                (proj_bias, flat_2),
                (ln2_gain, flat_3),
                (ln2_bias, flat_4),
                (down_bias, flat_5),
                (query_bias, flat_6),
                (value_bias, flat_7),
                (picture_ids, flat_slots_0),
                (live_slots, flat_slots_1),
                (up_bias_in, flat_up),
            )
        )
    ]
    for load in small + loads[4:] + loads[:4]:
        load.start()
    slots[...] = jnp.zeros_like(slots)
    tokens_swaps = [
        swapped(
            index,
            tokens_hbm.at[pl.ds(j * half_block, half_block)],
            all_tokens.at[pl.ds(block + j * half_block, half_block)],
        )
        for j, index in ((0, 2), (1, 17))
    ]
    for load in small:
        load.wait()
    named = (flat_0, flat_1, flat_2, flat_3, flat_4, flat_5, flat_6, flat_7)
    for i, value in enumerate(named):
        vectors[i : i + 1, :] = value[...].astype(full).reshape(1, thin)
    slots[0:1, :] = flat_slots_0[...].astype(full).reshape(1, block)
    slots[1:2, :] = flat_slots_1[...].astype(full).reshape(1, block)
    up_bias[0:1, :] = flat_up[...].astype(full).reshape(1, wide)
    pl.semaphore_wait(barrier, 5)

    vectors_swap = swapped(0, vectors, vectors_in)
    slots_swap = swapped(1, slots, all_slots.at[1])
    out_swaps = [
        swapped(
            index,
            out_hbm.at[pl.ds(j * half_block, half_block)],
            wide_left.at[1, pl.ds(block + j * half_block, half_block)],
        )
        for j, index in ((0, 3), (1, 13))
    ]
    part_swaps = [
        [
            swapped(
                4 + 2 * i + j,
                part_send.at[i, pl.ds(j * half_block, half_block)],
                part_in.at[i, pl.ds(j * half_block, half_block)],
            )
            for j in range(2)
        ]
        for i in range(3)
    ]
    mixed_swaps = [
        swapped(
            10 + b,
            thin_second.at[1, pl.ds(b * block, block)],
            mixed_other.at[pl.ds((1 - b) * block, block)],
        )
        for b in range(2)
    ]
    quarter = thin // 4
    most = width // 9 * 5
    rest_width = width - most
    own_rows = pl.ds((2 * low_bit + y_bit) * quarter, quarter)
    own_columns = pl.ds(pl.multiple_of(core * rest_width, 128), most)
    proj_piece = proj_other.at[own_rows, own_columns]
    proj_swap = swapped(12, proj_hbm.at[own_rows, own_columns], proj_piece)
    proj_y = remote(proj_piece, proj_piece, proj_send.at[0], proj_recv.at[0], y_peer)
    proj_low_piece = proj_other.at[pl.ds(low_bit * 2 * quarter, 2 * quarter), own_columns]
    proj_low = remote(proj_low_piece, proj_low_piece, proj_send.at[1], proj_recv.at[1], low_peer)
    proj_core_piece = proj_other.at[:, pl.ds(pl.multiple_of(core * most, 128), rest_width)]
    proj_core = remote(proj_core_piece, proj_core_piece, proj_send.at[2], proj_recv.at[2], partner)
    hidden_swaps = [
        swapped(
            14 + j,
            thin_left.at[1, pl.ds(j * half_block, half_block)],
            thin_left.at[1, pl.ds(block + j * half_block, half_block)],
        )
        for j in range(2)
    ]
    halves_swap = swapped(16, halves.at[1], halves_in)

    def pair_rows(index, source, target, b):
        here = pl.ds(b * block, block)
        return paired_copy(index + b, source.at[here], target.at[here])

    def left_pair(b):
        return pair_rows(0, wide_left.at[other], wide_left_in, b)

    def right_pair(q):
        here = pl.ds(q * half_block, half_block)
        return paired_copy(2 + q, wide_right.at[other, here], wide_right_in.at[here])

    def normed_pair(b):
        return pair_rows(6, thin_left.at[0], thin_left_in, b)

    def other_pair(b):
        return pair_rows(8, thin_left.at[other], thin_other_in, b)

    def first_pair(b):
        return pair_rows(10, thin_first.at[other], thin_first_in, b)

    def second_pair(b):
        return pair_rows(12, thin_second.at[other], thin_second_in, b)

    vectors_swap.start()
    slots_swap.start()
    proj_swap.start()
    for copy in tokens_swaps:
        copy.start()

    all_slots[0] = slots[...]
    for load in loads[4:]:
        load.wait()

    def mask_rows(b, first, count):
        alive = jnp.transpose(all_slots[b])[first : first + count, 1:2].astype(low)
        at = pl.ds(b * block + first, count)
        wide_left[1, at, :] = wide_left[1, at, :] * alive

    mask_rows(0, 0, block)
    totals[...] = jnp.zeros_like(totals)
    up_sum[0] = jnp.zeros(up_sum.shape[1:], full)

    vectors_swap.wait_recv()
    slots_swap.wait_recv()
    here_half = vectors[...]
    there_half = vectors_in[...]
    joined = jnp.where(
        shard == 0,
        jnp.concatenate([here_half, there_half], axis=1),
        jnp.concatenate([there_half, here_half], axis=1),
    )
    gain_one, shift_one, bias_proj = joined[0:1], joined[1:2], joined[2:3]
    gain_two, shift_two, bias_down = joined[3:4], joined[4:5], joined[5:6]
    bias_query, bias_value = here_half[6:7], here_half[7:8]

    def strips(count, first, body):
        def step(i, carry):
            body(pl.ds(pl.multiple_of(first + i * strip, strip), strip))
            return carry

        lax.fori_loop(0, count // strip, step, 0, unroll=2)

    def is_low_first(j):
        return jnp.logical_and(lax.rem(j, 4) == 1, j < chunks - 1)

    def first_pick(grads, k, low_first):
        if low_first:
            return grads.at[k, :, 1 - low_bit], low_peer
        return grads.at[k, :, :, 1 - y_bit], y_peer

    def second_pick(grads, k, low_first):
        if low_first:
            return grads.at[k, :, low_bit, 1 - y_bit], y_peer
        return grads.at[k, :, 1 - low_bit, y_bit], low_peer

    def first_copy(grads, k, j, low_first):
        source, peer = first_pick(grads, k, low_first)
        return remote(source, from_first.at[j], first_send.at[j], first_recv.at[j], peer)

    def second_copy(grads, k, j, low_first):
        source, peer = second_pick(grads, k, low_first)
        return remote(source, from_second.at[j], second_send.at[j], second_recv.at[j], peer)

    def high_copy(grads, k, j):
        return remote(
            grads.at[k, 1 - high_bit, low_bit, y_bit],
            from_high.at[j],
            high_send.at[j],
            high_recv.at[j],
            high_peer,
        )

    def by_order(j, action):
        low_first = is_low_first(j)

        @pl.when(low_first)
        def _():
            action(True)

        @pl.when(jnp.logical_not(low_first))
        def _():
            action(False)

    def issue(grads, k, j):
        by_order(j, lambda low_first: first_copy(grads, k, j, low_first).start())

    def emit(grads, k, j, value, ahead):
        for i in range(2):
            piece = value[:, i * SUB : (i + 1) * SUB].astype(low)
            grads[k + i] = piece.reshape(grads.shape[1:])

            @pl.when(j + i < ahead)
            def _():
                issue(grads, k + i, j + i)

    def take_first(grads, k, j):
        def action(low_first):
            first_copy(grads, k, j, low_first).wait_recv()
            if low_first:
                grads[k, :, low_bit] = add_low(grads[k, :, low_bit], from_first[j])
            else:
                grads[k, :, :, y_bit] = add_low(grads[k, :, :, y_bit], from_first[j])
            second_copy(grads, k, j, low_first).start()

        by_order(j, action)

    def take_second(grads, k, j):
        by_order(j, lambda low_first: second_copy(grads, k, j, low_first).wait_recv())
        grads[k, :, low_bit, y_bit] = add_low(grads[k, :, low_bit, y_bit], from_second[j])
        high_copy(grads, k, j).start()

    def wide_place(slot, j):
        return wide_out.at[slot, :, pl.ds(pl.multiple_of(j * SUB, SUB), SUB)]

    def thin_place(slot, j):
        tile = j // 2 - wide_chunks
        start = tile // 2 * CW + lax.rem(j, 2) * SUB
        return thin_out.at[slot, lax.rem(tile, 2), :, pl.ds(pl.multiple_of(start, SUB), SUB)]

    def rest_place(slot, j):
        return rest_out.at[slot, j - (chunks - 2)]

    def rest_copy(summed, j):
        return remote(
            summed.at[j, other], rest_out.at[core, 0], core_send.at[j], core_recv.at[j], partner
        )

    def core_copy(summed, j, place):
        return remote(
            summed.at[j, other], place(core, j), core_send.at[j], core_recv.at[j], partner
        )

    def take_high(grads, k, j, summed):
        high_copy(grads, k, j).wait_recv()
        total = grads[k, high_bit, low_bit, y_bit].astype(full) + from_high[j].astype(full)
        summed[j] = total.reshape(2, rows // 2, SUB)
        for where, place in (
            (j < wide_subs, wide_place),
            (jnp.logical_and(j >= wide_subs, j < chunks - 2), thin_place),
            (j >= chunks - 2, rest_place),
        ):

            @pl.when(where)
            def _():
                core_copy(summed, j, place).start()
                place(core, j)[...] = summed[j, core]

    def wide_value(j):
        columns = pl.ds(pl.multiple_of(j * CW, CW), CW)
        return product_tn(wide_left[core], wide_right[core, :, columns]) + product_tn(
            wide_left_in[...], wide_right_in[:, columns]
        )

    def mlp_scope(up_weight, down_weight, grad_act, wide_sem):
        wide_loads = [
            pltpu.make_async_copy(up_hbm, up_weight, wide_sem.at[0]),
            pltpu.make_async_copy(down_hbm, down_weight, wide_sem.at[1]),
        ]
        for load in wide_loads:
            load.start()

        def attend_step(b, carry):
            here = pl.ds(pl.multiple_of(b * block, block), block)

            @pl.when(b == 0)
            def _():
                proj_swap.wait_recv()
                proj_y.start()

            @pl.when(b == 1)
            def _():
                proj_y.wait_recv()
                proj_low.start()
                for copy in tokens_swaps:
                    copy.wait_recv()

            def norm_strip(at):
                xhat, _ = norm_stats(all_tokens[at, :].astype(full))
                thin_left[0, at, :] = (xhat * gain_one + shift_one).astype(low)

            strips(block, b * block, norm_strip)

            @pl.when(b == 0)
            def _():
                for load in loads[:4]:
                    load.wait()

            normed = thin_left[0, here, :]
            queries[here, :] = (product_nt(normed, query_weight[...]) + bias_query).astype(low)
            keys_all[here, :] = product_nt(normed, key_weight[...]).astype(low)
            values_all[here, :] = (product_nt(normed, value_weight[...]) + bias_value).astype(low)
            marks = all_slots[b]
            across = jnp.where(marks[1:2] == 1.0, marks[0:1], -1.0)
            down_ids = jnp.transpose(marks)[:, 0:1]
            allowed = down_ids == across
            q_all = queries[here, :]
            k_all = keys_all[here, :]
            v_all = values_all[here, :]
            for h in range(heads):
                cut = slice(h * HDIM, (h + 1) * HDIM)
                scores = product_nt(q_all[:, cut], k_all[:, cut]) * score_scale
                scores = jnp.where(allowed, scores, -1e30)
                scaled = jnp.exp(scores - jnp.max(scores, axis=-1, keepdims=True))
                share = 1.0 / jnp.sum(scaled, axis=-1, keepdims=True)
                probs_low = (scaled * share).astype(low)
                probs[b * heads + h] = probs_low
                thin_second[1, here, cut] = product(probs_low, v_all[:, cut]).astype(low)
            for i in range(2):

                @pl.when(b == i)
                def _():
                    mixed_swaps[i].start()

            return carry

        lax.fori_loop(0, 2, attend_step, 0)
        for copy in out_swaps:
            copy.start()
        for b in range(2):
            normed_pair(b).start()
        proj_low.wait_recv()
        proj_core.start()
        for load in wide_loads:
            load.wait()
        out_rows = wide_left[1, pl.ds(0, block), :]

        def act_tile(t, carry):
            at = pl.ds(pl.multiple_of(t * 512, 512), 512)
            grad_act[:, at] = product_nt(out_rows, down_weight[at, :]).astype(low)
            return carry

        lax.fori_loop(0, wide_chunks // 2, act_tile, 0)
        rest_from = wide_chunks * CW
        rest = wide - rest_from
        rest_at = pl.ds(rest_from, rest)
        grad_act[:, rest_at] = product_nt(out_rows, down_weight[rest_at, :]).astype(low)
        pad_at = pl.ds(rest_from, CW // 2)
        wide_right[0, :, pad_at] = jnp.zeros((2 * block, CW // 2), low)
        wide_right[1, :, pad_at] = jnp.zeros((2 * block, CW // 2), low)

        def make_hidden(b):
            here = pl.ds(b * block, block)
            mixed_swaps[1 - b].wait_recv()
            mixed = thin_second[1, here, :]
            mixed_far = mixed_other[here, :]

            def proj_tile(n, inner):
                at = pl.ds(pl.multiple_of(n * 384, 384), 384)
                own_part[:, at] = product(mixed, proj_weight[:, at]) + product(
                    mixed_far, proj_other[:, at]
                )
                return inner

            lax.fori_loop(0, width // 384, proj_tile, 0)

            def hidden_strip(at):
                there = pl.ds(at.start + b * block, strip)
                value = all_tokens[there, :].astype(full) + own_part[at, :] + bias_proj
                if b == 0:
                    hidden[at, :] = value
                xhat, _ = norm_stats(value)
                wide_left[0, there, :] = (xhat * gain_two + shift_two).astype(low)

            strips(block, 0, hidden_strip)

        def gelu_parts(here, at):
            value = product_nt(wide_left[0, here, :], up_weight[at, :]) + up_bias[0:1, at]
            square = value * value
            bent = jnp.tanh(GELU_SCALE * value * (1.0 + 0.044715 * square))
            bulge = 0.5 * (1.0 + bent)
            wide_right[1, here, at] = (value * bulge).astype(low)
            return bulge + 0.5 * value * (1.0 - bent * bent) * (
                GELU_SCALE * (1.0 + 0.134145 * square)
            )

        def keep_grad(here, at, value):
            grad = value.astype(low)
            wide_right[0, here, at] = grad
            up_sum[0, :, at] += jnp.sum(grad.astype(full), axis=0, keepdims=True)

        def over_tiles(tile):
            def step(t, inner):
                tile(pl.ds(pl.multiple_of(t * CW, CW), CW))
                return inner

            lax.fori_loop(0, wide_chunks, step, 0, unroll=UNROLL)
            tile(rest_at)

        near = pl.ds(0, block)
        far = pl.ds(block, block)

        def far_tile(at):
            wide_right[0, far, at] = gelu_parts(far, at).astype(low)

        def near_tile(at):
            keep_grad(near, at, gelu_parts(near, at) * grad_act[:, at].astype(full))

        def back_tiles(b):
            grad_rows = wide_right[0, pl.ds(b * block, block), pl.ds(0, wide)]

            def back_tile(n, inner):
                at = pl.ds(pl.multiple_of(n * 384, 384), 384)
                value = product(grad_rows, up_weight[:, at])
                if b == 0:
                    own_part[:, at] = value
                else:
                    part_send[0, :, at] = value.astype(low)
                return inner

            lax.fori_loop(0, width // 384, back_tile, 0)

        proj_core.wait_recv()
        make_hidden(1)
        over_tiles(far_tile)
        make_hidden(0)
        left_pair(0).start()
        over_tiles(near_tile)
        for q in range(2):
            right_pair(q).start()
        back_tiles(0)
        for j in range(2):
            out_swaps[j].wait_recv()
            mask_rows(1, j * half_block, half_block)
            here = pl.ds(block + j * half_block, half_block)

            def slope_tile(at):
                grad = product_nt(wide_left[1, here, :], down_weight[at, :])
                keep_grad(here, at, wide_right[0, here, at].astype(full) * grad)

            if j == 1:
                left_pair(1).start()
            over_tiles(slope_tile)
            right_pair(2 + j).start()
        for i in range(2):
            left_pair(i).wait_recv()
        for q in range(4):
            right_pair(q).wait_recv()

        def early_step(j, inner):
            emit(early, 2 * j, 2 * j, wide_value(j), AHEAD)
            return inner

        lax.fori_loop(0, early_chunks // 2, early_step, 0)
        back_tiles(1)
        for copy in part_swaps[0]:
            copy.start()
        act_rows = wide_right[1, :, pl.ds(0, wide)]

        def down_tile(n, inner):
            at = pl.ds(pl.multiple_of(n * 384, 384), 384)
            value = product(act_rows, down_weight[:, at])
            own_down[:, at] = value[:block]
            part_send[1, :, at] = value[block:].astype(low)
            return inner

        lax.fori_loop(0, width // 384, down_tile, 0)

    pl.run_scoped(
        mlp_scope,
        pltpu.VMEM(up_hbm.shape, low),
        pltpu.VMEM(down_hbm.shape, low),
        pltpu.VMEM((block, wide_right.shape[2]), low),
        pltpu.SemaphoreType.DMA((2,)),
    )

    def grad_scope(grads, summed):
        def held(j, action):
            @pl.when(j < early_chunks)
            def _():
                action(early, j, j)

            @pl.when(j >= early_chunks)
            def _():
                action(grads, j - early_chunks, j)

        def pump_step(i, carry):
            @pl.when(i >= core_lag)
            def _():
                rest_copy(summed, i - core_lag).wait_recv()

            @pl.when(jnp.logical_and(i >= high_lag, i < chunks + high_lag))
            def _():
                held(i - high_lag, lambda ref, k, j: take_high(ref, k, j, summed))

            @pl.when(jnp.logical_and(i >= second_lag, i < chunks + second_lag))
            def _():
                held(i - second_lag, take_second)

            @pl.when(i < chunks)
            def _():
                held(i, take_first)

            return carry

        def pump(first, last, made=wide_subs):
            def step(i, carry):
                pump_step(i, carry)

                @pl.when(i + AHEAD < made)
                def _():
                    issue(grads, i + AHEAD - early_chunks, i + AHEAD)

                return carry

            lax.fori_loop(first, last, step, 0)

        def emit_late(j, value, ahead):
            emit(grads, j - early_chunks, j, value, ahead)

        def wide_step(j, carry):
            emit_late(2 * j, wide_value(j), AHEAD)
            return carry

        lax.fori_loop(early_chunks // 2, wide_chunks, wide_step, 0)
        pump(0, 3)

        for j in range(2):
            part_swaps[0][j].wait_recv()

            def norm_back_strip(at):
                grad = own_part[at, :] + part_in[0, at, :].astype(full)
                kept = hidden[at, :]
                xhat, inverse = norm_stats(kept)
                own_down[at, :] += kept
                out_rows = wide_left[1, at, :].astype(full)
                value = out_rows + norm_grad(xhat, inverse, gain_two, grad)
                hidden[at, :] = value
                rounded = value.astype(low)
                thin_left[1, at, :] = rounded
                totals[2:3] += column_sums(rounded.astype(full))[None]
                totals[3:4] += column_sums(grad * xhat)[None]
                totals[4:5] += column_sums(grad)[None]
                totals[5:6] += column_sums(out_rows)[None]

            strips(half_block, j * half_block, norm_back_strip)
            hidden_swaps[j].start()
        for copy in part_swaps[1]:
            copy.start()

        pump(3, 5)

        def back_step(b, carry):
            here = pl.ds(pl.multiple_of(b * block, block), block)

            @pl.when(b == 1)
            def _():
                for copy in hidden_swaps:
                    copy.wait_recv()
                for i in range(2):
                    other_pair(i).start()

            grad_mixed = product_nt(thin_left[1, here, :], proj_weight[...]).astype(low)
            q_all = queries[here, :]
            k_all = keys_all[here, :]
            v_all = values_all[here, :]
            for h in range(heads):
                cut = slice(h * HDIM, (h + 1) * HDIM)
                probs_low = probs[b * heads + h]
                probs_full = probs_low.astype(full)
                mixed_grad = grad_mixed[:, cut]
                grad_probs = product_nt(mixed_grad, v_all[:, cut])
                weighted = probs_full * grad_probs
                grad_scores = (
                    weighted - probs_full * jnp.sum(weighted, axis=-1, keepdims=True)
                ).astype(low)
                thin_first[0, here, cut] = (product(grad_scores, k_all[:, cut]) * score_scale).astype(low)
                thin_second[0, here, cut] = (
                    product_tn(grad_scores, q_all[:, cut]) * score_scale
                ).astype(low)
                thin_first[1, here, cut] = product_tn(probs_low, mixed_grad).astype(low)

            @pl.when(b == 0)
            def _():
                first_pair(0).start()
                second_pair(0).start()

            @pl.when(b == 1)
            def _():
                first_pair(1).start()
                second_pair(1).start()

            grad_q = thin_first[0, here, :]
            grad_k = thin_second[0, here, :]
            grad_v = thin_first[1, here, :]

            def normed_tile(n, inner):
                at = pl.ds(pl.multiple_of(n * 384, 384), 384)
                value = (
                    product(grad_q, query_weight[:, at])
                    + product(grad_k, key_weight[:, at])
                    + product(grad_v, value_weight[:, at])
                )

                @pl.when(b == 0)
                def _():
                    own_part[:, at] = value

                @pl.when(b == 1)
                def _():
                    part_send[2, :, at] = value.astype(low)

                return inner

            lax.fori_loop(0, width // 384, normed_tile, 0)
            pump(5 + 4 * b, 9 + 4 * b)
            return carry

        lax.fori_loop(0, 2, back_step, 0)
        for copy in part_swaps[2]:
            copy.start()

        for b in range(2):
            for pair in (normed_pair, other_pair, first_pair, second_pair):
                pair(b).wait_recv()

        def first_part(columns):
            return product_tn(thin_left[0], thin_first[core, :, columns]) + product_tn(
                thin_left_in[...], thin_first_in[:, columns]
            )

        def second_part(columns):
            return product_tn(thin_left[core], thin_second[core, :, columns]) + product_tn(
                thin_other_in[...], thin_second_in[:, columns]
            )

        def thin_step(j, carry):
            columns = pl.ds(pl.multiple_of(j * CW, CW), CW)
            emit_late(2 * (wide_chunks + 2 * j), first_part(columns), 13 + AHEAD)
            emit_late(2 * (wide_chunks + 2 * j + 1), second_part(columns), 13 + AHEAD)
            return carry

        lax.fori_loop(0, 2, thin_step, 0)
        thin_rest = pl.ds(2 * CW, thin - 2 * CW)
        wide_rest = pl.ds(wide_chunks * CW, CW // 2)
        emit_late(
            chunks - 2,
            jnp.concatenate(
                [
                    product_tn(wide_left[core], wide_right[core, :, wide_rest])
                    + product_tn(wide_left_in[...], wide_right_in[:, wide_rest]),
                    first_part(thin_rest),
                    second_part(thin_rest),
                ],
                axis=1,
            ),
            13 + AHEAD,
        )
        pump(13, 17, chunks)

        for copy in part_swaps[2]:
            copy.wait_recv()

        def final_strip(at):
            grad = own_part[at, :] + part_in[2, at, :].astype(full)
            xhat, inverse = norm_stats(all_tokens[at, :].astype(full))
            rows_out[1, at, :] = (
                hidden[at, :] + norm_grad(xhat, inverse, gain_one, grad)
            ).astype(low)
            totals[0:1] += column_sums(grad * xhat)[None]
            totals[1:2] += column_sums(grad)[None]

        strips(block, 0, final_strip)
        sums = totals[...]
        lower = sums[:, :thin]
        upper = sums[:, thin:]
        halves[0] = jnp.where(shard == 0, lower, upper)
        halves[1] = jnp.where(shard == 0, upper, lower)
        halves_swap.start()
        grad_query_bias = column_sums(thin_first[0].astype(full))[None]
        grad_value_bias = column_sums(thin_first[1].astype(full))[None]
        pump(17, 19, chunks)
        halves_swap.wait_recv()
        vector_sum[0] = halves[0] + halves_in[...]
        vector_sum[0, 6:7] = grad_query_bias
        vector_sum[0, 7:8] = grad_value_bias

        def vector_copies(i):
            return (
                remote(
                    vector_sum.at[i], vector_in.at[i], vec_send.at[2 * i], vec_recv.at[2 * i], vector_peers[i]
                ),
                remote(
                    up_sum.at[i], up_in.at[i], vec_send.at[2 * i + 1], vec_recv.at[2 * i + 1], vector_peers[i]
                ),
            )

        def vector_start(i):
            for copy in vector_copies(i):
                copy.start()

        def vector_finish(i):
            for copy in vector_copies(i):
                copy.wait_recv()
            vector_sum[i + 1] = vector_sum[i] + vector_in[i]
            up_sum[i + 1] = up_sum[i] + up_in[i]

        vector_start(0)
        for copy in part_swaps[1]:
            copy.wait_recv()

        def out_strip(at):
            value = own_down[at, :] + part_in[1, at, :].astype(full) + bias_down
            rows_out[0, at, :] = value.astype(low)

        strips(block, 0, out_strip)
        alive = jnp.transpose(all_slots[0])[:, 1:2].astype(low)
        rows_out[0] = rows_out[0] * alive

        row_copy = pltpu.make_async_copy(rows_out, rows_hbm, out_sem.at[0])
        row_copy.start()
        vector_finish(0)
        vector_start(1)
        pump(19, 22, chunks)
        vector_finish(1)
        vector_start(2)
        pump(22, chunks - 1, chunks)
        wide_copy = pltpu.make_async_copy(wide_out, wide_hbm, out_sem.at[1])
        wide_copy.start()
        vector_finish(2)
        vector_start(3)
        pump(chunks - 1, chunks + second_lag, chunks)
        vector_finish(3)
        last_copies = [
            pltpu.make_async_copy(vector_sum.at[4], vectors_hbm, out_sem.at[2]),
            pltpu.make_async_copy(up_sum.at[4], up_sum_hbm, out_sem.at[3]),
            pltpu.make_async_copy(thin_out, thin_hbm, out_sem.at[4]),
            pltpu.make_async_copy(rest_out, rest_hbm, out_sem.at[5]),
        ]
        for copy in last_copies[:2]:
            copy.start()
        pump(chunks + second_lag, chunks + core_lag, chunks)
        for copy in last_copies[2:]:
            copy.start()
        for copy in [row_copy, wide_copy] + last_copies:
            copy.wait()

        def drain(j, carry):
            held(j, lambda ref, k, i: first_copy(ref, k, i, False).wait_send())
            held(j, lambda ref, k, i: second_copy(ref, k, i, False).wait_send())
            held(j, lambda ref, k, i: high_copy(ref, k, i).wait_send())
            rest_copy(summed, j).wait_send()
            return carry

        lax.fori_loop(0, chunks, drain, 0)
        for i in range(4):
            for copy in vector_copies(i):
                copy.wait_send()

    pl.run_scoped(
        grad_scope,
        pltpu.VMEM((chunks - early_chunks, 2, 2, 2, rows, SUB), low),
        pltpu.VMEM((chunks, 2, rows // 2, SUB), full),
    )
    for copy in [vectors_swap, slots_swap, *tokens_swaps, *out_swaps, *mixed_swaps, proj_swap, halves_swap]:
        copy.wait_send()
    for copies in part_swaps + [hidden_swaps]:
        for copy in copies:
            copy.wait_send()
    for copy in (proj_y, proj_low, proj_core):
        copy.wait_send()
    for q in range(4):
        right_pair(q).wait_send()
    for b in range(2):
        for pair in (left_pair, normed_pair, other_pair, first_pair, second_pair):
            pair(b).wait_send()


def publish_kernel(rows_in, wide_in, thin_in, rest_in, vectors_in, up_in, *refs):
    outs, refs = refs[:17], refs[17:]
    rows_at, wide_at, thin_at, rest_at, vectors_at, up_at = refs[:6]
    flats, in_sem, out_sem = refs[6:15], refs[15], refs[16]
    wide_main = wide_in.shape[2]
    thin_main = thin_in.shape[3]
    wide, thin = wide_at.shape[2], thin_at.shape[3]
    loads = [
        pltpu.make_async_copy(source, target, in_sem.at[i])
        for i, (source, target) in enumerate(
            (
                (vectors_in, vectors_at),
                (up_in, up_at),
                (rest_in, rest_at),
                (rows_in, rows_at),
                (thin_in, thin_at.at[:, :, :, pl.ds(0, thin_main)]),
                (wide_in, wide_at.at[:, :, pl.ds(0, wide_main)]),
            )
        )
    ]
    for load in loads:
        load.start()
    stores = []

    def store(source, place):
        copy = pltpu.make_async_copy(source, outs[place], out_sem.at[place])
        copy.start()
        stores.append(copy)

    loads[0].wait()
    loads[1].wait()
    for i in range(8):
        flats[i][...] = vectors_at[i : i + 1, :].reshape(flats[i].shape)
    flats[8][...] = up_at[:, :wide].reshape(flats[8].shape)
    loads[2].wait()
    loads[3].wait()
    store(rows_at.at[0], 0)
    store(rows_at.at[1], 1)
    for slot in range(2):
        wide_at[slot, :, wide_main:] = rest_at[slot, 0, :, : wide - wide_main]
        for place in range(2):
            start = place * (thin - thin_main)
            thin_at[slot, place, :, thin_main:] = rest_at[
                slot, 1, :, start : start + thin - thin_main
            ]
    loads[4].wait()
    for i, place in enumerate((4, 6, 7, 9)):
        store(thin_at.at[i // 2, i % 2], place)
    loads[5].wait()
    store(wide_at.at[0], 13)
    store(wide_at.at[1], 15)
    for flat, place in zip(flats, (2, 3, 10, 11, 12, 16, 5, 8, 14)):
        store(flat, place)
    for copy in stores:
        copy.wait()


def publish_call(packed, wide):
    full = jnp.float32
    rows_out, wide_out, thin_out, rest_out, vectors, up_bias_grad = packed
    thin = vectors.shape[1]
    half = wide_out.shape[1]
    anywhere = pl.BlockSpec(memory_space=pl.ANY)
    vector = jax.ShapeDtypeStruct((thin,), full)
    matrix = jax.ShapeDtypeStruct((half, thin), full)
    tall = jax.ShapeDtypeStruct((half, wide), full)
    rows = jax.ShapeDtypeStruct(rows_out.shape[1:], rows_out.dtype)
    return pl.pallas_call(
        publish_kernel,
        out_shape=(
            rows, rows, vector, vector, matrix, vector, matrix, matrix, vector, matrix, vector,
            vector, vector, tall, jax.ShapeDtypeStruct((wide,), full), tall, vector,
        ),
        in_specs=[anywhere] * 6,
        out_specs=(anywhere,) * 17,
        scratch_shapes=[
            pltpu.VMEM(rows_out.shape, rows_out.dtype),
            pltpu.VMEM((2, half, wide), full),
            pltpu.VMEM((2, 2, half, thin), full),
            pltpu.VMEM(rest_out.shape, full),
            pltpu.VMEM(vectors.shape, full),
            pltpu.VMEM(up_bias_grad.shape, full),
            *[pltpu.VMEM((thin,), full)] * 8,
            pltpu.VMEM((wide,), full),
            pltpu.SemaphoreType.DMA((6,)),
            pltpu.SemaphoreType.DMA((17,)),
        ],
        name="publish",
    )(*packed)


def layer_call(tokens, out_grad, slots, vectors, up_bias, matrices):
    query_weight, up_weight, down_weight = matrices[0], matrices[4], matrices[5]
    low = jnp.bfloat16
    full = jnp.float32
    block, width = tokens.shape
    thin = query_weight.shape[0]
    wide = up_weight.shape[0]
    wide_pad = wide + -wide % 128
    heads = thin // HDIM
    replicas = lax.axis_size("replica")
    rows = width // replicas * 2
    wide_main = wide // CW * CW
    chunks = 2 * (wide // CW + 5)
    half = rows // 2
    both = 2 * block
    anywhere = pl.BlockSpec(memory_space=pl.ANY)
    dma = pltpu.SemaphoreType.DMA
    return pl.pallas_call(
        layer_kernel,
        out_shape=(
            jax.ShapeDtypeStruct((2,) + tokens.shape, low),
            jax.ShapeDtypeStruct((2, half, wide_main), full),
            jax.ShapeDtypeStruct((2, 2, half, 2 * CW), full),
            jax.ShapeDtypeStruct((2, 2, half, SUB), full),
            jax.ShapeDtypeStruct((8, thin), full),
            jax.ShapeDtypeStruct((1, wide_pad), full),
        ),
        in_specs=[anywhere] * 19,
        out_specs=(anywhere,) * 6,
        scratch_shapes=[
            pltpu.VMEM((2,) + tokens.shape, low),
            pltpu.VMEM((2, half, wide_main), full),
            pltpu.VMEM((2, 2, half, 2 * CW), full),
            pltpu.VMEM((2, 2, half, SUB), full),
            pltpu.VMEM((8, block), full),
            pltpu.VMEM((8, thin), full),
            pltpu.VMEM((8, wide), full),
            pltpu.VMEM((thin, width), low),
            pltpu.VMEM((thin, width), low),
            pltpu.VMEM((thin, width), low),
            pltpu.VMEM((thin, width), low),
            pltpu.VMEM((thin, width), low),
            pltpu.VMEM((both, thin), low),
            pltpu.VMEM((both, width), low),
            pltpu.VMEM((2, 8, block), full),
            pltpu.VMEM((8, thin), full),
            pltpu.VMEM((both, thin), low),
            pltpu.VMEM((both, thin), low),
            pltpu.VMEM((both, thin), low),
            pltpu.VMEM((2 * heads, block, block), low),
            pltpu.VMEM((block, width), full),
            pltpu.VMEM((block, width), full),
            pltpu.VMEM((block, width), full),
            pltpu.VMEM((3, block, width), low),
            pltpu.VMEM((3, block, width), low),
            pltpu.VMEM((2, both, width), low),
            pltpu.VMEM((2, both, wide_pad), low),
            pltpu.VMEM((2, both, width), low),
            pltpu.VMEM((2, both, thin), low),
            pltpu.VMEM((2, both, thin), low),
            pltpu.VMEM((both, width), low),
            pltpu.VMEM((both, wide_pad), low),
            pltpu.VMEM((both, width), low),
            pltpu.VMEM((both, width), low),
            pltpu.VMEM((both, thin), low),
            pltpu.VMEM((both, thin), low),
            pltpu.VMEM((EARLY, 2, 2, 2, rows, SUB), low),
            pltpu.VMEM((chunks, 2, 2, rows, SUB), low),
            pltpu.VMEM((chunks, 2, rows, SUB), low),
            pltpu.VMEM((chunks, rows, SUB), low),
            pltpu.VMEM((8, width), full),
            pltpu.VMEM((2, 8, thin), full),
            pltpu.VMEM((8, thin), full),
            pltpu.VMEM((5, 8, thin), full),
            pltpu.VMEM((4, 8, thin), full),
            pltpu.VMEM((5, 1, wide_pad), full),
            pltpu.VMEM((4, 1, wide_pad), full),
            *[pltpu.VMEM((thin,), low)] * 8,
            *[pltpu.VMEM((block,), jnp.int32)] * 2,
            pltpu.VMEM((wide,), low),
            dma((11,)),
            dma((6,)),
            dma((18,)),
            dma((18,)),
            dma((3,)),
            dma((3,)),
            dma((14,)),
            dma((14,)),
            dma((chunks,)),
            dma((chunks,)),
            dma((chunks,)),
            dma((chunks,)),
            dma((chunks,)),
            dma((chunks,)),
            dma((chunks,)),
            dma((chunks,)),
            dma((8,)),
            dma((8,)),
            dma((6,)),
        ],
        compiler_params=pltpu.CompilerParams(
            collective_id=0, has_side_effects=True, vmem_limit_bytes=67043328
        ),
        name="layer",
    )(tokens, out_grad, *slots, *vectors, up_bias, *matrices)


def whole_layer(
    tokens, out_grad, picture_ids, live_slots, ln1_gain, ln1_bias, query_weight, query_bias,
    key_weight, value_weight, value_bias, proj_weight, proj_bias, ln2_gain, ln2_bias, up_weight,
    up_bias, down_weight, down_bias,
):
    width = tokens.shape[1]
    if not by_kernel(lax.axis_size("replica"), width):
        return paired(
            tokens, out_grad, picture_ids, live_slots, ln1_gain, ln1_bias, query_weight,
            query_bias, key_weight, value_weight, value_bias, proj_weight, proj_bias, ln2_gain,
            ln2_bias, up_weight, up_bias, down_weight, down_bias,
        )
    packed = layer_call(
        tokens,
        out_grad,
        (picture_ids, live_slots),
        (ln1_gain, ln1_bias, proj_bias, ln2_gain, ln2_bias, down_bias, query_bias, value_bias),
        up_bias,
        (query_weight.T, key_weight.T, value_weight.T, proj_weight, up_weight.T, down_weight),
    )
    outs = list(publish_call(packed, up_weight.shape[1]))
    outs[9] = outs[9].T
    outs[15] = outs[15].T
    return tuple(outs)


def solution(mesh):
    in_specs = (
        P(("shard", "replica"), None),
        P(("shard", "replica"), None),
        P(("shard", "replica")),
        P(("shard", "replica")),
        P("shard"),
        P("shard"),
        P(None, "shard"),
        P("shard"),
        P(None, "shard"),
        P(None, "shard"),
        P("shard"),
        P("shard", None),
        P("shard"),
        P("shard"),
        P("shard"),
        P(None, "shard"),
        P("shard"),
        P("shard", None),
        P("shard"),
    )
    out_specs = (
        P(("shard", "replica"), None),
        P(("shard", "replica"), None),
        P("shard"),
        P("shard"),
        P("replica", "shard"),
        P("shard"),
        P("replica", "shard"),
        P("replica", "shard"),
        P("shard"),
        P("shard", "replica"),
        P("shard"),
        P("shard"),
        P("shard"),
        P("replica", "shard"),
        P("shard"),
        P("shard", "replica"),
        P("shard"),
    )
    return jax.shard_map(whole_layer, mesh=mesh, in_specs=in_specs, out_specs=out_specs, check_vma=False)
```

```python
import functools

import jax
import jax.numpy as jnp
from jax import lax
from jax.experimental import pallas as pl
from jax.experimental.pallas import tpu as pltpu
from jax.sharding import PartitionSpec as P

HDIM = 72
norm_eps = 1e-06
MESH = pl.DeviceIdType.MESH
CW = 256
SUB = 128
EARLY = 6
AHEAD = 6
FIRST = 2
LAGS = (3, 6, 8)
UNROLL = 2
GELU_SCALE = 0.7978845608028654


def norm_stats(values):
    centered = values - jnp.mean(values, axis=-1, keepdims=True)
    variance = jnp.mean(centered * centered, axis=-1, keepdims=True)
    inverse = lax.rsqrt(variance + norm_eps)
    return centered * inverse, inverse


def norm_grad(xhat, inverse, gain, grad):
    scaled = grad * gain
    return (
        scaled
        - jnp.mean(scaled, axis=-1, keepdims=True)
        - xhat * jnp.mean(scaled * xhat, axis=-1, keepdims=True)
    ) * inverse


def gelu_tanh(values):
    return jax.nn.gelu(values, approximate=True)


def product(left_side, right_side):
    return jnp.dot(left_side, right_side, preferred_element_type=jnp.float32)


def product_nt(left_side, right_side):
    return lax.dot_general(
        left_side, right_side, (((1,), (1,)), ((), ())), preferred_element_type=jnp.float32
    )


def product_tn(left_side, right_side):
    return lax.dot_general(
        left_side, right_side, (((0,), (0,)), ((), ())), preferred_element_type=jnp.float32
    )


def column_sums(matrix):
    return jnp.sum(matrix, axis=0, dtype=jnp.float32)


def swap(value):
    return lax.ppermute(value, "shard", [(0, 1), (1, 0)])


def split_heads(matrix, block_rows):
    return matrix.reshape(-1, block_rows, matrix.shape[1] // HDIM, HDIM)


def attend(queries, keys_in, values_in, allowed, block_rows):
    scores = jnp.einsum(
        "bqhd,bkhd->bhqk",
        split_heads(queries, block_rows),
        split_heads(keys_in, block_rows),
        preferred_element_type=jnp.float32,
    ) * HDIM ** (-0.5)
    scores = jnp.where(allowed[:, None, :, :], scores, -1e30)
    highest = jnp.max(scores, axis=-1, keepdims=True)
    scaled_exp = jnp.exp(scores - highest)
    totals = jnp.sum(scaled_exp, axis=-1, keepdims=True)
    probs = scaled_exp / totals
    mixed_out = jnp.einsum(
        "bhqk,bkhd->bqhd",
        probs.astype(jnp.bfloat16),
        split_heads(values_in, block_rows),
        preferred_element_type=jnp.float32,
    )
    return mixed_out.reshape(queries.shape), probs


def attend_back(queries, keys_in, values_in, grad_mixed, probs, block_rows):
    score_scale = HDIM ** (-0.5)
    split_grad = split_heads(grad_mixed, block_rows)
    grad_probs = jnp.einsum(
        "bqhd,bkhd->bhqk",
        split_grad,
        split_heads(values_in, block_rows),
        preferred_element_type=jnp.float32,
    )
    grad_scores = (
        probs * (grad_probs - jnp.sum(probs * grad_probs, axis=-1, keepdims=True))
    ).astype(jnp.bfloat16)
    grad_queries = (
        jnp.einsum(
            "bhqk,bkhd->bqhd",
            grad_scores,
            split_heads(keys_in, block_rows),
            preferred_element_type=jnp.float32,
        )
        * score_scale
    )
    grad_keys = (
        jnp.einsum(
            "bhqk,bqhd->bkhd",
            grad_scores,
            split_heads(queries, block_rows),
            preferred_element_type=jnp.float32,
        )
        * score_scale
    )
    grad_values = jnp.einsum(
        "bhqk,bqhd->bkhd",
        probs.astype(jnp.bfloat16),
        split_grad,
        preferred_element_type=jnp.float32,
    )
    return (
        grad_queries.astype(jnp.bfloat16).reshape(queries.shape),
        grad_keys.astype(jnp.bfloat16).reshape(queries.shape),
        grad_values.astype(jnp.bfloat16).reshape(queries.shape),
    )


def add_low(first, second):
    return (first.astype(jnp.float32) + second.astype(jnp.float32)).astype(jnp.bfloat16)


def by_kernel(replicas, width):
    return replicas == 2**4 and width % (replicas // 2 * 16) == 0


def plain_sums(block_out, tokens_grad, vectors, half, wide, query, key, value, proj, up, down):
    def owned(pair):
        return lax.psum_scatter(product_tn(*pair), "replica", scatter_dimension=0, tiled=True)

    vectors = lax.psum(vectors, "replica")

    def vector_at(i):
        return vectors[i * half : (i + 1) * half]

    return (
        block_out, tokens_grad, vector_at(0), vector_at(1), owned(query), vector_at(6),
        owned(key), owned(value), vector_at(7), owned(proj).T, vector_at(2), vector_at(3),
        vector_at(4), owned(up), vectors[8 * half : 8 * half + wide], owned(down).T, vector_at(5),
    )


def paired(
    tokens, out_grad, picture_ids, live_slots, ln1_gain, ln1_bias, query_weight, query_bias,
    key_weight, value_weight, value_bias, proj_weight, proj_bias, ln2_gain, ln2_bias, up_weight,
    up_bias, down_weight, down_bias,
):
    low = jnp.bfloat16
    full = jnp.float32
    rows, width = tokens.shape
    half = width // 2
    wide = up_weight.shape[1]
    shard = lax.axis_index("shard")
    own_vectors = jnp.stack([ln1_gain, ln1_bias, proj_bias, ln2_gain, ln2_bias, down_bias])
    slots = jnp.stack([picture_ids, live_slots])
    peer_tokens, peer_out, peer_vectors, peer_slots = (
        swap(tokens), swap(out_grad), swap(own_vectors), swap(slots),
    )
    gain_one, shift_one, bias_proj, gain_two, shift_two, bias_down = jnp.where(
        shard == 0,
        jnp.concatenate([own_vectors, peer_vectors], axis=1),
        jnp.concatenate([peer_vectors, own_vectors], axis=1),
    ).astype(full)
    slots = jnp.concatenate([slots, peer_slots], axis=1)
    alive = slots[1].astype(full)[:, None]
    ids = slots[0].reshape(2, rows)
    living = slots[1].reshape(2, rows)
    allowed = (ids[:, :, None] == ids[:, None, :]) & (living[:, None, :] == 1)
    all_tokens = jnp.concatenate([tokens, peer_tokens]).astype(full)
    all_out = jnp.concatenate([out_grad, peer_out]) * alive.astype(low)
    xhat_one, inverse_one = norm_stats(all_tokens)
    normed = (xhat_one * gain_one + shift_one).astype(low)
    queries = (product(normed, query_weight) + query_bias.astype(full)).astype(low)
    keys_all = product(normed, key_weight).astype(low)
    values_all = (product(normed, value_weight) + value_bias.astype(full)).astype(low)
    mixed_out, probs = attend(queries, keys_all, values_all, allowed, rows)
    mixed = mixed_out.astype(low)
    partial = product(mixed, proj_weight)
    hidden = all_tokens[:rows] + partial[:rows] + swap(partial[rows:].astype(low)).astype(full) + bias_proj
    xhat_two, inverse_two = norm_stats(hidden)
    normed_own = (xhat_two * gain_two + shift_two).astype(low)
    normed_two = jnp.concatenate([normed_own, swap(normed_own)])
    up_proj = product(normed_two, up_weight) + up_bias.astype(full)
    activated = gelu_tanh(up_proj).astype(low)
    grad_act = product_nt(all_out, down_weight)
    grad_up = jax.vjp(gelu_tanh, up_proj)[1](grad_act)[0].astype(low)
    partial = product_nt(grad_up, up_weight)
    grad_two = partial[:rows] + swap(partial[rows:].astype(low)).astype(full)
    partial = product(activated, down_weight)
    block_out = (
        (hidden + partial[:rows] + swap(partial[rows:].astype(low)).astype(full) + bias_down)
        * alive[:rows]
    ).astype(low)
    grad_hidden = all_out[:rows].astype(full) + norm_grad(xhat_two, inverse_two, gain_two, grad_two)
    hidden_own = grad_hidden.astype(low)
    hidden_low = jnp.concatenate([hidden_own, swap(hidden_own)])
    grad_mixed = product_nt(hidden_low, proj_weight).astype(low)
    grad_queries, grad_keys, grad_values = attend_back(
        queries, keys_all, values_all, grad_mixed, probs, rows
    )
    partial = (
        product_nt(grad_queries, query_weight)
        + product_nt(grad_keys, key_weight)
        + product_nt(grad_values, value_weight)
    )
    grad_one = partial[:rows] + swap(partial[rows:].astype(low)).astype(full)
    tokens_grad = (
        grad_hidden + norm_grad(xhat_one[:rows], inverse_one[:rows], gain_one, grad_one)
    ).astype(low)
    wholes = jnp.stack(
        [
            column_sums(grad_one * xhat_one[:rows]),
            column_sums(grad_one),
            column_sums(hidden_own),
            column_sums(grad_two * xhat_two),
            column_sums(grad_two),
            column_sums(all_out[:rows]),
        ]
    )
    mine = lax.dynamic_slice_in_dim(wholes, shard * half, half, 1)
    theirs = lax.dynamic_slice_in_dim(wholes, (1 - shard) * half, half, 1)
    halves = mine + swap(theirs)
    vectors = jnp.concatenate(
        [
            halves.reshape(-1),
            column_sums(grad_queries),
            column_sums(grad_values),
            column_sums(grad_up),
        ]
    )
    return plain_sums(
        block_out, tokens_grad, vectors, half, wide,
        (normed, grad_queries), (normed, grad_keys), (normed, grad_values),
        (hidden_low, mixed), (normed_two, grad_up), (all_out, activated),
    )


def take(ref, start, count):
    return ref.at[pl.ds(start, count)]


def layer_kernel(
    tokens_hbm,
    out_hbm,
    picture_ids,
    live_slots,
    ln1_gain,
    ln1_bias,
    proj_bias,
    ln2_gain,
    ln2_bias,
    down_bias,
    query_bias,
    value_bias,
    up_bias_in,
    query_hbm,
    key_hbm,
    value_hbm,
    proj_hbm,
    up_hbm,
    down_hbm,
    rows_hbm,
    wide_hbm,
    thin_hbm,
    rest_hbm,
    vectors_hbm,
    up_sum_hbm,
    rows_out,
    wide_out,
    thin_out,
    rest_out,
    slots,
    vectors,
    up_bias,
    query_weight,
    key_weight,
    value_weight,
    proj_weight,
    proj_other,
    all_tokens,
    all_slots,
    vectors_in,
    queries,
    keys_all,
    values_all,
    probs,
    hidden,
    own_part,
    own_down,
    part_send,
    part_in,
    wide_left,
    wide_right,
    thin_left,
    thin_first,
    thin_second,
    wide_left_in,
    wide_right_in,
    rest_right_in,
    thin_left_in,
    thin_other_in,
    thin_first_in,
    thin_second_in,
    early,
    from_first,
    from_second,
    from_high,
    totals,
    halves,
    halves_in,
    vector_sum,
    vector_in,
    up_sum,
    up_in,
    flat_0,
    flat_1,
    flat_2,
    flat_3,
    flat_4,
    flat_5,
    flat_6,
    flat_7,
    flat_slots_0,
    flat_slots_1,
    flat_up,
    small_sem,
    load_sem,
    swap_send,
    swap_recv,
    proj_send,
    proj_recv,
    pair_send,
    pair_recv,
    first_send,
    first_recv,
    second_send,
    second_recv,
    high_send,
    high_recv,
    core_send,
    core_recv,
    vec_send,
    vec_recv,
    out_sem,
):
    full = jnp.float32
    low = jnp.bfloat16
    chunks = from_first.shape[0]
    rows = from_first.shape[3]
    early_chunks = early.shape[0]
    second_lag, high_lag, core_lag = LAGS
    block, width = tokens_hbm.shape
    thin = queries.shape[1]
    wide = up_bias.shape[1]
    heads = thin // HDIM
    score_scale = HDIM ** (-0.5)
    wide_chunks = chunks // 2 - 5
    wide_subs = 2 * wide_chunks
    half_block = block // 2
    strip = 32
    shard = lax.axis_index("shard")
    replica = lax.axis_index("replica")
    core = lax.rem(replica, 2)
    other = 1 - core
    y_bit = lax.rem(replica // 2, 2)
    low_bit = lax.rem(replica // 4, 2)
    high_bit = lax.rem(replica // 8, 2)
    twin = (1 - shard, replica)
    partner = (shard, replica + 1 - 2 * core)
    y_peer = (shard, replica + 2 - 4 * y_bit)
    low_peer = (shard, replica + 4 - 8 * low_bit)
    high_peer = (shard, replica + 8 - 16 * high_bit)
    peers = (partner, y_peer, low_peer, high_peer)
    vector_peers = (partner, high_peer, low_peer, y_peer)

    def remote(source, target, send, recv, peer):
        return pltpu.make_async_remote_copy(
            src_ref=source,
            dst_ref=target,
            send_sem=send,
            recv_sem=recv,
            device_id=peer,
            device_id_type=MESH,
        )

    def swapped(index, source, target):
        return remote(source, target, swap_send.at[index], swap_recv.at[index], twin)

    def paired_copy(index, source, target):
        return remote(source, target, pair_send.at[index], pair_recv.at[index], partner)

    loads = [
        pltpu.make_async_copy(source, target, load_sem.at[i])
        for i, (source, target) in enumerate(
            (
                (query_hbm, query_weight),
                (key_hbm, key_weight),
                (value_hbm, value_weight),
                (proj_hbm, proj_weight),
                (tokens_hbm, take(all_tokens, 0, block)),
                (out_hbm, wide_left.at[1, pl.ds(0, block)]),
            )
        )
    ]
    barrier = pltpu.get_barrier_semaphore()
    for peer in (twin,) + peers:
        pl.semaphore_signal(barrier, inc=1, device_id=peer, device_id_type=MESH)
    small = [
        pltpu.make_async_copy(source, target, small_sem.at[i])
        for i, (source, target) in enumerate(
            (
                (ln1_gain, flat_0),
                (ln1_bias, flat_1),
                (proj_bias, flat_2),
                (ln2_gain, flat_3),
                (ln2_bias, flat_4),
                (down_bias, flat_5),
                (query_bias, flat_6),
                (value_bias, flat_7),
                (picture_ids, flat_slots_0),
                (live_slots, flat_slots_1),
                (up_bias_in, flat_up),
            )
        )
    ]
    for load in small + loads[4:] + loads[:4]:
        load.start()
    slots[...] = jnp.zeros_like(slots)
    tokens_swaps = [
        swapped(
            index,
            tokens_hbm.at[pl.ds(j * half_block, half_block)],
            all_tokens.at[pl.ds(block + j * half_block, half_block)],
        )
        for j, index in ((0, 2), (1, 17))
    ]
    for load in small:
        load.wait()
    named = (flat_0, flat_1, flat_2, flat_3, flat_4, flat_5, flat_6, flat_7)
    for i, value in enumerate(named):
        vectors[i : i + 1, :] = value[...].astype(full).reshape(1, thin)
    slots[0:1, :] = flat_slots_0[...].astype(full).reshape(1, block)
    slots[1:2, :] = flat_slots_1[...].astype(full).reshape(1, block)
    up_bias[0:1, :] = flat_up[...].astype(full).reshape(1, wide)
    pl.semaphore_wait(barrier, 5)

    vectors_swap = swapped(0, vectors, vectors_in)
    slots_swap = swapped(1, slots, all_slots.at[1])
    out_swaps = [
        swapped(
            index,
            out_hbm.at[pl.ds(j * half_block, half_block)],
            wide_left.at[1, pl.ds(block + j * half_block, half_block)],
        )
        for j, index in ((0, 3), (1, 13))
    ]
    part_swaps = [
        [
            swapped(
                4 + 2 * i + j,
                part_send.at[i % 2, pl.ds(j * half_block, half_block)],
                part_in.at[i % 2, pl.ds(j * half_block, half_block)],
            )
            for j in range(2)
        ]
        for i in range(3)
    ]
    mixed_swaps = [
        swapped(
            10 + b,
            thin_second.at[1, pl.ds(b * block, block)],
            thin_first_in.at[pl.ds((1 - b) * block, block)],
        )
        for b in range(2)
    ]
    quarter = thin // 4
    most = width // 9 * 5
    rest_width = width - most
    own_rows = pl.ds((2 * low_bit + y_bit) * quarter, quarter)
    own_columns = pl.ds(pl.multiple_of(core * rest_width, 128), most)
    proj_piece = proj_other.at[own_rows, own_columns]
    proj_swap = swapped(12, proj_hbm.at[own_rows, own_columns], proj_piece)
    proj_y = remote(proj_piece, proj_piece, proj_send.at[0], proj_recv.at[0], y_peer)
    proj_low_piece = proj_other.at[pl.ds(low_bit * 2 * quarter, 2 * quarter), own_columns]
    proj_low = remote(proj_low_piece, proj_low_piece, proj_send.at[1], proj_recv.at[1], low_peer)
    proj_core_piece = proj_other.at[:, pl.ds(pl.multiple_of(core * most, 128), rest_width)]
    proj_core = remote(proj_core_piece, proj_core_piece, proj_send.at[2], proj_recv.at[2], partner)
    hidden_swaps = [
        swapped(
            14 + j,
            thin_left.at[1, pl.ds(j * half_block, half_block)],
            thin_left.at[1, pl.ds(block + j * half_block, half_block)],
        )
        for j in range(2)
    ]
    halves_swap = swapped(16, halves.at[1], halves_in)

    def pair_rows(index, source, target, b):
        here = pl.ds(b * block, block)
        return paired_copy(index + b, source.at[here], target.at[here])

    half_wide = wide_right_in.shape[2]
    pieces = ((0, block), (block, half_block), (block + half_block, half_block))

    def out_pair(p):
        here = pl.ds(*pieces[p])
        return paired_copy(p, wide_left.at[1, here], wide_left_in.at[1, here])

    def left_pair(b):
        return pair_rows(3, wide_left.at[0], wide_left_in.at[0], b)

    def theirs(kind, here):
        columns = pl.ds(pl.multiple_of(other * half_wide, CW), half_wide)
        return wide_right.at[kind, here, columns]

    def act_pair(b):
        here = pl.ds(b * block, block)
        return paired_copy(5 + b, theirs(1, here), wide_right_in.at[1, here])

    def grad_pair(p):
        here = pl.ds(*pieces[p])
        return paired_copy(7 + p, theirs(0, here), wide_right_in.at[0, here])

    def rest_pair():
        source = wide_right.at[other, :, pl.ds(2 * half_wide, SUB)]
        return paired_copy(10, source, rest_right_in)

    def normed_pair(b):
        return pair_rows(11, thin_left.at[0], thin_left_in, b)

    def other_pair(b):
        return pair_rows(13, thin_left.at[other], thin_other_in, b)

    def first_pair(b):
        return pair_rows(15, thin_first.at[other], thin_first_in, b)

    def second_pair(b):
        return pair_rows(17, thin_second.at[other], thin_second_in, b)

    vectors_swap.start()
    slots_swap.start()
    proj_swap.start()
    for copy in tokens_swaps:
        copy.start()

    all_slots[0] = slots[...]
    for load in loads[4:]:
        load.wait()

    def mask_rows(b, first, count):
        alive = jnp.transpose(all_slots[b])[first : first + count, 1:2].astype(low)
        at = pl.ds(b * block + first, count)
        wide_left[1, at, :] = wide_left[1, at, :] * alive

    mask_rows(0, 0, block)
    totals[...] = jnp.zeros_like(totals)
    up_sum[0] = jnp.zeros(up_sum.shape[1:], full)

    vectors_swap.wait_recv()
    slots_swap.wait_recv()
    here_half = vectors[...]
    there_half = vectors_in[...]
    joined = jnp.where(
        shard == 0,
        jnp.concatenate([here_half, there_half], axis=1),
        jnp.concatenate([there_half, here_half], axis=1),
    )
    gain_one, shift_one, bias_proj = joined[0:1], joined[1:2], joined[2:3]
    gain_two, shift_two, bias_down = joined[3:4], joined[4:5], joined[5:6]
    bias_query, bias_value = here_half[6:7], here_half[7:8]

    def strips(count, first, body):
        def step(i, carry):
            body(pl.ds(pl.multiple_of(first + i * strip, strip), strip))
            return carry

        lax.fori_loop(0, count // strip, step, 0, unroll=2)

    def is_low_first(j):
        return jnp.logical_and(lax.rem(j, 4) == 1, j < chunks - 1)

    def first_pick(grads, k, low_first):
        if low_first:
            return grads.at[k, :, 1 - low_bit], low_peer
        return grads.at[k, :, :, 1 - y_bit], y_peer

    def second_pick(grads, k, low_first):
        if low_first:
            return grads.at[k, :, low_bit, 1 - y_bit], y_peer
        return grads.at[k, :, 1 - low_bit, y_bit], low_peer

    def first_copy(grads, k, j, low_first):
        source, peer = first_pick(grads, k, low_first)
        return remote(source, from_first.at[j], first_send.at[j], first_recv.at[j], peer)

    def second_copy(grads, k, j, low_first):
        source, peer = second_pick(grads, k, low_first)
        return remote(source, from_second.at[j], second_send.at[j], second_recv.at[j], peer)

    def high_copy(grads, k, j):
        return remote(
            grads.at[k, 1 - high_bit, low_bit, y_bit],
            from_high.at[j],
            high_send.at[j],
            high_recv.at[j],
            high_peer,
        )

    def by_order(j, action):
        low_first = is_low_first(j)

        @pl.when(low_first)
        def _():
            action(True)

        @pl.when(jnp.logical_not(low_first))
        def _():
            action(False)

    def issue(grads, k, j):
        by_order(j, lambda low_first: first_copy(grads, k, j, low_first).start())

    def emit(grads, k, j, value, ahead):
        for i in range(2):
            piece = value[:, i * SUB : (i + 1) * SUB].astype(low)
            grads[k + i] = piece.reshape(grads.shape[1:])

            @pl.when(j + i < ahead)
            def _():
                issue(grads, k + i, j + i)

    def take_first(grads, k, j):
        def action(low_first):
            first_copy(grads, k, j, low_first).wait_recv()
            if low_first:
                grads[k, :, low_bit] = add_low(grads[k, :, low_bit], from_first[j])
            else:
                grads[k, :, :, y_bit] = add_low(grads[k, :, :, y_bit], from_first[j])
            second_copy(grads, k, j, low_first).start()

        by_order(j, action)

    def take_second(grads, k, j):
        by_order(j, lambda low_first: second_copy(grads, k, j, low_first).wait_recv())
        grads[k, :, low_bit, y_bit] = add_low(grads[k, :, low_bit, y_bit], from_second[j])
        high_copy(grads, k, j).start()

    def wide_place(slot, j):
        tile = j // 2
        start = slot * half_wide + lax.rem(tile, wide_chunks // 2) * CW + lax.rem(j, 2) * SUB
        kind = jnp.where(tile < wide_chunks // 2, 1, 0)
        return wide_out.at[kind, :, pl.ds(pl.multiple_of(start, SUB), SUB)]

    def thin_place(slot, j):
        tile = j // 2 - wide_chunks
        start = tile // 2 * CW + lax.rem(j, 2) * SUB
        return thin_out.at[slot, lax.rem(tile, 2), :, pl.ds(pl.multiple_of(start, SUB), SUB)]

    def rest_place(slot, j):
        return rest_out.at[slot, j - (chunks - 2)]

    def rest_copy(summed, j):
        return remote(
            summed.at[j, other], rest_out.at[core, 0], core_send.at[j], core_recv.at[j], partner
        )

    def core_copy(summed, j, place):
        return remote(
            summed.at[j, other], place(core, j), core_send.at[j], core_recv.at[j], partner
        )

    def take_high(grads, k, j, summed):
        high_copy(grads, k, j).wait_recv()
        total = grads[k, high_bit, low_bit, y_bit].astype(full) + from_high[j].astype(full)
        summed[j] = total.reshape(2, rows // 2, SUB)
        for where, place in (
            (j < wide_subs, wide_place),
            (jnp.logical_and(j >= wide_subs, j < chunks - 2), thin_place),
            (j >= chunks - 2, rest_place),
        ):

            @pl.when(where)
            def _():
                core_copy(summed, j, place).start()
                place(core, j)[...] = summed[j, core]

    def wide_value(tile, before=None):
        kind = jnp.where(tile < wide_chunks // 2, 1, 0)
        start = lax.rem(tile, wide_chunks // 2) * CW
        mine = pl.ds(pl.multiple_of(core * half_wide + start, CW), CW)
        value = product_tn(wide_left[kind], wide_right[kind, :, mine])
        if before is not None:
            before()
        columns = pl.ds(pl.multiple_of(start, CW), CW)
        return value + product_tn(wide_left_in[kind], wide_right_in[kind, :, columns])

    def mlp_scope(up_weight, down_weight, wide_sem):
        wide_loads = [
            pltpu.make_async_copy(up_hbm, up_weight, wide_sem.at[0]),
            pltpu.make_async_copy(down_hbm, down_weight, wide_sem.at[1]),
        ]
        for load in wide_loads:
            load.start()

        def attend_step(b, carry):
            here = pl.ds(pl.multiple_of(b * block, block), block)

            @pl.when(b == 0)
            def _():
                proj_swap.wait_recv()
                proj_y.start()

            @pl.when(b == 1)
            def _():
                proj_y.wait_recv()
                proj_low.start()
                for copy in tokens_swaps:
                    copy.wait_recv()

            def norm_strip(at):
                xhat, _ = norm_stats(all_tokens[at, :].astype(full))
                thin_left[0, at, :] = (xhat * gain_one + shift_one).astype(low)

            strips(block, b * block, norm_strip)

            @pl.when(b == 0)
            def _():
                for load in loads[:4]:
                    load.wait()

            normed = thin_left[0, here, :]
            queries[here, :] = (product_nt(normed, query_weight[...]) + bias_query).astype(low)
            keys_all[here, :] = product_nt(normed, key_weight[...]).astype(low)
            values_all[here, :] = (product_nt(normed, value_weight[...]) + bias_value).astype(low)
            marks = all_slots[b]
            across = jnp.where(marks[1:2] == 1.0, marks[0:1], -1.0)
            down_ids = jnp.transpose(marks)[:, 0:1]
            allowed = down_ids == across
            q_all = queries[here, :]
            k_all = keys_all[here, :]
            v_all = values_all[here, :]
            for h in range(heads):
                cut = slice(h * HDIM, (h + 1) * HDIM)
                scores = product_nt(q_all[:, cut], k_all[:, cut]) * score_scale
                scores = jnp.where(allowed, scores, -1e30)
                scaled = jnp.exp(scores - jnp.max(scores, axis=-1, keepdims=True))
                share = 1.0 / jnp.sum(scaled, axis=-1, keepdims=True)
                probs_low = (scaled * share).astype(low)
                probs[b * heads + h] = probs_low
                thin_second[1, here, cut] = product(probs_low, v_all[:, cut]).astype(low)
            for i in range(2):

                @pl.when(b == i)
                def _():
                    mixed_swaps[i].start()

            return carry

        lax.fori_loop(0, 2, attend_step, 0)
        for copy in out_swaps:
            copy.start()
        for b in range(2):
            normed_pair(b).start()
        proj_low.wait_recv()
        proj_core.start()
        for load in wide_loads:
            load.wait()
        out_pair(0).start()
        near = pl.ds(0, block)
        out_rows = wide_left[1, near, :]

        def act_tile(t, carry):
            at = pl.ds(pl.multiple_of(t * 512, 512), 512)
            wide_right[0, near, at] = product_nt(out_rows, down_weight[at, :]).astype(low)
            return carry

        lax.fori_loop(0, wide_chunks // 2, act_tile, 0)
        rest_from = wide_chunks * CW
        rest = wide - rest_from
        rest_at = pl.ds(rest_from, rest)
        pad_at = pl.ds(rest_from, CW // 2)
        wide_right[0, :, pad_at] = jnp.zeros((2 * block, CW // 2), low)
        wide_right[1, :, pad_at] = jnp.zeros((2 * block, CW // 2), low)
        wide_right[0, near, rest_at] = product_nt(out_rows, down_weight[rest_at, :]).astype(low)

        def make_hidden(b):
            here = pl.ds(b * block, block)
            mixed_swaps[1 - b].wait_recv()
            mixed = thin_second[1, here, :]
            mixed_far = thin_first_in[here, :]

            def proj_tile(n, inner):
                at = pl.ds(pl.multiple_of(n * 384, 384), 384)
                own_part[:, at] = product(mixed, proj_weight[:, at]) + product(
                    mixed_far, proj_other[:, at]
                )
                return inner

            lax.fori_loop(0, width // 384, proj_tile, 0)

            def hidden_strip(at):
                there = pl.ds(at.start + b * block, strip)
                value = all_tokens[there, :].astype(full) + own_part[at, :] + bias_proj
                if b == 0:
                    hidden[at, :] = value
                xhat, _ = norm_stats(value)
                wide_left[0, there, :] = (xhat * gain_two + shift_two).astype(low)

            strips(block, 0, hidden_strip)

        def gelu_parts(here, at):
            value = product_nt(wide_left[0, here, :], up_weight[at, :]) + up_bias[0:1, at]
            square = value * value
            bent = jnp.tanh(GELU_SCALE * value * (1.0 + 0.044715 * square))
            bulge = 0.5 * (1.0 + bent)
            wide_right[1, here, at] = (value * bulge).astype(low)
            return bulge + 0.5 * value * (1.0 - bent * bent) * (
                GELU_SCALE * (1.0 + 0.134145 * square)
            )

        def keep_grad(here, at, value):
            grad = value.astype(low)
            wide_right[0, here, at] = grad
            up_sum[0, :, at] += jnp.sum(grad.astype(full), axis=0, keepdims=True)

        def over_tiles(tile):
            def step(t, inner):
                tile(pl.ds(pl.multiple_of(t * CW, CW), CW))
                return inner

            lax.fori_loop(0, wide_chunks, step, 0, unroll=UNROLL)
            tile(rest_at)

        far = pl.ds(block, block)

        def far_tile(at):
            wide_right[0, far, at] = gelu_parts(far, at).astype(low)

        def near_tile(at):
            keep_grad(near, at, gelu_parts(near, at) * wide_right[0, near, at].astype(full))

        def back_tiles(b):
            grad_rows = wide_right[0, pl.ds(b * block, block), pl.ds(0, wide)]

            def back_tile(n, inner):
                at = pl.ds(pl.multiple_of(n * 384, 384), 384)
                value = product(grad_rows, up_weight[:, at])
                if b == 0:
                    own_part[:, at] = value
                else:
                    part_send[0, :, at] = value.astype(low)
                return inner

            lax.fori_loop(0, width // 384, back_tile, 0)

        proj_core.wait_recv()
        make_hidden(1)
        over_tiles(far_tile)
        left_pair(1).start()
        act_pair(1).start()
        make_hidden(0)
        left_pair(0).start()
        over_tiles(near_tile)
        act_pair(0).start()
        grad_pair(0).start()

        def slope_rows(j):
            here = pl.ds(block + j * half_block, half_block)

            def slope_tile(at):
                grad = product_nt(wide_left[1, here, :], down_weight[at, :])
                keep_grad(here, at, wide_right[0, here, at].astype(full) * grad)

            over_tiles(slope_tile)
            grad_pair(1 + j).start()

        def out_arrived(j):
            out_swaps[j].wait_recv()
            mask_rows(1, j * half_block, half_block)
            out_pair(1 + j).start()

        out_arrived(0)
        slope_rows(0)
        back_tiles(0)
        out_arrived(1)

        def pair_arrived():
            for p in range(3):
                out_pair(p).wait_recv()
            for i in range(2):
                act_pair(i).wait_recv()

        emit(early, 0, 0, wide_value(0, pair_arrived), AHEAD)

        def early_step(j, inner):
            emit(early, 2 * j, 2 * j, wide_value(j), AHEAD)
            return inner

        lax.fori_loop(1, early_chunks // 2, early_step, 0)
        slope_rows(1)
        rest_pair().start()
        back_tiles(1)
        for copy in part_swaps[0]:
            copy.start()
        for i in range(FIRST):
            take_first(early, i, i)
        act_rows = wide_right[1, :, pl.ds(0, wide)]

        def down_tile(n, inner):
            at = pl.ds(pl.multiple_of(n * 384, 384), 384)
            value = product(act_rows, down_weight[:, at])
            own_down[:, at] = value[:block]
            part_send[1, :, at] = value[block:].astype(low)
            return inner

        lax.fori_loop(0, width // 384, down_tile, 0)

    pl.run_scoped(
        mlp_scope,
        pltpu.VMEM(up_hbm.shape, low),
        pltpu.VMEM(down_hbm.shape, low),
        pltpu.SemaphoreType.DMA((2,)),
    )

    def grad_scope(grads, summed):
        def held(j, action):
            @pl.when(j < early_chunks)
            def _():
                action(early, j, j)

            @pl.when(j >= early_chunks)
            def _():
                action(grads, j - early_chunks, j)

        def pump_step(i, carry):
            @pl.when(i >= core_lag)
            def _():
                rest_copy(summed, i - core_lag).wait_recv()

            @pl.when(jnp.logical_and(i >= high_lag, i < chunks + high_lag))
            def _():
                held(i - high_lag, lambda ref, k, j: take_high(ref, k, j, summed))

            @pl.when(jnp.logical_and(i >= second_lag, i < chunks + second_lag))
            def _():
                held(i - second_lag, take_second)

            @pl.when(i < chunks)
            def _():
                held(i, take_first)

            return carry

        def pump(first, last, made=wide_subs):
            def step(i, carry):
                pump_step(i, carry)

                @pl.when(i + AHEAD < made)
                def _():
                    issue(grads, i + AHEAD - early_chunks, i + AHEAD)

                return carry

            lax.fori_loop(first, last, step, 0)

        def emit_late(j, value, ahead):
            emit(grads, j - early_chunks, j, value, ahead)

        for i in range(2):
            left_pair(i).wait_recv()
        for p in range(3):
            grad_pair(p).wait_recv()

        def wide_step(j, carry):
            emit_late(2 * j, wide_value(j), FIRST + AHEAD)
            return carry

        lax.fori_loop(early_chunks // 2, wide_chunks, wide_step, 0)
        pump(FIRST, 4)

        for j in range(2):
            part_swaps[0][j].wait_recv()

            def norm_back_strip(at):
                grad = own_part[at, :] + part_in[0, at, :].astype(full)
                kept = hidden[at, :]
                xhat, inverse = norm_stats(kept)
                own_down[at, :] += kept
                out_rows = wide_left[1, at, :].astype(full)
                value = out_rows + norm_grad(xhat, inverse, gain_two, grad)
                hidden[at, :] = value
                rounded = value.astype(low)
                thin_left[1, at, :] = rounded
                totals[2:3] += column_sums(rounded.astype(full))[None]
                totals[3:4] += column_sums(grad * xhat)[None]
                totals[4:5] += column_sums(grad)[None]
                totals[5:6] += column_sums(out_rows)[None]

            strips(half_block, j * half_block, norm_back_strip)
            hidden_swaps[j].start()
            if j == 0:
                pump(4, 5)
        for copy in part_swaps[1]:
            copy.start()

        pump(5, 7)

        def back_step(b, carry):
            here = pl.ds(pl.multiple_of(b * block, block), block)

            @pl.when(b == 1)
            def _():
                for copy in part_swaps[0]:
                    copy.wait_send()
                for copy in hidden_swaps:
                    copy.wait_recv()
                for i in range(2):
                    other_pair(i).start()

            grad_mixed = product_nt(thin_left[1, here, :], proj_weight[...]).astype(low)
            q_all = queries[here, :]
            k_all = keys_all[here, :]
            v_all = values_all[here, :]
            for h in range(heads):
                cut = slice(h * HDIM, (h + 1) * HDIM)
                probs_low = probs[b * heads + h]
                probs_full = probs_low.astype(full)
                mixed_grad = grad_mixed[:, cut]
                grad_probs = product_nt(mixed_grad, v_all[:, cut])
                weighted = probs_full * grad_probs
                grad_scores = (
                    weighted - probs_full * jnp.sum(weighted, axis=-1, keepdims=True)
                ).astype(low)
                thin_first[0, here, cut] = (product(grad_scores, k_all[:, cut]) * score_scale).astype(low)
                thin_second[0, here, cut] = (
                    product_tn(grad_scores, q_all[:, cut]) * score_scale
                ).astype(low)
                thin_first[1, here, cut] = product_tn(probs_low, mixed_grad).astype(low)

            @pl.when(b == 0)
            def _():
                first_pair(0).start()
                second_pair(0).start()

            @pl.when(b == 1)
            def _():
                first_pair(1).start()
                second_pair(1).start()

            grad_q = thin_first[0, here, :]
            grad_k = thin_second[0, here, :]
            grad_v = thin_first[1, here, :]

            def normed_tile(n, inner):
                at = pl.ds(pl.multiple_of(n * 384, 384), 384)
                value = (
                    product(grad_q, query_weight[:, at])
                    + product(grad_k, key_weight[:, at])
                    + product(grad_v, value_weight[:, at])
                )

                @pl.when(b == 0)
                def _():
                    own_part[:, at] = value

                @pl.when(b == 1)
                def _():
                    part_send[0, :, at] = value.astype(low)

                return inner

            lax.fori_loop(0, width // 384, normed_tile, 0)
            pump(7 + 4 * b, 11 + 3 * b)
            return carry

        lax.fori_loop(0, 2, back_step, 0)
        for copy in part_swaps[2]:
            copy.start()

        for b in range(2):
            for pair in (normed_pair, other_pair, first_pair, second_pair):
                pair(b).wait_recv()
        rest_pair().wait_recv()

        def first_part(columns):
            return product_tn(thin_left[0], thin_first[core, :, columns]) + product_tn(
                thin_left_in[...], thin_first_in[:, columns]
            )

        def second_part(columns):
            return product_tn(thin_left[core], thin_second[core, :, columns]) + product_tn(
                thin_other_in[...], thin_second_in[:, columns]
            )

        def thin_step(j, carry):
            columns = pl.ds(pl.multiple_of(j * CW, CW), CW)
            ahead = 14 + j + AHEAD
            emit_late(2 * (wide_chunks + 2 * j), first_part(columns), ahead)
            emit_late(2 * (wide_chunks + 2 * j + 1), second_part(columns), ahead)
            pump(14 + j, 15 + 2 * j, 2 * (wide_chunks + 2 * j + 2))
            return carry

        lax.fori_loop(0, 2, thin_step, 0)
        thin_rest = pl.ds(2 * CW, thin - 2 * CW)
        wide_rest = pl.ds(wide_chunks * CW, CW // 2)
        emit_late(
            chunks - 2,
            jnp.concatenate(
                [
                    product_tn(wide_left[core], wide_right[core, :, wide_rest])
                    + product_tn(wide_left_in[core], rest_right_in[...]),
                    first_part(thin_rest),
                    second_part(thin_rest),
                ],
                axis=1,
            ),
            17 + AHEAD,
        )
        pump(17, 19, chunks)

        for copy in part_swaps[2]:
            copy.wait_recv()

        def final_strip(at):
            grad = own_part[at, :] + part_in[0, at, :].astype(full)
            xhat, inverse = norm_stats(all_tokens[at, :].astype(full))
            rows_out[1, at, :] = (
                hidden[at, :] + norm_grad(xhat, inverse, gain_one, grad)
            ).astype(low)
            totals[0:1] += column_sums(grad * xhat)[None]
            totals[1:2] += column_sums(grad)[None]

        strips(block, 0, final_strip)
        sums = totals[...]
        lower = sums[:, :thin]
        upper = sums[:, thin:]
        halves[0] = jnp.where(shard == 0, lower, upper)
        halves[1] = jnp.where(shard == 0, upper, lower)
        halves_swap.start()
        grad_query_bias = column_sums(thin_first[0].astype(full))[None]
        grad_value_bias = column_sums(thin_first[1].astype(full))[None]
        pump(19, 21, chunks)
        halves_swap.wait_recv()
        vector_sum[0] = halves[0] + halves_in[...]
        vector_sum[0, 6:7] = grad_query_bias
        vector_sum[0, 7:8] = grad_value_bias

        def vector_copies(i):
            return (
                remote(
                    vector_sum.at[i], vector_in.at[i], vec_send.at[2 * i], vec_recv.at[2 * i], vector_peers[i]
                ),
                remote(
                    up_sum.at[i], up_in.at[i], vec_send.at[2 * i + 1], vec_recv.at[2 * i + 1], vector_peers[i]
                ),
            )

        def vector_start(i):
            for copy in vector_copies(i):
                copy.start()

        def vector_finish(i):
            for copy in vector_copies(i):
                copy.wait_recv()
            vector_sum[i + 1] = vector_sum[i] + vector_in[i]
            up_sum[i + 1] = up_sum[i] + up_in[i]

        vector_start(0)
        for copy in part_swaps[1]:
            copy.wait_recv()

        def out_strip(at):
            value = own_down[at, :] + part_in[1, at, :].astype(full) + bias_down
            rows_out[0, at, :] = value.astype(low)

        strips(block, 0, out_strip)
        alive = jnp.transpose(all_slots[0])[:, 1:2].astype(low)
        rows_out[0] = rows_out[0] * alive

        def drain(j, carry):
            held(j, lambda ref, k, i: first_copy(ref, k, i, False).wait_send())
            held(j, lambda ref, k, i: second_copy(ref, k, i, False).wait_send())
            held(j, lambda ref, k, i: high_copy(ref, k, i).wait_send())
            rest_copy(summed, j).wait_send()
            return carry

        out_copies = [
            pltpu.make_async_copy(source, target, out_sem.at[i])
            for i, (source, target) in enumerate(
                (
                    (rows_out, rows_hbm),
                    (wide_out, wide_hbm),
                    (vector_sum.at[4], vectors_hbm),
                    (up_sum.at[4], up_sum_hbm),
                    (thin_out, thin_hbm),
                    (rest_out, rest_hbm),
                )
            )
        ]
        out_copies[0].start()
        pump(21, 22, chunks)
        vector_finish(0)
        vector_start(1)
        pump(22, 24, chunks)
        out_copies[1].start()
        vector_finish(1)
        vector_start(2)
        pump(24, 25, chunks)
        vector_finish(2)
        vector_start(3)
        pump(25, 29, chunks)
        vector_finish(3)
        out_copies[2].start()
        out_copies[3].start()
        lax.fori_loop(0, chunks - core_lag, drain, 0)
        pump(29, 32, chunks)
        out_copies[4].start()
        pump(32, chunks + core_lag, chunks)
        out_copies[5].start()
        lax.fori_loop(chunks - core_lag, chunks, drain, 0)
        for copy in out_copies:
            copy.wait()
        for i in range(4):
            for copy in vector_copies(i):
                copy.wait_send()

    pl.run_scoped(
        grad_scope,
        pltpu.VMEM((chunks - early_chunks, 2, 2, 2, rows, SUB), low),
        pltpu.VMEM((chunks, 2, rows // 2, SUB), full),
    )
    for copy in [vectors_swap, slots_swap, *tokens_swaps, *out_swaps, *mixed_swaps, proj_swap, halves_swap]:
        copy.wait_send()
    for copies in part_swaps[1:] + [hidden_swaps]:
        for copy in copies:
            copy.wait_send()
    for copy in (proj_y, proj_low, proj_core):
        copy.wait_send()
    for p in range(3):
        out_pair(p).wait_send()
        grad_pair(p).wait_send()
    rest_pair().wait_send()
    for b in range(2):
        for pair in (left_pair, act_pair, normed_pair, other_pair, first_pair, second_pair):
            pair(b).wait_send()


def publish_kernel(rows_in, wide_in, thin_in, rest_in, vectors_in, up_in, *refs):
    outs, refs = refs[:17], refs[17:]
    rows_at, wide_at, thin_at, rest_at, vectors_at, up_at = refs[:6]
    flats, in_sem, out_sem = refs[6:15], refs[15], refs[16]
    wide_main = wide_in.shape[2]
    thin_main = thin_in.shape[3]
    wide, thin = wide_at.shape[2], thin_at.shape[3]
    loads = [
        pltpu.make_async_copy(source, target, in_sem.at[i])
        for i, (source, target) in enumerate(
            (
                (vectors_in, vectors_at),
                (up_in, up_at),
                (rest_in, rest_at),
                (rows_in, rows_at),
                (thin_in, thin_at.at[:, :, :, pl.ds(0, thin_main)]),
                (wide_in, wide_at.at[:, :, pl.ds(0, wide_main)]),
            )
        )
    ]
    for load in loads:
        load.start()
    stores = []

    def store(source, place):
        copy = pltpu.make_async_copy(source, outs[place], out_sem.at[place])
        copy.start()
        stores.append(copy)

    loads[0].wait()
    loads[1].wait()
    for i in range(8):
        flats[i][...] = vectors_at[i : i + 1, :].reshape(flats[i].shape)
    flats[8][...] = up_at[:, :wide].reshape(flats[8].shape)
    loads[2].wait()
    loads[3].wait()
    store(rows_at.at[0], 0)
    store(rows_at.at[1], 1)
    for slot in range(2):
        wide_at[slot, :, wide_main:] = rest_at[slot, 0, :, : wide - wide_main]
        for place in range(2):
            start = place * (thin - thin_main)
            thin_at[slot, place, :, thin_main:] = rest_at[
                slot, 1, :, start : start + thin - thin_main
            ]
    loads[4].wait()
    for i, place in enumerate((4, 6, 7, 9)):
        store(thin_at.at[i // 2, i % 2], place)
    loads[5].wait()
    store(wide_at.at[0], 13)
    store(wide_at.at[1], 15)
    for flat, place in zip(flats, (2, 3, 10, 11, 12, 16, 5, 8, 14)):
        store(flat, place)
    for copy in stores:
        copy.wait()


def publish_call(packed, wide):
    full = jnp.float32
    rows_out, wide_out, thin_out, rest_out, vectors, up_bias_grad = packed
    thin = vectors.shape[1]
    half = wide_out.shape[1]
    anywhere = pl.BlockSpec(memory_space=pl.ANY)
    vector = jax.ShapeDtypeStruct((thin,), full)
    matrix = jax.ShapeDtypeStruct((half, thin), full)
    tall = jax.ShapeDtypeStruct((half, wide), full)
    rows = jax.ShapeDtypeStruct(rows_out.shape[1:], rows_out.dtype)
    return pl.pallas_call(
        publish_kernel,
        out_shape=(
            rows, rows, vector, vector, matrix, vector, matrix, matrix, vector, matrix, vector,
            vector, vector, tall, jax.ShapeDtypeStruct((wide,), full), tall, vector,
        ),
        in_specs=[anywhere] * 6,
        out_specs=(anywhere,) * 17,
        scratch_shapes=[
            pltpu.VMEM(rows_out.shape, rows_out.dtype),
            pltpu.VMEM((2, half, wide), full),
            pltpu.VMEM((2, 2, half, thin), full),
            pltpu.VMEM(rest_out.shape, full),
            pltpu.VMEM(vectors.shape, full),
            pltpu.VMEM(up_bias_grad.shape, full),
            *[pltpu.VMEM((thin,), full)] * 8,
            pltpu.VMEM((wide,), full),
            pltpu.SemaphoreType.DMA((6,)),
            pltpu.SemaphoreType.DMA((17,)),
        ],
        name="publish",
    )(*packed)


def layer_call(tokens, out_grad, slots, vectors, up_bias, matrices):
    query_weight, up_weight, down_weight = matrices[0], matrices[4], matrices[5]
    low = jnp.bfloat16
    full = jnp.float32
    block, width = tokens.shape
    thin = query_weight.shape[0]
    wide = up_weight.shape[0]
    wide_pad = wide + -wide % 128
    heads = thin // HDIM
    replicas = lax.axis_size("replica")
    rows = width // replicas * 2
    wide_main = wide // CW * CW
    chunks = 2 * (wide // CW + 5)
    half = rows // 2
    both = 2 * block
    anywhere = pl.BlockSpec(memory_space=pl.ANY)
    dma = pltpu.SemaphoreType.DMA
    return pl.pallas_call(
        layer_kernel,
        out_shape=(
            jax.ShapeDtypeStruct((2,) + tokens.shape, low),
            jax.ShapeDtypeStruct((2, half, wide_main), full),
            jax.ShapeDtypeStruct((2, 2, half, 2 * CW), full),
            jax.ShapeDtypeStruct((2, 2, half, SUB), full),
            jax.ShapeDtypeStruct((8, thin), full),
            jax.ShapeDtypeStruct((1, wide_pad), full),
        ),
        in_specs=[anywhere] * 19,
        out_specs=(anywhere,) * 6,
        scratch_shapes=[
            pltpu.VMEM((2,) + tokens.shape, low),
            pltpu.VMEM((2, half, wide_main), full),
            pltpu.VMEM((2, 2, half, 2 * CW), full),
            pltpu.VMEM((2, 2, half, SUB), full),
            pltpu.VMEM((8, block), full),
            pltpu.VMEM((8, thin), full),
            pltpu.VMEM((8, wide), full),
            pltpu.VMEM((thin, width), low),
            pltpu.VMEM((thin, width), low),
            pltpu.VMEM((thin, width), low),
            pltpu.VMEM((thin, width), low),
            pltpu.VMEM((thin, width), low),
            pltpu.VMEM((both, width), low),
            pltpu.VMEM((2, 8, block), full),
            pltpu.VMEM((8, thin), full),
            pltpu.VMEM((both, thin), low),
            pltpu.VMEM((both, thin), low),
            pltpu.VMEM((both, thin), low),
            pltpu.VMEM((2 * heads, block, block), low),
            pltpu.VMEM((block, width), full),
            pltpu.VMEM((block, width), full),
            pltpu.VMEM((block, width), full),
            pltpu.VMEM((2, block, width), low),
            pltpu.VMEM((2, block, width), low),
            pltpu.VMEM((2, both, width), low),
            pltpu.VMEM((2, both, wide_pad), low),
            pltpu.VMEM((2, both, width), low),
            pltpu.VMEM((2, both, thin), low),
            pltpu.VMEM((2, both, thin), low),
            pltpu.VMEM((2, both, width), low),
            pltpu.VMEM((2, both, wide_main // 2), low),
            pltpu.VMEM((both, SUB), low),
            pltpu.VMEM((both, width), low),
            pltpu.VMEM((both, width), low),
            pltpu.VMEM((both, thin), low),
            pltpu.VMEM((both, thin), low),
            pltpu.VMEM((EARLY, 2, 2, 2, rows, SUB), low),
            pltpu.VMEM((chunks, 2, 2, rows, SUB), low),
            pltpu.VMEM((chunks, 2, rows, SUB), low),
            pltpu.VMEM((chunks, rows, SUB), low),
            pltpu.VMEM((8, width), full),
            pltpu.VMEM((2, 8, thin), full),
            pltpu.VMEM((8, thin), full),
            pltpu.VMEM((5, 8, thin), full),
            pltpu.VMEM((4, 8, thin), full),
            pltpu.VMEM((5, 1, wide_pad), full),
            pltpu.VMEM((4, 1, wide_pad), full),
            *[pltpu.VMEM((thin,), low)] * 8,
            *[pltpu.VMEM((block,), jnp.int32)] * 2,
            pltpu.VMEM((wide,), low),
            dma((11,)),
            dma((6,)),
            dma((18,)),
            dma((18,)),
            dma((3,)),
            dma((3,)),
            dma((19,)),
            dma((19,)),
            dma((chunks,)),
            dma((chunks,)),
            dma((chunks,)),
            dma((chunks,)),
            dma((chunks,)),
            dma((chunks,)),
            dma((chunks,)),
            dma((chunks,)),
            dma((8,)),
            dma((8,)),
            dma((6,)),
        ],
        compiler_params=pltpu.CompilerParams(
            collective_id=0, has_side_effects=True, vmem_limit_bytes=67043328
        ),
        name="layer",
    )(tokens, out_grad, *slots, *vectors, up_bias, *matrices)


def whole_layer(
    tokens, out_grad, picture_ids, live_slots, ln1_gain, ln1_bias, query_weight, query_bias,
    key_weight, value_weight, value_bias, proj_weight, proj_bias, ln2_gain, ln2_bias, up_weight,
    up_bias, down_weight, down_bias,
):
    width = tokens.shape[1]
    if not by_kernel(lax.axis_size("replica"), width):
        return paired(
            tokens, out_grad, picture_ids, live_slots, ln1_gain, ln1_bias, query_weight,
            query_bias, key_weight, value_weight, value_bias, proj_weight, proj_bias, ln2_gain,
            ln2_bias, up_weight, up_bias, down_weight, down_bias,
        )
    packed = layer_call(
        tokens,
        out_grad,
        (picture_ids, live_slots),
        (ln1_gain, ln1_bias, proj_bias, ln2_gain, ln2_bias, down_bias, query_bias, value_bias),
        up_bias,
        (query_weight.T, key_weight.T, value_weight.T, proj_weight, up_weight.T, down_weight),
    )
    outs = list(publish_call(packed, up_weight.shape[1]))
    outs[9] = outs[9].T
    outs[15] = outs[15].T
    return tuple(outs)


def solution(mesh):
    in_specs = (
        P(("shard", "replica"), None),
        P(("shard", "replica"), None),
        P(("shard", "replica")),
        P(("shard", "replica")),
        P("shard"),
        P("shard"),
        P(None, "shard"),
        P("shard"),
        P(None, "shard"),
        P(None, "shard"),
        P("shard"),
        P("shard", None),
        P("shard"),
        P("shard"),
        P("shard"),
        P(None, "shard"),
        P("shard"),
        P("shard", None),
        P("shard"),
    )
    out_specs = (
        P(("shard", "replica"), None),
        P(("shard", "replica"), None),
        P("shard"),
        P("shard"),
        P("replica", "shard"),
        P("shard"),
        P("replica", "shard"),
        P("replica", "shard"),
        P("shard"),
        P("shard", "replica"),
        P("shard"),
        P("shard"),
        P("shard"),
        P("replica", "shard"),
        P("shard"),
        P("shard", "replica"),
        P("shard"),
    )
    return jax.shard_map(whole_layer, mesh=mesh, in_specs=in_specs, out_specs=out_specs, check_vma=False)
```

```python
import functools

import jax
import jax.numpy as jnp
from jax import lax
from jax.experimental import pallas as pl
from jax.experimental.pallas import tpu as pltpu
from jax.sharding import PartitionSpec as P

HDIM = 72
norm_eps = 1e-06
MESH = pl.DeviceIdType.MESH
CW = 256
SUB = 128
EARLY = 6
AHEAD = 6
FIRST = 2
LAGS = (3, 6, 8)
UNROLL = 2
GELU_SCALE = 0.7978845608028654


def norm_stats(values):
    centered = values - jnp.mean(values, axis=-1, keepdims=True)
    variance = jnp.mean(centered * centered, axis=-1, keepdims=True)
    inverse = lax.rsqrt(variance + norm_eps)
    return centered * inverse, inverse


def norm_grad(xhat, inverse, gain, grad):
    scaled = grad * gain
    return (
        scaled
        - jnp.mean(scaled, axis=-1, keepdims=True)
        - xhat * jnp.mean(scaled * xhat, axis=-1, keepdims=True)
    ) * inverse


def gelu_tanh(values):
    return jax.nn.gelu(values, approximate=True)


def product(left_side, right_side):
    return jnp.dot(left_side, right_side, preferred_element_type=jnp.float32)


def product_nt(left_side, right_side):
    return lax.dot_general(
        left_side, right_side, (((1,), (1,)), ((), ())), preferred_element_type=jnp.float32
    )


def product_tn(left_side, right_side):
    return lax.dot_general(
        left_side, right_side, (((0,), (0,)), ((), ())), preferred_element_type=jnp.float32
    )


def column_sums(matrix):
    return jnp.sum(matrix, axis=0, dtype=jnp.float32)


def swap(value):
    return lax.ppermute(value, "shard", [(0, 1), (1, 0)])


def split_heads(matrix, block_rows):
    return matrix.reshape(-1, block_rows, matrix.shape[1] // HDIM, HDIM)


def attend(queries, keys_in, values_in, allowed, block_rows):
    scores = jnp.einsum(
        "bqhd,bkhd->bhqk",
        split_heads(queries, block_rows),
        split_heads(keys_in, block_rows),
        preferred_element_type=jnp.float32,
    ) * HDIM ** (-0.5)
    scores = jnp.where(allowed[:, None, :, :], scores, -1e30)
    highest = jnp.max(scores, axis=-1, keepdims=True)
    scaled_exp = jnp.exp(scores - highest)
    totals = jnp.sum(scaled_exp, axis=-1, keepdims=True)
    probs = scaled_exp / totals
    mixed_out = jnp.einsum(
        "bhqk,bkhd->bqhd",
        probs.astype(jnp.bfloat16),
        split_heads(values_in, block_rows),
        preferred_element_type=jnp.float32,
    )
    return mixed_out.reshape(queries.shape), probs


def attend_back(queries, keys_in, values_in, grad_mixed, probs, block_rows):
    score_scale = HDIM ** (-0.5)
    split_grad = split_heads(grad_mixed, block_rows)
    grad_probs = jnp.einsum(
        "bqhd,bkhd->bhqk",
        split_grad,
        split_heads(values_in, block_rows),
        preferred_element_type=jnp.float32,
    )
    grad_scores = (
        probs * (grad_probs - jnp.sum(probs * grad_probs, axis=-1, keepdims=True))
    ).astype(jnp.bfloat16)
    grad_queries = (
        jnp.einsum(
            "bhqk,bkhd->bqhd",
            grad_scores,
            split_heads(keys_in, block_rows),
            preferred_element_type=jnp.float32,
        )
        * score_scale
    )
    grad_keys = (
        jnp.einsum(
            "bhqk,bqhd->bkhd",
            grad_scores,
            split_heads(queries, block_rows),
            preferred_element_type=jnp.float32,
        )
        * score_scale
    )
    grad_values = jnp.einsum(
        "bhqk,bqhd->bkhd",
        probs.astype(jnp.bfloat16),
        split_grad,
        preferred_element_type=jnp.float32,
    )
    return (
        grad_queries.astype(jnp.bfloat16).reshape(queries.shape),
        grad_keys.astype(jnp.bfloat16).reshape(queries.shape),
        grad_values.astype(jnp.bfloat16).reshape(queries.shape),
    )


def add_low(first, second):
    return (first.astype(jnp.float32) + second.astype(jnp.float32)).astype(jnp.bfloat16)


def by_kernel(replicas, width):
    return replicas == 2**4 and width % (replicas // 2 * 16) == 0


def plain_sums(block_out, tokens_grad, vectors, half, wide, query, key, value, proj, up, down):
    def owned(pair):
        return lax.psum_scatter(product_tn(*pair), "replica", scatter_dimension=0, tiled=True)

    vectors = lax.psum(vectors, "replica")

    def vector_at(i):
        return vectors[i * half : (i + 1) * half]

    return (
        block_out, tokens_grad, vector_at(0), vector_at(1), owned(query), vector_at(6),
        owned(key), owned(value), vector_at(7), owned(proj).T, vector_at(2), vector_at(3),
        vector_at(4), owned(up), vectors[8 * half : 8 * half + wide], owned(down).T, vector_at(5),
    )


def paired(
    tokens, out_grad, picture_ids, live_slots, ln1_gain, ln1_bias, query_weight, query_bias,
    key_weight, value_weight, value_bias, proj_weight, proj_bias, ln2_gain, ln2_bias, up_weight,
    up_bias, down_weight, down_bias,
):
    low = jnp.bfloat16
    full = jnp.float32
    rows, width = tokens.shape
    half = width // 2
    wide = up_weight.shape[1]
    shard = lax.axis_index("shard")
    own_vectors = jnp.stack([ln1_gain, ln1_bias, proj_bias, ln2_gain, ln2_bias, down_bias])
    slots = jnp.stack([picture_ids, live_slots])
    peer_tokens, peer_out, peer_vectors, peer_slots = (
        swap(tokens), swap(out_grad), swap(own_vectors), swap(slots),
    )
    gain_one, shift_one, bias_proj, gain_two, shift_two, bias_down = jnp.where(
        shard == 0,
        jnp.concatenate([own_vectors, peer_vectors], axis=1),
        jnp.concatenate([peer_vectors, own_vectors], axis=1),
    ).astype(full)
    slots = jnp.concatenate([slots, peer_slots], axis=1)
    alive = slots[1].astype(full)[:, None]
    ids = slots[0].reshape(2, rows)
    living = slots[1].reshape(2, rows)
    allowed = (ids[:, :, None] == ids[:, None, :]) & (living[:, None, :] == 1)
    all_tokens = jnp.concatenate([tokens, peer_tokens]).astype(full)
    all_out = jnp.concatenate([out_grad, peer_out]) * alive.astype(low)
    xhat_one, inverse_one = norm_stats(all_tokens)
    normed = (xhat_one * gain_one + shift_one).astype(low)
    queries = (product(normed, query_weight) + query_bias.astype(full)).astype(low)
    keys_all = product(normed, key_weight).astype(low)
    values_all = (product(normed, value_weight) + value_bias.astype(full)).astype(low)
    mixed_out, probs = attend(queries, keys_all, values_all, allowed, rows)
    mixed = mixed_out.astype(low)
    partial = product(mixed, proj_weight)
    hidden = all_tokens[:rows] + partial[:rows] + swap(partial[rows:].astype(low)).astype(full) + bias_proj
    xhat_two, inverse_two = norm_stats(hidden)
    normed_own = (xhat_two * gain_two + shift_two).astype(low)
    normed_two = jnp.concatenate([normed_own, swap(normed_own)])
    up_proj = product(normed_two, up_weight) + up_bias.astype(full)
    activated = gelu_tanh(up_proj).astype(low)
    grad_act = product_nt(all_out, down_weight)
    grad_up = jax.vjp(gelu_tanh, up_proj)[1](grad_act)[0].astype(low)
    partial = product_nt(grad_up, up_weight)
    grad_two = partial[:rows] + swap(partial[rows:].astype(low)).astype(full)
    partial = product(activated, down_weight)
    block_out = (
        (hidden + partial[:rows] + swap(partial[rows:].astype(low)).astype(full) + bias_down)
        * alive[:rows]
    ).astype(low)
    grad_hidden = all_out[:rows].astype(full) + norm_grad(xhat_two, inverse_two, gain_two, grad_two)
    hidden_own = grad_hidden.astype(low)
    hidden_low = jnp.concatenate([hidden_own, swap(hidden_own)])
    grad_mixed = product_nt(hidden_low, proj_weight).astype(low)
    grad_queries, grad_keys, grad_values = attend_back(
        queries, keys_all, values_all, grad_mixed, probs, rows
    )
    partial = (
        product_nt(grad_queries, query_weight)
        + product_nt(grad_keys, key_weight)
        + product_nt(grad_values, value_weight)
    )
    grad_one = partial[:rows] + swap(partial[rows:].astype(low)).astype(full)
    tokens_grad = (
        grad_hidden + norm_grad(xhat_one[:rows], inverse_one[:rows], gain_one, grad_one)
    ).astype(low)
    wholes = jnp.stack(
        [
            column_sums(grad_one * xhat_one[:rows]),
            column_sums(grad_one),
            column_sums(hidden_own),
            column_sums(grad_two * xhat_two),
            column_sums(grad_two),
            column_sums(all_out[:rows]),
        ]
    )
    mine = lax.dynamic_slice_in_dim(wholes, shard * half, half, 1)
    theirs = lax.dynamic_slice_in_dim(wholes, (1 - shard) * half, half, 1)
    halves = mine + swap(theirs)
    vectors = jnp.concatenate(
        [
            halves.reshape(-1),
            column_sums(grad_queries),
            column_sums(grad_values),
            column_sums(grad_up),
        ]
    )
    return plain_sums(
        block_out, tokens_grad, vectors, half, wide,
        (normed, grad_queries), (normed, grad_keys), (normed, grad_values),
        (hidden_low, mixed), (normed_two, grad_up), (all_out, activated),
    )


def take(ref, start, count):
    return ref.at[pl.ds(start, count)]


def layer_kernel(
    tokens_hbm,
    out_hbm,
    picture_ids,
    live_slots,
    ln1_gain,
    ln1_bias,
    proj_bias,
    ln2_gain,
    ln2_bias,
    down_bias,
    query_bias,
    value_bias,
    up_bias_in,
    query_hbm,
    key_hbm,
    value_hbm,
    proj_hbm,
    up_hbm,
    down_hbm,
    rows_hbm,
    wide_hbm,
    thin_hbm,
    rest_hbm,
    vectors_hbm,
    up_sum_hbm,
    wide_out,
    thin_out,
    rest_out,
    slots,
    vectors,
    up_bias,
    query_weight,
    key_weight,
    value_weight,
    proj_weight,
    proj_other,
    all_tokens,
    all_slots,
    vectors_in,
    queries,
    keys_all,
    values_all,
    probs,
    hidden,
    own_part,
    own_down,
    part_send,
    part_in,
    wide_left,
    wide_right,
    thin_left,
    thin_first,
    thin_second,
    wide_left_in,
    wide_right_in,
    rest_right_in,
    thin_left_in,
    thin_other_in,
    thin_first_in,
    thin_second_in,
    early,
    from_first,
    from_second,
    from_high,
    totals,
    halves,
    halves_in,
    vector_sum,
    vector_in,
    up_sum,
    up_in,
    flat_0,
    flat_1,
    flat_2,
    flat_3,
    flat_4,
    flat_5,
    flat_6,
    flat_7,
    flat_slots_0,
    flat_slots_1,
    flat_up,
    small_sem,
    load_sem,
    swap_send,
    swap_recv,
    proj_send,
    proj_recv,
    pair_send,
    pair_recv,
    first_send,
    first_recv,
    second_send,
    second_recv,
    high_send,
    high_recv,
    core_send,
    core_recv,
    vec_send,
    vec_recv,
    out_sem,
):
    full = jnp.float32
    low = jnp.bfloat16
    chunks = from_first.shape[0]
    rows = from_first.shape[3]
    early_chunks = early.shape[0]
    second_lag, high_lag, core_lag = LAGS
    block, width = tokens_hbm.shape
    thin = queries.shape[1]
    wide = up_bias.shape[1]
    heads = thin // HDIM
    score_scale = HDIM ** (-0.5)
    wide_chunks = chunks // 2 - 5
    wide_subs = 2 * wide_chunks
    half_block = block // 2
    strip = 32
    shard = lax.axis_index("shard")
    replica = lax.axis_index("replica")
    core = lax.rem(replica, 2)
    other = 1 - core
    y_bit = lax.rem(replica // 2, 2)
    low_bit = lax.rem(replica // 4, 2)
    high_bit = lax.rem(replica // 8, 2)
    twin = (1 - shard, replica)
    partner = (shard, replica + 1 - 2 * core)
    y_peer = (shard, replica + 2 - 4 * y_bit)
    low_peer = (shard, replica + 4 - 8 * low_bit)
    high_peer = (shard, replica + 8 - 16 * high_bit)
    peers = (partner, y_peer, low_peer, high_peer)
    vector_peers = (partner, high_peer, low_peer, y_peer)

    def remote(source, target, send, recv, peer):
        return pltpu.make_async_remote_copy(
            src_ref=source,
            dst_ref=target,
            send_sem=send,
            recv_sem=recv,
            device_id=peer,
            device_id_type=MESH,
        )

    def swapped(index, source, target):
        return remote(source, target, swap_send.at[index], swap_recv.at[index], twin)

    def paired_copy(index, source, target):
        return remote(source, target, pair_send.at[index], pair_recv.at[index], partner)

    loads = [
        pltpu.make_async_copy(source, target, load_sem.at[i])
        for i, (source, target) in enumerate(
            (
                (query_hbm, query_weight),
                (key_hbm, key_weight),
                (value_hbm, value_weight),
                (proj_hbm, proj_weight),
                (tokens_hbm, take(all_tokens, 0, block)),
                (out_hbm, wide_left.at[1, pl.ds(0, block)]),
            )
        )
    ]
    barrier = pltpu.get_barrier_semaphore()
    for peer in (twin,) + peers:
        pl.semaphore_signal(barrier, inc=1, device_id=peer, device_id_type=MESH)
    small = [
        pltpu.make_async_copy(source, target, small_sem.at[i])
        for i, (source, target) in enumerate(
            (
                (ln1_gain, flat_0),
                (ln1_bias, flat_1),
                (proj_bias, flat_2),
                (ln2_gain, flat_3),
                (ln2_bias, flat_4),
                (down_bias, flat_5),
                (query_bias, flat_6),
                (value_bias, flat_7),
                (picture_ids, flat_slots_0),
                (live_slots, flat_slots_1),
                (up_bias_in, flat_up),
            )
        )
    ]
    for load in small + loads[4:] + loads[:4]:
        load.start()
    slots[...] = jnp.zeros_like(slots)
    tokens_swaps = [
        swapped(
            index,
            tokens_hbm.at[pl.ds(j * half_block, half_block)],
            all_tokens.at[pl.ds(block + j * half_block, half_block)],
        )
        for j, index in ((0, 2), (1, 17))
    ]
    for load in small:
        load.wait()
    named = (flat_0, flat_1, flat_2, flat_3, flat_4, flat_5, flat_6, flat_7)
    for i, value in enumerate(named):
        vectors[i : i + 1, :] = value[...].astype(full).reshape(1, thin)
    slots[0:1, :] = flat_slots_0[...].astype(full).reshape(1, block)
    slots[1:2, :] = flat_slots_1[...].astype(full).reshape(1, block)
    up_bias[0:1, :] = flat_up[...].astype(full).reshape(1, wide)
    pl.semaphore_wait(barrier, 5)

    vectors_swap = swapped(0, vectors, vectors_in)
    slots_swap = swapped(1, slots, all_slots.at[1])
    out_swaps = [
        swapped(
            index,
            out_hbm.at[pl.ds(j * half_block, half_block)],
            wide_left.at[1, pl.ds(block + j * half_block, half_block)],
        )
        for j, index in ((0, 3), (1, 13))
    ]
    part_swaps = [
        [
            swapped(
                4 + 2 * i + j,
                part_send.at[i % 2, pl.ds(j * half_block, half_block)],
                part_in.at[i % 2, pl.ds(j * half_block, half_block)],
            )
            for j in range(2)
        ]
        for i in range(3)
    ]
    mixed_swaps = [
        swapped(
            10 + b,
            thin_second.at[1, pl.ds(b * block, block)],
            thin_first_in.at[pl.ds((1 - b) * block, block)],
        )
        for b in range(2)
    ]
    quarter = thin // 4
    most = width // 9 * 5
    rest_width = width - most
    some = quarter // 9 * 5
    own_quarter = (2 * low_bit + y_bit) * quarter
    own_columns = pl.ds(pl.multiple_of(core * rest_width, 128), most)

    def proj_rows(start, count):
        return pl.ds(pl.multiple_of(start, 16), count)

    own_rows = proj_rows(own_quarter + high_bit * (quarter - some), some)
    proj_swap = swapped(
        12, proj_hbm.at[own_rows, own_columns], proj_other.at[own_rows, own_columns]
    )

    def proj_copy(index, rows_at, columns, peer):
        piece = proj_other.at[rows_at, columns]
        return remote(piece, piece, proj_send.at[index], proj_recv.at[index], peer)

    proj_high = proj_copy(
        3, proj_rows(own_quarter + high_bit * some, quarter - some), own_columns, high_peer
    )
    proj_y = proj_copy(0, proj_rows(own_quarter, quarter), own_columns, y_peer)
    proj_low = [
        proj_copy(1, proj_rows(own_quarter, quarter), own_columns, low_peer),
        proj_copy(
            4, proj_rows((2 * low_bit + 1 - y_bit) * quarter, quarter), own_columns, low_peer
        ),
    ]
    proj_core = proj_copy(
        2, pl.ds(0, thin), pl.ds(pl.multiple_of(core * most, 128), rest_width), partner
    )
    hidden_swaps = [
        swapped(
            14 + j,
            thin_left.at[1, pl.ds(j * half_block, half_block)],
            thin_left.at[1, pl.ds(block + j * half_block, half_block)],
        )
        for j in range(2)
    ]
    halves_swap = swapped(16, halves.at[1], halves_in)

    def pair_rows(index, source, target, b):
        here = pl.ds(b * block, block)
        return paired_copy(index + b, source.at[here], target.at[here])

    half_wide = wide_right_in.shape[2]
    pieces = ((0, block), (block, half_block), (block + half_block, half_block))

    def out_pair(p):
        here = pl.ds(*pieces[p])
        return paired_copy(p, wide_left.at[1, here], wide_left_in.at[1, here])

    def left_pair(b):
        return pair_rows(3, wide_left.at[0], wide_left_in.at[0], b)

    def theirs(kind, here):
        columns = pl.ds(pl.multiple_of(other * half_wide, CW), half_wide)
        return wide_right.at[kind, here, columns]

    def act_pair(b):
        here = pl.ds(b * block, block)
        return paired_copy(5 + b, theirs(1, here), wide_right_in.at[1, here])

    def grad_pair(p):
        here = pl.ds(*pieces[p])
        return paired_copy(7 + p, theirs(0, here), wide_right_in.at[0, here])

    def rest_pair():
        source = wide_right.at[other, :, pl.ds(2 * half_wide, SUB)]
        return paired_copy(10, source, rest_right_in)

    def normed_pair(b):
        return pair_rows(11, thin_left.at[0], thin_left_in, b)

    def other_pair(b):
        return pair_rows(13, thin_left.at[other], thin_other_in, b)

    def first_pair(b):
        return pair_rows(15, thin_first.at[other], thin_first_in, b)

    def second_pair(b):
        return pair_rows(17, thin_second.at[other], thin_second_in, b)

    vectors_swap.start()
    slots_swap.start()
    proj_swap.start()
    for copy in tokens_swaps:
        copy.start()

    all_slots[0] = slots[...]
    for load in loads[4:]:
        load.wait()

    def mask_rows(b, first, count):
        alive = jnp.transpose(all_slots[b])[first : first + count, 1:2].astype(low)
        at = pl.ds(b * block + first, count)
        wide_left[1, at, :] = wide_left[1, at, :] * alive

    mask_rows(0, 0, block)
    totals[...] = jnp.zeros_like(totals)
    up_sum[0] = jnp.zeros(up_sum.shape[1:], full)

    vectors_swap.wait_recv()
    slots_swap.wait_recv()
    here_half = vectors[...]
    there_half = vectors_in[...]
    joined = jnp.where(
        shard == 0,
        jnp.concatenate([here_half, there_half], axis=1),
        jnp.concatenate([there_half, here_half], axis=1),
    )
    gain_one, shift_one, bias_proj = joined[0:1], joined[1:2], joined[2:3]
    gain_two, shift_two, bias_down = joined[3:4], joined[4:5], joined[5:6]
    bias_query, bias_value = here_half[6:7], here_half[7:8]

    def strips(count, first, body):
        def step(i, carry):
            body(pl.ds(pl.multiple_of(first + i * strip, strip), strip))
            return carry

        lax.fori_loop(0, count // strip, step, 0, unroll=2)

    def is_low_first(j):
        return jnp.logical_and(lax.rem(j, 4) == 1, j < chunks - 1)

    def first_pick(grads, k, low_first):
        if low_first:
            return grads.at[k, :, 1 - low_bit], low_peer
        return grads.at[k, :, :, 1 - y_bit], y_peer

    def second_pick(grads, k, low_first):
        if low_first:
            return grads.at[k, :, low_bit, 1 - y_bit], y_peer
        return grads.at[k, :, 1 - low_bit, y_bit], low_peer

    def first_copy(grads, k, j, low_first):
        source, peer = first_pick(grads, k, low_first)
        return remote(source, from_first.at[j], first_send.at[j], first_recv.at[j], peer)

    def second_copy(grads, k, j, low_first):
        source, peer = second_pick(grads, k, low_first)
        return remote(source, from_second.at[j], second_send.at[j], second_recv.at[j], peer)

    def high_copy(grads, k, j):
        return remote(
            grads.at[k, 1 - high_bit, low_bit, y_bit],
            from_high.at[j],
            high_send.at[j],
            high_recv.at[j],
            high_peer,
        )

    def by_order(j, action):
        low_first = is_low_first(j)

        @pl.when(low_first)
        def _():
            action(True)

        @pl.when(jnp.logical_not(low_first))
        def _():
            action(False)

    def issue(grads, k, j):
        by_order(j, lambda low_first: first_copy(grads, k, j, low_first).start())

    def emit(grads, k, j, value, ahead):
        for i in range(2):
            piece = value[:, i * SUB : (i + 1) * SUB].astype(low)
            grads[k + i] = piece.reshape(grads.shape[1:])

            @pl.when(j + i < ahead)
            def _():
                issue(grads, k + i, j + i)

    def take_first(grads, k, j):
        def action(low_first):
            first_copy(grads, k, j, low_first).wait_recv()
            if low_first:
                grads[k, :, low_bit] = add_low(grads[k, :, low_bit], from_first[j])
            else:
                grads[k, :, :, y_bit] = add_low(grads[k, :, :, y_bit], from_first[j])
            second_copy(grads, k, j, low_first).start()

        by_order(j, action)

    def take_second(grads, k, j):
        by_order(j, lambda low_first: second_copy(grads, k, j, low_first).wait_recv())
        grads[k, :, low_bit, y_bit] = add_low(grads[k, :, low_bit, y_bit], from_second[j])
        high_copy(grads, k, j).start()

    def wide_place(slot, j):
        tile = j // 2
        start = slot * half_wide + lax.rem(tile, wide_chunks // 2) * CW + lax.rem(j, 2) * SUB
        kind = jnp.where(tile < wide_chunks // 2, 1, 0)
        return wide_out.at[kind, :, pl.ds(pl.multiple_of(start, SUB), SUB)]

    def thin_place(slot, j):
        tile = j // 2 - wide_chunks
        start = tile // 2 * CW + lax.rem(j, 2) * SUB
        return thin_out.at[slot, lax.rem(tile, 2), :, pl.ds(pl.multiple_of(start, SUB), SUB)]

    def rest_place(slot, j):
        return rest_out.at[slot, j - (chunks - 2)]

    def rest_copy(summed, j):
        return remote(
            summed.at[j, other], rest_out.at[core, 0], core_send.at[j], core_recv.at[j], partner
        )

    def core_copy(summed, j, place):
        return remote(
            summed.at[j, other], place(core, j), core_send.at[j], core_recv.at[j], partner
        )

    def take_high(grads, k, j, summed):
        high_copy(grads, k, j).wait_recv()
        total = grads[k, high_bit, low_bit, y_bit].astype(full) + from_high[j].astype(full)
        summed[j] = total.reshape(2, rows // 2, SUB)
        for where, place in (
            (j < wide_subs, wide_place),
            (jnp.logical_and(j >= wide_subs, j < chunks - 2), thin_place),
            (j >= chunks - 2, rest_place),
        ):

            @pl.when(where)
            def _():
                core_copy(summed, j, place).start()
                place(core, j)[...] = summed[j, core]

    def first_value(arrived, last_arrived):
        mine = pl.ds(pl.multiple_of(core * half_wide, CW), CW)
        known = pl.ds(0, block + half_block)
        final = pl.ds(block + half_block, half_block)
        columns = pl.ds(0, CW)
        value = product_tn(wide_left[1], wide_right[1, :, mine])
        arrived()
        value += product_tn(wide_left_in[1, known, :], wide_right_in[1, known, columns])
        last_arrived()
        return value + product_tn(wide_left_in[1, final, :], wide_right_in[1, final, columns])

    def wide_value(tile):
        kind = jnp.where(tile < wide_chunks // 2, 1, 0)
        start = lax.rem(tile, wide_chunks // 2) * CW
        mine = pl.ds(pl.multiple_of(core * half_wide + start, CW), CW)
        value = product_tn(wide_left[kind], wide_right[kind, :, mine])
        columns = pl.ds(pl.multiple_of(start, CW), CW)
        return value + product_tn(wide_left_in[kind], wide_right_in[kind, :, columns])

    def mlp_scope(up_weight, down_weight, wide_sem):
        wide_loads = [
            pltpu.make_async_copy(up_hbm, up_weight, wide_sem.at[0]),
            pltpu.make_async_copy(down_hbm, down_weight, wide_sem.at[1]),
        ]
        for load in wide_loads:
            load.start()

        def attend_step(b, carry):
            here = pl.ds(pl.multiple_of(b * block, block), block)

            @pl.when(b == 0)
            def _():
                proj_swap.wait_recv()
                proj_high.start()

            @pl.when(b == 1)
            def _():
                proj_high.wait_recv()
                proj_y.start()
                proj_low[0].start()
                proj_y.wait_recv()
                proj_low[1].start()
                for copy in tokens_swaps:
                    copy.wait_recv()

            def norm_strip(at):
                xhat, _ = norm_stats(all_tokens[at, :].astype(full))
                thin_left[0, at, :] = (xhat * gain_one + shift_one).astype(low)

            strips(block, b * block, norm_strip)

            @pl.when(b == 0)
            def _():
                for load in loads[:4]:
                    load.wait()

            normed = thin_left[0, here, :]
            queries[here, :] = (product_nt(normed, query_weight[...]) + bias_query).astype(low)
            keys_all[here, :] = product_nt(normed, key_weight[...]).astype(low)
            values_all[here, :] = (product_nt(normed, value_weight[...]) + bias_value).astype(low)
            marks = all_slots[b]
            across = jnp.where(marks[1:2] == 1.0, marks[0:1], -1.0)
            down_ids = jnp.transpose(marks)[:, 0:1]
            allowed = down_ids == across
            q_all = queries[here, :]
            k_all = keys_all[here, :]
            v_all = values_all[here, :]
            for h in range(heads):
                cut = slice(h * HDIM, (h + 1) * HDIM)
                scores = product_nt(q_all[:, cut], k_all[:, cut]) * score_scale
                scores = jnp.where(allowed, scores, -1e30)
                scaled = jnp.exp(scores - jnp.max(scores, axis=-1, keepdims=True))
                share = 1.0 / jnp.sum(scaled, axis=-1, keepdims=True)
                probs_low = (scaled * share).astype(low)
                probs[b * heads + h] = probs_low
                thin_second[1, here, cut] = product(probs_low, v_all[:, cut]).astype(low)
            for i in range(2):

                @pl.when(b == i)
                def _():
                    mixed_swaps[i].start()

            return carry

        lax.fori_loop(0, 2, attend_step, 0)
        for copy in out_swaps:
            copy.start()
        for b in range(2):
            normed_pair(b).start()
        for copy in proj_low:
            copy.wait_recv()
        proj_core.start()
        for load in wide_loads:
            load.wait()
        out_pair(0).start()
        near = pl.ds(0, block)
        out_rows = wide_left[1, near, :]

        def act_tile(t, carry):
            at = pl.ds(pl.multiple_of(t * 512, 512), 512)
            wide_right[0, near, at] = product_nt(out_rows, down_weight[at, :]).astype(low)
            return carry

        lax.fori_loop(0, wide_chunks // 2, act_tile, 0)
        rest_from = wide_chunks * CW
        rest = wide - rest_from
        rest_at = pl.ds(rest_from, rest)
        pad_at = pl.ds(rest_from, CW // 2)
        wide_right[0, :, pad_at] = jnp.zeros((2 * block, CW // 2), low)
        wide_right[1, :, pad_at] = jnp.zeros((2 * block, CW // 2), low)
        wide_right[0, near, rest_at] = product_nt(out_rows, down_weight[rest_at, :]).astype(low)

        def make_hidden(b):
            here = pl.ds(b * block, block)
            mixed_swaps[1 - b].wait_recv()
            mixed = thin_second[1, here, :]
            mixed_far = thin_first_in[here, :]

            def proj_tile(n, inner):
                at = pl.ds(pl.multiple_of(n * 384, 384), 384)
                own_part[:, at] = product(mixed, proj_weight[:, at]) + product(
                    mixed_far, proj_other[:, at]
                )
                return inner

            lax.fori_loop(0, width // 384, proj_tile, 0)

            def hidden_strip(at):
                there = pl.ds(at.start + b * block, strip)
                value = all_tokens[there, :].astype(full) + own_part[at, :] + bias_proj
                if b == 0:
                    hidden[at, :] = value
                xhat, _ = norm_stats(value)
                wide_left[0, there, :] = (xhat * gain_two + shift_two).astype(low)

            strips(block, 0, hidden_strip)

        def gelu_parts(here, at):
            value = product_nt(wide_left[0, here, :], up_weight[at, :]) + up_bias[0:1, at]
            square = value * value
            bent = jnp.tanh(GELU_SCALE * value * (1.0 + 0.044715 * square))
            bulge = 0.5 * (1.0 + bent)
            wide_right[1, here, at] = (value * bulge).astype(low)
            return bulge + 0.5 * value * (1.0 - bent * bent) * (
                GELU_SCALE * (1.0 + 0.134145 * square)
            )

        def keep_grad(here, at, value):
            grad = value.astype(low)
            wide_right[0, here, at] = grad
            up_sum[0, :, at] += jnp.sum(grad.astype(full), axis=0, keepdims=True)

        def over_tiles(tile):
            def step(t, inner):
                tile(pl.ds(pl.multiple_of(t * CW, CW), CW))
                return inner

            lax.fori_loop(0, wide_chunks, step, 0, unroll=UNROLL)
            tile(rest_at)

        far = pl.ds(block, block)

        def far_tile(at):
            wide_right[0, far, at] = gelu_parts(far, at).astype(low)

        def near_tile(at):
            keep_grad(near, at, gelu_parts(near, at) * wide_right[0, near, at].astype(full))

        def back_tiles(b):
            grad_rows = wide_right[0, pl.ds(b * block, block), pl.ds(0, wide)]

            def back_tile(n, inner):
                at = pl.ds(pl.multiple_of(n * 384, 384), 384)
                value = product(grad_rows, up_weight[:, at])
                if b == 0:
                    own_part[:, at] = value
                else:
                    part_send[0, :, at] = value.astype(low)
                return inner

            lax.fori_loop(0, width // 384, back_tile, 0)

        proj_core.wait_recv()
        make_hidden(1)
        over_tiles(far_tile)
        left_pair(1).start()
        act_pair(1).start()
        make_hidden(0)
        left_pair(0).start()
        over_tiles(near_tile)
        act_pair(0).start()
        grad_pair(0).start()

        def slope_rows(j):
            here = pl.ds(block + j * half_block, half_block)

            def slope_tile(at):
                grad = product_nt(wide_left[1, here, :], down_weight[at, :])
                keep_grad(here, at, wide_right[0, here, at].astype(full) * grad)

            over_tiles(slope_tile)
            grad_pair(1 + j).start()

        def out_arrived(j):
            out_swaps[j].wait_recv()
            mask_rows(1, j * half_block, half_block)
            out_pair(1 + j).start()

        out_arrived(0)
        slope_rows(0)
        back_tiles(0)
        out_arrived(1)

        def pair_arrived():
            for p in range(2):
                out_pair(p).wait_recv()
            for i in range(2):
                act_pair(i).wait_recv()

        emit(early, 0, 0, first_value(pair_arrived, lambda: out_pair(2).wait_recv()), AHEAD)

        def early_step(j, inner):
            emit(early, 2 * j, 2 * j, wide_value(j), AHEAD)
            return inner

        lax.fori_loop(1, early_chunks // 2, early_step, 0)
        slope_rows(1)
        rest_pair().start()
        back_tiles(1)
        for copy in part_swaps[0]:
            copy.start()
        for i in range(FIRST):
            take_first(early, i, i)
        act_rows = wide_right[1, :, pl.ds(0, wide)]

        def down_tile(n, inner):
            at = pl.ds(pl.multiple_of(n * 384, 384), 384)
            value = product(act_rows, down_weight[:, at])
            own_down[:, at] = value[:block]
            part_send[1, :, at] = value[block:].astype(low)
            return inner

        lax.fori_loop(0, width // 384, down_tile, 0)

    pl.run_scoped(
        mlp_scope,
        pltpu.VMEM(up_hbm.shape, low),
        pltpu.VMEM(down_hbm.shape, low),
        pltpu.SemaphoreType.DMA((2,)),
    )

    def grad_scope(grads, summed):
        def held(j, action):
            @pl.when(j < early_chunks)
            def _():
                action(early, j, j)

            @pl.when(j >= early_chunks)
            def _():
                action(grads, j - early_chunks, j)

        def pump_step(i, carry):
            @pl.when(i >= core_lag)
            def _():
                rest_copy(summed, i - core_lag).wait_recv()

            @pl.when(jnp.logical_and(i >= high_lag, i < chunks + high_lag))
            def _():
                held(i - high_lag, lambda ref, k, j: take_high(ref, k, j, summed))

            @pl.when(jnp.logical_and(i >= second_lag, i < chunks + second_lag))
            def _():
                held(i - second_lag, take_second)

            @pl.when(i < chunks)
            def _():
                held(i, take_first)

            return carry

        def pump(first, last, made=wide_subs):
            def step(i, carry):
                pump_step(i, carry)

                @pl.when(i + AHEAD < made)
                def _():
                    issue(grads, i + AHEAD - early_chunks, i + AHEAD)

                return carry

            lax.fori_loop(first, last, step, 0)

        def emit_late(j, value, ahead):
            emit(grads, j - early_chunks, j, value, ahead)

        for i in range(2):
            left_pair(i).wait_recv()
        for p in range(3):
            grad_pair(p).wait_recv()

        def wide_step(j, carry):
            emit_late(2 * j, wide_value(j), FIRST + AHEAD)
            return carry

        lax.fori_loop(early_chunks // 2, wide_chunks, wide_step, 0)
        pump(FIRST, 4)

        for j in range(2):
            part_swaps[0][j].wait_recv()

            def norm_back_strip(at):
                grad = own_part[at, :] + part_in[0, at, :].astype(full)
                kept = hidden[at, :]
                xhat, inverse = norm_stats(kept)
                own_down[at, :] += kept
                out_rows = wide_left[1, at, :].astype(full)
                value = out_rows + norm_grad(xhat, inverse, gain_two, grad)
                hidden[at, :] = value
                rounded = value.astype(low)
                thin_left[1, at, :] = rounded
                totals[2:3] += column_sums(rounded.astype(full))[None]
                totals[3:4] += column_sums(grad * xhat)[None]
                totals[4:5] += column_sums(grad)[None]
                totals[5:6] += column_sums(out_rows)[None]

            strips(half_block, j * half_block, norm_back_strip)
            hidden_swaps[j].start()
            if j == 0:
                pump(4, 5)
        for copy in part_swaps[1]:
            copy.start()

        pump(5, 7)

        def back_step(b, carry):
            here = pl.ds(pl.multiple_of(b * block, block), block)

            @pl.when(b == 1)
            def _():
                for copy in part_swaps[0]:
                    copy.wait_send()
                for copy in hidden_swaps:
                    copy.wait_recv()
                for i in range(2):
                    other_pair(i).start()

            grad_mixed = product_nt(thin_left[1, here, :], proj_weight[...]).astype(low)
            q_all = queries[here, :]
            k_all = keys_all[here, :]
            v_all = values_all[here, :]
            for h in range(heads):
                cut = slice(h * HDIM, (h + 1) * HDIM)
                probs_low = probs[b * heads + h]
                probs_full = probs_low.astype(full)
                mixed_grad = grad_mixed[:, cut]
                grad_probs = product_nt(mixed_grad, v_all[:, cut])
                weighted = probs_full * grad_probs
                grad_scores = (
                    weighted - probs_full * jnp.sum(weighted, axis=-1, keepdims=True)
                ).astype(low)
                thin_first[0, here, cut] = (product(grad_scores, k_all[:, cut]) * score_scale).astype(low)
                thin_second[0, here, cut] = (
                    product_tn(grad_scores, q_all[:, cut]) * score_scale
                ).astype(low)
                thin_first[1, here, cut] = product_tn(probs_low, mixed_grad).astype(low)

            @pl.when(b == 0)
            def _():
                first_pair(0).start()
                second_pair(0).start()

            @pl.when(b == 1)
            def _():
                first_pair(1).start()
                second_pair(1).start()

            grad_q = thin_first[0, here, :]
            grad_k = thin_second[0, here, :]
            grad_v = thin_first[1, here, :]

            def normed_tile(n, inner):
                at = pl.ds(pl.multiple_of(n * 384, 384), 384)
                value = (
                    product(grad_q, query_weight[:, at])
                    + product(grad_k, key_weight[:, at])
                    + product(grad_v, value_weight[:, at])
                )

                @pl.when(b == 0)
                def _():
                    own_part[:, at] = value

                @pl.when(b == 1)
                def _():
                    part_send[0, :, at] = value.astype(low)

                return inner

            lax.fori_loop(0, width // 384, normed_tile, 0)
            pump(7 + 4 * b, 11 + 3 * b)
            return carry

        lax.fori_loop(0, 2, back_step, 0)
        for copy in part_swaps[2]:
            copy.start()

        for b in range(2):
            for pair in (normed_pair, other_pair, first_pair, second_pair):
                pair(b).wait_recv()
        rest_pair().wait_recv()

        def first_part(columns):
            return product_tn(thin_left[0], thin_first[core, :, columns]) + product_tn(
                thin_left_in[...], thin_first_in[:, columns]
            )

        def second_part(columns):
            return product_tn(thin_left[core], thin_second[core, :, columns]) + product_tn(
                thin_other_in[...], thin_second_in[:, columns]
            )

        def thin_step(j, carry):
            columns = pl.ds(pl.multiple_of(j * CW, CW), CW)
            ahead = 14 + j + AHEAD
            emit_late(2 * (wide_chunks + 2 * j), first_part(columns), ahead)
            emit_late(2 * (wide_chunks + 2 * j + 1), second_part(columns), ahead)
            pump(14 + j, 15 + 2 * j, 2 * (wide_chunks + 2 * j + 2))
            return carry

        lax.fori_loop(0, 2, thin_step, 0)
        thin_rest = pl.ds(2 * CW, thin - 2 * CW)
        wide_rest = pl.ds(wide_chunks * CW, CW // 2)
        emit_late(
            chunks - 2,
            jnp.concatenate(
                [
                    product_tn(wide_left[core], wide_right[core, :, wide_rest])
                    + product_tn(wide_left_in[core], rest_right_in[...]),
                    first_part(thin_rest),
                    second_part(thin_rest),
                ],
                axis=1,
            ),
            17 + AHEAD,
        )
        pump(17, 19, chunks)

        for copy in part_swaps[2]:
            copy.wait_recv()
        for copy in part_swaps[1]:
            copy.wait_send()

        def final_strip(at):
            grad = own_part[at, :] + part_in[0, at, :].astype(full)
            xhat, inverse = norm_stats(all_tokens[at, :].astype(full))
            part_send[1, at, :] = (
                hidden[at, :] + norm_grad(xhat, inverse, gain_one, grad)
            ).astype(low)
            totals[0:1] += column_sums(grad * xhat)[None]
            totals[1:2] += column_sums(grad)[None]

        strips(block, 0, final_strip)
        sums = totals[...]
        lower = sums[:, :thin]
        upper = sums[:, thin:]
        halves[0] = jnp.where(shard == 0, lower, upper)
        halves[1] = jnp.where(shard == 0, upper, lower)
        halves_swap.start()
        grad_query_bias = column_sums(thin_first[0].astype(full))[None]
        grad_value_bias = column_sums(thin_first[1].astype(full))[None]
        pump(19, 21, chunks)
        halves_swap.wait_recv()
        vector_sum[0] = halves[0] + halves_in[...]
        vector_sum[0, 6:7] = grad_query_bias
        vector_sum[0, 7:8] = grad_value_bias

        def vector_copies(i):
            return (
                remote(
                    vector_sum.at[i], vector_in.at[i], vec_send.at[2 * i], vec_recv.at[2 * i], vector_peers[i]
                ),
                remote(
                    up_sum.at[i], up_in.at[i], vec_send.at[2 * i + 1], vec_recv.at[2 * i + 1], vector_peers[i]
                ),
            )

        def vector_start(i):
            for copy in vector_copies(i):
                copy.start()

        def vector_finish(i):
            for copy in vector_copies(i):
                copy.wait_recv()
            vector_sum[i + 1] = vector_sum[i] + vector_in[i]
            up_sum[i + 1] = up_sum[i] + up_in[i]

        vector_start(0)
        for copy in part_swaps[1]:
            copy.wait_recv()
        for copy in part_swaps[2]:
            copy.wait_send()

        def out_strip(at):
            value = own_down[at, :] + part_in[1, at, :].astype(full) + bias_down
            part_send[0, at, :] = value.astype(low)

        strips(block, 0, out_strip)
        alive = jnp.transpose(all_slots[0])[:, 1:2].astype(low)
        part_send[0] = part_send[0] * alive

        def drain(j, carry):
            held(j, lambda ref, k, i: first_copy(ref, k, i, False).wait_send())
            held(j, lambda ref, k, i: second_copy(ref, k, i, False).wait_send())
            held(j, lambda ref, k, i: high_copy(ref, k, i).wait_send())
            rest_copy(summed, j).wait_send()
            return carry

        out_copies = [
            pltpu.make_async_copy(source, target, out_sem.at[i])
            for i, (source, target) in enumerate(
                (
                    (part_send, rows_hbm),
                    (wide_out, wide_hbm),
                    (vector_sum.at[4], vectors_hbm),
                    (up_sum.at[4], up_sum_hbm),
                    (thin_out, thin_hbm),
                    (rest_out, rest_hbm),
                )
            )
        ]
        out_copies[0].start()
        pump(21, 22, chunks)
        vector_finish(0)
        vector_start(1)
        pump(22, 24, chunks)
        out_copies[1].start()
        vector_finish(1)
        vector_start(2)
        pump(24, 25, chunks)
        vector_finish(2)
        vector_start(3)
        pump(25, 29, chunks)
        vector_finish(3)
        out_copies[2].start()
        out_copies[3].start()
        lax.fori_loop(0, chunks - core_lag, drain, 0)
        pump(29, 32, chunks)
        out_copies[4].start()
        pump(32, chunks + core_lag, chunks)
        out_copies[5].start()
        lax.fori_loop(chunks - core_lag, chunks, drain, 0)
        for copy in out_copies:
            copy.wait()
        for i in range(4):
            for copy in vector_copies(i):
                copy.wait_send()

    pl.run_scoped(
        grad_scope,
        pltpu.VMEM((chunks - early_chunks, 2, 2, 2, rows, SUB), low),
        pltpu.VMEM((chunks, 2, rows // 2, SUB), full),
    )
    for copy in [vectors_swap, slots_swap, *tokens_swaps, *out_swaps, *mixed_swaps, proj_swap, halves_swap]:
        copy.wait_send()
    for copy in hidden_swaps:
        copy.wait_send()
    for copy in (proj_high, proj_y, *proj_low, proj_core):
        copy.wait_send()
    for p in range(3):
        out_pair(p).wait_send()
        grad_pair(p).wait_send()
    rest_pair().wait_send()
    for b in range(2):
        for pair in (left_pair, act_pair, normed_pair, other_pair, first_pair, second_pair):
            pair(b).wait_send()


def publish_kernel(rows_in, wide_in, thin_in, rest_in, vectors_in, up_in, *refs):
    outs, refs = refs[:17], refs[17:]
    rows_at, wide_at, thin_at, rest_at, vectors_at, up_at = refs[:6]
    flats, in_sem, out_sem = refs[6:15], refs[15], refs[16]
    wide_main = wide_in.shape[2]
    thin_main = thin_in.shape[3]
    wide, thin = wide_at.shape[2], thin_at.shape[3]
    loads = [
        pltpu.make_async_copy(source, target, in_sem.at[i])
        for i, (source, target) in enumerate(
            (
                (vectors_in, vectors_at),
                (up_in, up_at),
                (rest_in, rest_at),
                (rows_in, rows_at),
                (thin_in, thin_at.at[:, :, :, pl.ds(0, thin_main)]),
                (wide_in, wide_at.at[:, :, pl.ds(0, wide_main)]),
            )
        )
    ]
    for load in loads:
        load.start()
    stores = []

    def store(source, place):
        copy = pltpu.make_async_copy(source, outs[place], out_sem.at[place])
        copy.start()
        stores.append(copy)

    loads[0].wait()
    loads[1].wait()
    for i in range(8):
        flats[i][...] = vectors_at[i : i + 1, :].reshape(flats[i].shape)
    flats[8][...] = up_at[:, :wide].reshape(flats[8].shape)
    loads[2].wait()
    loads[3].wait()
    store(rows_at.at[0], 0)
    store(rows_at.at[1], 1)
    for slot in range(2):
        wide_at[slot, :, wide_main:] = rest_at[slot, 0, :, : wide - wide_main]
        for place in range(2):
            start = place * (thin - thin_main)
            thin_at[slot, place, :, thin_main:] = rest_at[
                slot, 1, :, start : start + thin - thin_main
            ]
    loads[4].wait()
    for i, place in enumerate((4, 6, 7, 9)):
        store(thin_at.at[i // 2, i % 2], place)
    loads[5].wait()
    store(wide_at.at[0], 13)
    store(wide_at.at[1], 15)
    for flat, place in zip(flats, (2, 3, 10, 11, 12, 16, 5, 8, 14)):
        store(flat, place)
    for copy in stores:
        copy.wait()


def publish_call(packed, wide):
    full = jnp.float32
    rows_out, wide_out, thin_out, rest_out, vectors, up_bias_grad = packed
    thin = vectors.shape[1]
    half = wide_out.shape[1]
    anywhere = pl.BlockSpec(memory_space=pl.ANY)
    vector = jax.ShapeDtypeStruct((thin,), full)
    matrix = jax.ShapeDtypeStruct((half, thin), full)
    tall = jax.ShapeDtypeStruct((half, wide), full)
    rows = jax.ShapeDtypeStruct(rows_out.shape[1:], rows_out.dtype)
    return pl.pallas_call(
        publish_kernel,
        out_shape=(
            rows, rows, vector, vector, matrix, vector, matrix, matrix, vector, matrix, vector,
            vector, vector, tall, jax.ShapeDtypeStruct((wide,), full), tall, vector,
        ),
        in_specs=[anywhere] * 6,
        out_specs=(anywhere,) * 17,
        scratch_shapes=[
            pltpu.VMEM(rows_out.shape, rows_out.dtype),
            pltpu.VMEM((2, half, wide), full),
            pltpu.VMEM((2, 2, half, thin), full),
            pltpu.VMEM(rest_out.shape, full),
            pltpu.VMEM(vectors.shape, full),
            pltpu.VMEM(up_bias_grad.shape, full),
            *[pltpu.VMEM((thin,), full)] * 8,
            pltpu.VMEM((wide,), full),
            pltpu.SemaphoreType.DMA((6,)),
            pltpu.SemaphoreType.DMA((17,)),
        ],
        name="publish",
    )(*packed)


def layer_call(tokens, out_grad, slots, vectors, up_bias, matrices):
    query_weight, up_weight, down_weight = matrices[0], matrices[4], matrices[5]
    low = jnp.bfloat16
    full = jnp.float32
    block, width = tokens.shape
    thin = query_weight.shape[0]
    wide = up_weight.shape[0]
    wide_pad = wide + -wide % 128
    heads = thin // HDIM
    replicas = lax.axis_size("replica")
    rows = width // replicas * 2
    wide_main = wide // CW * CW
    chunks = 2 * (wide // CW + 5)
    half = rows // 2
    both = 2 * block
    anywhere = pl.BlockSpec(memory_space=pl.ANY)
    dma = pltpu.SemaphoreType.DMA
    return pl.pallas_call(
        layer_kernel,
        out_shape=(
            jax.ShapeDtypeStruct((2,) + tokens.shape, low),
            jax.ShapeDtypeStruct((2, half, wide_main), full),
            jax.ShapeDtypeStruct((2, 2, half, 2 * CW), full),
            jax.ShapeDtypeStruct((2, 2, half, SUB), full),
            jax.ShapeDtypeStruct((8, thin), full),
            jax.ShapeDtypeStruct((1, wide_pad), full),
        ),
        in_specs=[anywhere] * 19,
        out_specs=(anywhere,) * 6,
        scratch_shapes=[
            pltpu.VMEM((2, half, wide_main), full),
            pltpu.VMEM((2, 2, half, 2 * CW), full),
            pltpu.VMEM((2, 2, half, SUB), full),
            pltpu.VMEM((8, block), full),
            pltpu.VMEM((8, thin), full),
            pltpu.VMEM((8, wide), full),
            pltpu.VMEM((thin, width), low),
            pltpu.VMEM((thin, width), low),
            pltpu.VMEM((thin, width), low),
            pltpu.VMEM((thin, width), low),
            pltpu.VMEM((thin, width), low),
            pltpu.VMEM((both, width), low),
            pltpu.VMEM((2, 8, block), full),
            pltpu.VMEM((8, thin), full),
            pltpu.VMEM((both, thin), low),
            pltpu.VMEM((both, thin), low),
            pltpu.VMEM((both, thin), low),
            pltpu.VMEM((2 * heads, block, block), low),
            pltpu.VMEM((block, width), full),
            pltpu.VMEM((block, width), full),
            pltpu.VMEM((block, width), full),
            pltpu.VMEM((2, block, width), low),
            pltpu.VMEM((2, block, width), low),
            pltpu.VMEM((2, both, width), low),
            pltpu.VMEM((2, both, wide_pad), low),
            pltpu.VMEM((2, both, width), low),
            pltpu.VMEM((2, both, thin), low),
            pltpu.VMEM((2, both, thin), low),
            pltpu.VMEM((2, both, width), low),
            pltpu.VMEM((2, both, wide_main // 2), low),
            pltpu.VMEM((both, SUB), low),
            pltpu.VMEM((both, width), low),
            pltpu.VMEM((both, width), low),
            pltpu.VMEM((both, thin), low),
            pltpu.VMEM((both, thin), low),
            pltpu.VMEM((EARLY, 2, 2, 2, rows, SUB), low),
            pltpu.VMEM((chunks, 2, 2, rows, SUB), low),
            pltpu.VMEM((chunks, 2, rows, SUB), low),
            pltpu.VMEM((chunks, rows, SUB), low),
            pltpu.VMEM((8, width), full),
            pltpu.VMEM((2, 8, thin), full),
            pltpu.VMEM((8, thin), full),
            pltpu.VMEM((5, 8, thin), full),
            pltpu.VMEM((4, 8, thin), full),
            pltpu.VMEM((5, 1, wide_pad), full),
            pltpu.VMEM((4, 1, wide_pad), full),
            *[pltpu.VMEM((thin,), low)] * 8,
            *[pltpu.VMEM((block,), jnp.int32)] * 2,
            pltpu.VMEM((wide,), low),
            dma((11,)),
            dma((6,)),
            dma((18,)),
            dma((18,)),
            dma((5,)),
            dma((5,)),
            dma((19,)),
            dma((19,)),
            dma((chunks,)),
            dma((chunks,)),
            dma((chunks,)),
            dma((chunks,)),
            dma((chunks,)),
            dma((chunks,)),
            dma((chunks,)),
            dma((chunks,)),
            dma((8,)),
            dma((8,)),
            dma((6,)),
        ],
        compiler_params=pltpu.CompilerParams(
            collective_id=0, has_side_effects=True, vmem_limit_bytes=67043328
        ),
        name="layer",
    )(tokens, out_grad, *slots, *vectors, up_bias, *matrices)


def whole_layer(
    tokens, out_grad, picture_ids, live_slots, ln1_gain, ln1_bias, query_weight, query_bias,
    key_weight, value_weight, value_bias, proj_weight, proj_bias, ln2_gain, ln2_bias, up_weight,
    up_bias, down_weight, down_bias,
):
    width = tokens.shape[1]
    if not by_kernel(lax.axis_size("replica"), width):
        return paired(
            tokens, out_grad, picture_ids, live_slots, ln1_gain, ln1_bias, query_weight,
            query_bias, key_weight, value_weight, value_bias, proj_weight, proj_bias, ln2_gain,
            ln2_bias, up_weight, up_bias, down_weight, down_bias,
        )
    packed = layer_call(
        tokens,
        out_grad,
        (picture_ids, live_slots),
        (ln1_gain, ln1_bias, proj_bias, ln2_gain, ln2_bias, down_bias, query_bias, value_bias),
        up_bias,
        (query_weight.T, key_weight.T, value_weight.T, proj_weight, up_weight.T, down_weight),
    )
    outs = list(publish_call(packed, up_weight.shape[1]))
    outs[9] = outs[9].T
    outs[15] = outs[15].T
    return tuple(outs)


def solution(mesh):
    in_specs = (
        P(("shard", "replica"), None),
        P(("shard", "replica"), None),
        P(("shard", "replica")),
        P(("shard", "replica")),
        P("shard"),
        P("shard"),
        P(None, "shard"),
        P("shard"),
        P(None, "shard"),
        P(None, "shard"),
        P("shard"),
        P("shard", None),
        P("shard"),
        P("shard"),
        P("shard"),
        P(None, "shard"),
        P("shard"),
        P("shard", None),
        P("shard"),
    )
    out_specs = (
        P(("shard", "replica"), None),
        P(("shard", "replica"), None),
        P("shard"),
        P("shard"),
        P("replica", "shard"),
        P("shard"),
        P("replica", "shard"),
        P("replica", "shard"),
        P("shard"),
        P("shard", "replica"),
        P("shard"),
        P("shard"),
        P("shard"),
        P("replica", "shard"),
        P("shard"),
        P("shard", "replica"),
        P("shard"),
    )
    return jax.shard_map(whole_layer, mesh=mesh, in_specs=in_specs, out_specs=out_specs, check_vma=False)
```
